256 devices in a mesh: gx: 8 (over z_lo, core), gy: 32 (over z_hi, y, x).
Axes of the slice: x: 4, y: 4, z: 8 (z_hi: 2, z_lo: 4; z = z_hi * 4 + z_lo), core: 2. Of those that a mesh axis runs over, the one named last changes fastest.
Arguments:
- density: float32 [128, 512, 256], P('gx', 'gy'), may hold values from 0.5 to 2
- momentum: float32 [3, 128, 512, 256], P(None, 'gx', 'gy'), may hold values from -3 to 3
- energy: float32 [128, 512, 256], P('gx', 'gy'), may hold values from 1 to 3
- parcel_mass: float32 [2097152], P(('gx', 'gy')), may hold values from 0.2 to 2
- droplet_velocity: float32 [3, 2097152], P(None, ('gx', 'gy')), may hold values from -4 to 4
- parcel_temp: float32 [2097152], P(('gx', 'gy')), may hold values from 0.1 to 4
- parcel_cell: int32 [3, 2097152], P(None, ('gx', 'gy')), may hold values from 0 to 511, as said below
- parcel_count: int32 [256], P(('gx', 'gy')), may hold values from 2048 to 8192, as said below
Outputs:
- updated_fluid_density: float32 [128, 512, 256], P('gx', 'gy')
- updated_fluid_impulse: float32 [3, 128, 512, 256], P(None, 'gx', 'gy')
- energy_out: float32 [128, 512, 256], P('gx', 'gy')
- moved_state: float32 [5, 2621440], P(None, ('gx', 'gy'))
- moved_cell: int32 [3, 2621440], P(None, ('gx', 'gy'))
- time_step: float32 [], replicated
The draws below stay inside these ranges and needn't reach their ends.
Inputs may be any that keep to these rules, and one draw needn't show every extreme that they name: `parcel_cell`: each row of device d lies in d's block of 16 x 16 x 256 cells or in the layer of cells just beyond one of its four side faces inside the grid, never beyond an edge. Among the live rows of one device at most 512 lie beyond any one face; on every device some face along each of the two axes has exactly 512. `parcel_count`: some devices are full.
All inputs are finite; a program needn't handle non-finite values.
Results may differ from the reference program's by a relative error of at most 0.0003.
Values sent between devices are 32-bit elements; how exact they have to be, the bound alone decides.
No kernel may reach another device: no remote copies, remote signals or barrier semaphores. Data moves between devices by JAX's collectives and lax.ppermute only.
A program may use at most 192 MiB of HBM per device.

```python
import math
import jax
import jax.numpy as jnp
from jax import lax

CX = 16
CY = 16
NZ = 256
P_DEV = 8192
MOVE = 512
SLOTS = 10240
NX = 128
NY = 512
PARCELS = 2097152
N_GX = 8
N_GY = 32
DEVICES = 256


def parcel_state_tables(key):
    base = jax.random.fold_in(key, 11)
    keys = jax.random.split(base, 8)
    device = jnp.arange(DEVICES, dtype=jnp.int32)
    col_x = device // N_GY
    col_y = device % N_GY
    partial_parcel_count = jax.random.randint(keys[0], (DEVICES,), P_DEV // 4, P_DEV // 2 + 1, dtype=jnp.int32)
    count = jnp.where(col_x == 0, P_DEV, partial_parcel_count).astype(jnp.int32)
    exists = jnp.stack([col_x > 0, col_x < N_GX - 1, col_y > 0, col_y < N_GY - 1], axis=1)
    loads = jax.random.randint(keys[1], (DEVICES, 4), MOVE // 4, MOVE + 1, dtype=jnp.int32)
    drag_horizontal = jnp.where(col_x < N_GX - 1, 1, 0)
    force_y = jnp.where(col_y < N_GY - 1, 3, 2)
    which = jnp.arange(4, dtype=jnp.int32)[None]
    loads = jnp.where((which == drag_horizontal[:, None]) | (which == force_y[:, None]), MOVE, loads)
    loads = jnp.where(exists, loads, 0)
    ends = jnp.cumsum(loads, axis=1)
    row_index = jnp.arange(P_DEV, dtype=jnp.int32)[None]
    spread = 2 ** 30 // (2 * P_DEV)
    scores = jax.random.randint(keys[2], (DEVICES, P_DEV), 0, spread, dtype=jnp.int32) * P_DEV + row_index
    scores = jnp.where(row_index < count[:, None], scores, 2 ** 30 + row_index)
    order = jnp.argsort(scores, axis=1, stable=True)
    position = jnp.argsort(order, axis=1, stable=True).astype(jnp.int32)
    heading = jnp.sum((position[:, :, None] >= ends[:, None, :]).astype(jnp.int32), axis=2)
    inside_x = jax.random.randint(keys[3], (DEVICES, P_DEV), 0, CX, dtype=jnp.int32) + col_x[:, None] * CX
    inside_y = jax.random.randint(keys[4], (DEVICES, P_DEV), 0, CY, dtype=jnp.int32) + col_y[:, None] * CY
    depth = jax.random.randint(keys[5], (DEVICES, P_DEV), 0, NZ, dtype=jnp.int32)
    cell_x = jnp.where(heading == 0, col_x[:, None] * CX - 1, jnp.where(heading == 1, col_x[:, None] * CX + CX, inside_x))
    cell_y = jnp.where(heading == 2, col_y[:, None] * CY - 1, jnp.where(heading == 3, col_y[:, None] * CY + CY, inside_y))
    cells = jnp.stack([cell_x, cell_y, depth]).reshape(3, DEVICES * P_DEV).astype(jnp.int32)
    return (cells, count)


def draw_parcel_cell(key, part):
    return parcel_state_tables(key)[0]


def draw_parcel_count(key, part):
    return parcel_state_tables(key)[1]


def level_of(stream_key, dims, cuts, smallest, top_value):
    loudness = 1.0
    for dim, blocks in cuts:
        heights = jax.random.uniform(jax.random.fold_in(jax.random.fold_in(stream_key, 6), dim), (blocks,), jnp.float32, smallest / len(cuts), top_value / len(cuts))
        loudness = loudness * jnp.repeat(jnp.exp(heights), dims[dim] // blocks).reshape((-1,) + (1,) * (len(dims) - 1 - dim))
    return loudness


def noise(stream_key, extent, deviation, reach, shards=(), held_as=jnp.bfloat16):
    values = jax.random.normal(stream_key, extent, jnp.float32) * deviation
    if len(shards) > 0:
        values = level_of(stream_key, extent, shards, -0.22, 0.18) * values
    return jnp.clip(values, min=-reach, max=reach).astype(held_as)


def setup_inputs(seed: int = 0) -> dict:
    key_of = jax.random.split(jax.random.key(seed), 9)
    density = jnp.clip(0.5 + 1.5 * jax.random.uniform(key_of[0], (NX, NY, NZ), jnp.float32) ** level_of(key_of[0], (NX, NY, NZ), ((0, 8), (1, 32)), -0.2, 0.2), 0.5, 2.0)
    momentum = noise(key_of[1], (3, NX, NY, NZ), 0.5, 3.0, ((1, 8), (2, 32)), jnp.float32)
    energy = jnp.clip(1.0 + 2.0 * jax.random.uniform(key_of[2], (NX, NY, NZ), jnp.float32) ** level_of(key_of[2], (NX, NY, NZ), ((0, 8), (1, 32)), -0.2, 0.2), 1.0, 3.0)
    parcel_mass = jnp.clip(jnp.exp(math.log(2.0) - 2.3025851 * jax.random.uniform(key_of[3], (PARCELS,), jnp.float32) ** level_of(key_of[3], (PARCELS,), ((0, 256),), -0.2, 0.2)), 0.2, 2.0)
    droplet_velocity = noise(key_of[4], (3, PARCELS), 1.0, 4.0, ((1, 256),), jnp.float32)
    parcel_temp = jnp.clip(0.1 + 3.9 * jax.random.uniform(key_of[5], (PARCELS,), jnp.float32) ** level_of(key_of[5], (PARCELS,), ((0, 256),), -0.2, 0.2), 0.1, 4.0)
    parcel_cell = draw_parcel_cell(jax.random.fold_in(key_of[8], 71), 0)
    parcel_count = draw_parcel_count(jax.random.fold_in(key_of[8], 71), 0)
    return dict(density=density, momentum=momentum, energy=energy, parcel_mass=parcel_mass, droplet_velocity=droplet_velocity, parcel_temp=parcel_temp, parcel_cell=parcel_cell, parcel_count=parcel_count)


ADIABATIC_INDEX = 1.4
KICK = 0.25
COURANT = 0.4
SHRINK = 0.5

def cell_sums(values, cell_ids, segments):
    return jax.ops.segment_sum(values, cell_ids, num_segments=segments)

def reference(density, momentum, energy, parcel_mass, droplet_velocity, parcel_temp, parcel_cell, parcel_count):
    row_index = jnp.arange(parcel_mass.shape[0], dtype=jnp.int32)
    device = row_index // P_DEV
    local_row = row_index % P_DEV
    live = local_row < parcel_count[device]
    boiled_off_amount = jnp.where(live, parcel_mass * jax.nn.sigmoid(2.0 * (parcel_temp - 2.0)), 0.0)
    specific_movement_budget = 0.5 * lax.optimization_barrier(jnp.sum(droplet_velocity * droplet_velocity, axis=0))
    sources = jnp.concatenate([boiled_off_amount[None], boiled_off_amount[None] * droplet_velocity, (boiled_off_amount * (parcel_temp + specific_movement_budget))[None]], axis=0)
    flat_cell = (parcel_cell[0] * NY + parcel_cell[1]) * NZ + parcel_cell[2]
    deposit = jax.vmap(lambda values: cell_sums(values, flat_cell, NX * NY * NZ))(sources).reshape(5, NX, NY, NZ)
    updated_fluid_density = density + deposit[0]
    energy_out = energy + deposit[4]
    lifted = momentum + deposit[1:4]
    normal_stress_field = (ADIABATIC_INDEX - 1.0) * energy_out
    padded = jnp.pad(normal_stress_field, 1)
    grad_x = 0.5 * (padded[2:, 1:-1, 1:-1] - padded[:-2, 1:-1, 1:-1])
    grad_y = 0.5 * (padded[1:-1, 2:, 1:-1] - padded[1:-1, :-2, 1:-1])
    grad_z = 0.5 * (padded[1:-1, 1:-1, 2:] - padded[1:-1, 1:-1, :-2])
    updated_fluid_impulse = lifted - KICK * jnp.stack([grad_x, grad_y, grad_z])
    ambient_stream_speed = updated_fluid_impulse / updated_fluid_density[None]
    acoustic_signal = lax.optimization_barrier(jnp.max(jnp.abs(ambient_stream_speed), axis=0)) + jnp.sqrt(ADIABATIC_INDEX * normal_stress_field / updated_fluid_density)
    time_step = COURANT / jnp.max(acoustic_signal)
    col_x = device // N_GY
    col_y = device % N_GY
    local_x = parcel_cell[0] - col_x * CX
    local_y = parcel_cell[1] - col_y * CY
    heading = jnp.where(local_x < 0, 0, jnp.where(local_x >= CX, 1, jnp.where(local_y < 0, 2, jnp.where(local_y >= CY, 3, 4))))
    heading = jnp.where(live, heading, 5).astype(jnp.int32)
    onehot = (heading[:, None] == jnp.arange(4, dtype=jnp.int32)[None]).astype(jnp.int32).reshape(DEVICES, P_DEV, 4)
    earlier = (jnp.cumsum(onehot, axis=1) - onehot).reshape(DEVICES * P_DEV, 4)
    rank = lax.optimization_barrier(jnp.sum(earlier * onehot.reshape(DEVICES * P_DEV, 4), axis=1))
    shift_table = jnp.array([-N_GY, N_GY, -1, 1, 0, 0], dtype=jnp.int32)
    bucket_table = jnp.array([1, 0, 3, 2, 0, 0], dtype=jnp.int32)
    target_dev = device + shift_table[heading]
    moving = jnp.where(heading < 4, target_dev * SLOTS + P_DEV + bucket_table[heading] * MOVE + rank, SLOTS * DEVICES)
    target = jnp.where(heading == 4, device * SLOTS + local_row, moving).astype(jnp.int32)
    carried_records = jnp.concatenate([(parcel_mass - SHRINK * boiled_off_amount)[None], droplet_velocity, parcel_temp[None], parcel_cell.astype(jnp.float32)], axis=0)
    table = jnp.zeros((8, SLOTS * DEVICES), carried_records.dtype).at[:, target].set(carried_records, mode='drop')
    moved_state = table[:5]
    moved_cell = table[5:].astype(jnp.int32)
    return (updated_fluid_density, updated_fluid_impulse, energy_out, moved_state, moved_cell, time_step)
```

```python
import functools

import jax
import jax.numpy as jnp
from jax import lax
from jax.experimental import pallas as pl
from jax.experimental.pallas import tpu as pltpu
from jax.sharding import PartitionSpec as P

ADIABATIC_INDEX = 1.4
KICK = 0.25
COURANT = 0.4
SHRINK = 0.5

F32 = jnp.float32
BF16 = jnp.bfloat16
I32 = jnp.int32
LANES = 128
VMEM = pltpu.VMEM
TRANSPOSED = (((1,), (1,)), ((), ()))


def iota(shape, dim, dtype=I32):
    return lax.broadcasted_iota(dtype, shape, dim)


def sigmoid_of(temp):
    return 1.0 / (1.0 + jnp.exp(-2.0 * (temp - 2.0)))


def prep_kernel(
    cells_x, cells_y, count, mass, temp, vel, cell,
    out0, out1, out2, out3, stay,
    pay, cx, cy, pos, compact, table_v, table_s, tiles, sem,
):
    chunks = mass.shape[0]
    anchor_x = lax.axis_index("gx") * cells_x
    anchor_y = lax.axis_index("gy") * cells_y
    for b in range(chunks):
        lanes = slice(b * LANES, (b + 1) * LANES)
        cx[b : b + 1, :] = cell[0:1, lanes]
        cy[b : b + 1, :] = cell[1:2, lanes]
    shape = (chunks, LANES)
    live = iota(shape, 0) * LANES + iota(shape, 1) < count[0]
    kept = mass[...] * (1.0 - SHRINK * jnp.where(live, sigmoid_of(temp[...]), 0.0))
    local_x = cx[...] - anchor_x
    local_y = cy[...] - anchor_y
    heading = jnp.where(
        local_x < 0,
        0,
        jnp.where(
            local_x >= cells_x, 1, jnp.where(local_y < 0, 2, jnp.where(local_y >= cells_y, 3, 4))
        ),
    )
    heading = jnp.where(live, heading, 5)
    masks = [jnp.where(heading == h, 1.0, 0.0) for h in range(4)]
    lane_r = iota((LANES, 2 * LANES), 0)
    lane_c = iota((LANES, 2 * LANES), 1)
    scan = jnp.where((lane_r < lane_c) | (lane_c >= LANES), 1.0, 0.0).astype(BF16)
    both = jnp.dot(
        jnp.concatenate(masks, axis=0).astype(BF16), scan, preferred_element_type=F32
    )
    inner = [both[h * chunks : (h + 1) * chunks, :LANES] for h in range(4)]
    total = [both[h * chunks : (h + 1) * chunks, LANES:] for h in range(4)]
    below = jnp.where(iota((chunks, chunks), 1) < iota((chunks, chunks), 0), 1.0, 0.0).astype(BF16)
    base = jnp.dot(
        below, jnp.concatenate(total, axis=1).astype(BF16), preferred_element_type=F32
    )
    lane = iota(shape, 1)
    offset = jnp.zeros(shape, F32)
    place = jnp.full(shape, -1.0, F32)
    words = jnp.zeros(shape, I32)
    for h in range(4):
        place = jnp.where(heading == h, inner[h] + offset, place)
        base_h = base[:, h * LANES : (h + 1) * LANES]
        word = base_h.astype(I32) + offset.astype(I32) * 1024 + total[h].astype(I32) * (1024 * 256)
        words = jnp.where(lane == h, word, words)
        offset = offset + total[h]
    table_v[...] = words
    load = pltpu.make_async_copy(table_v, table_s, sem)
    load.start()
    pos[...] = place
    pay[1:4, :] = vel[...]
    pay[5:8, :] = cell[...].astype(F32)
    stays = jnp.where(heading == 4, 1.0, 0.0)
    for b in range(chunks):
        lanes = slice(b * LANES, (b + 1) * LANES)
        pay[0:1, lanes] = kept[b : b + 1, :]
        pay[4:5, lanes] = temp[b : b + 1, :]
    for b in range(chunks):
        lanes = slice(b * LANES, (b + 1) * LANES)
        stay[:, lanes] = jnp.where(stays[b : b + 1, :] > 0.0, pay[:, lanes], 0.0)
    group = 16

    def pack(g, carry):
        for u in range(group):
            b = g * group + u
            slots = pos[pl.ds(b, 1), :]
            onehot = jnp.where(slots == iota((LANES, LANES), 0).astype(F32), 1.0, 0.0).astype(BF16)
            rows = pay[:, pl.ds(pl.multiple_of(b * LANES, LANES), LANES)]
            high = rows.astype(BF16).astype(F32)
            rest = rows - high
            middle = rest.astype(BF16).astype(F32)
            low = rest - middle
            parts = jnp.concatenate([high, middle, low, jnp.zeros_like(low)], axis=0).astype(BF16)
            got = lax.dot_general(parts, onehot, TRANSPOSED, preferred_element_type=F32)
            compact[b] = got[0:8] + got[8:16] + got[16:24]
        return carry

    lax.fori_loop(0, chunks // group, pack, 0)
    tiles[...] = jnp.zeros(tiles.shape, F32)
    load.wait()
    lane8 = iota((8, LANES), 1)
    unroll = 8

    def place_all(g, carry):
        carry = list(carry)
        for u in range(unroll):
            b = g * unroll + u
            rows = compact[b]
            for h in range(4):
                word = table_s[b, h]
                start = word & 1023
                first = (word >> 10) & 255
                number = word >> 18
                within = start & (LANES - 1)
                end = within + number
                turned = pltpu.roll(rows, (start - first) & (LANES - 1), 1)
                merged = jnp.where((lane8 >= within) & (lane8 < end), turned, carry[h])
                tiles[h, start >> 7] = merged
                over = jnp.where(lane8 < end - LANES, turned, 0.0)
                carry[h] = jnp.where(end >= LANES, over, merged)
        return tuple(carry)

    carry = lax.fori_loop(
        0, chunks // unroll, place_all, tuple(jnp.zeros((8, LANES), F32) for _ in range(4))
    )
    for h in range(4):
        word = table_s[chunks - 1, h]
        tiles[h, ((word & 1023) + (word >> 18)) >> 7] = carry[h]
    for h, out in enumerate((out0, out1, out2, out3)):
        for t in range(out.shape[1] // LANES):
            out[:, t * LANES : (t + 1) * LANES] = tiles[h, t]


def source_rows(rows):
    kept, temp = rows[0:1], rows[4:5]
    v0, v1, v2 = rows[1:2], rows[2:3], rows[3:4]
    share = sigmoid_of(temp)
    gone = kept * share / (1.0 - SHRINK * share)
    heat = temp + 0.5 * (v0 * v0 + v1 * v1 + v2 * v2)
    fields = [gone, gone * v0, gone * v1, gone * v2, gone * heat]
    high = [f.astype(BF16).astype(F32) for f in fields]
    low = [f - g for f, g in zip(fields, high)]
    return high + low


def spread(columns, sources, number):
    n = columns.shape[1]
    hot = jnp.where(columns == iota((number, n), 0).astype(F32), 1.0, 0.0).astype(BF16)
    hot = hot.reshape(number // 16, 16, n)
    parts = []
    for source in sources:
        value = jnp.broadcast_to(source, (16, n)).astype(BF16)
        parts.append((hot * value[None]).reshape(number, n))
    return jnp.concatenate(parts, axis=0)


def depth_onehot(rows, depth):
    n = rows.shape[1]
    return jnp.where(rows[7:8] == iota((depth, n), 0).astype(F32), 1.0, 0.0).astype(BF16)


def deposit_kernel(cells_x, cells_y, step, stay, state, where_to, dep, acc):
    total = stay.shape[1]
    columns = cells_x * cells_y
    depth = dep.shape[2]
    anchor_x = (lax.axis_index("gx") * cells_x).astype(F32)
    anchor_y = (lax.axis_index("gy") * cells_y).astype(F32)
    acc[...] = jnp.zeros(acc.shape, F32)

    def one(k, carry):
        rows = stay[:, pl.ds(pl.multiple_of(k * step, step), step)]
        column = (rows[5:6] - anchor_x) * cells_y + (rows[6:7] - anchor_y)
        left = spread(column, source_rows(rows), columns)
        acc[...] += lax.dot_general(
            left, depth_onehot(rows, depth), TRANSPOSED, preferred_element_type=F32
        )
        return carry

    lax.fori_loop(0, total // step, one, 0)
    for f in range(5):
        dep[f] = (
            acc[f * columns : (f + 1) * columns, :] + acc[(5 + f) * columns : (6 + f) * columns, :]
        )
    state[:, :total] = stay[0:5, :]
    where_to[:, :total] = stay[5:8, :].astype(I32)


def arrive_kernel(
    cells_x, cells_y, in0, in1, in2, in3, energy, dep4, state_in, where_in,
    planes, face_x0, face_x1, face_y0, face_y1, state, where_to,
):
    depth = planes.shape[3]
    anchor_x = (lax.axis_index("gx") * cells_x).astype(F32)
    anchor_y = (lax.axis_index("gy") * cells_y).astype(F32)
    capacity = in0.shape[1]
    for q, table in enumerate((in0, in1, in2, in3)):
        rows = table[...]
        along = (rows[6:7] - anchor_y) if q < 2 else (rows[5:6] - anchor_x)
        number = cells_y if q < 2 else cells_x
        left = spread(along, source_rows(rows), number)
        got = lax.dot_general(left, depth_onehot(rows, depth), TRANSPOSED, preferred_element_type=F32)
        for f in range(5):
            planes[q, f] = (
                got[f * number : (f + 1) * number] + got[(5 + f) * number : (6 + f) * number]
            )
        lanes = slice(q * capacity, (q + 1) * capacity)
        state[:, lanes] = rows[0:5]
        where_to[:, lanes] = rows[5:8].astype(I32)
    scale = ADIABATIC_INDEX - 1.0
    row = iota((cells_y, depth), 0)
    for q, face, x in ((0, face_x0, 0), (1, face_x1, cells_x - 1)):
        plane = energy[x] + dep4[x] + planes[q, 4]
        plane = plane + jnp.where(row == 0, planes[2, 4, x : x + 1, :], 0.0)
        plane = plane + jnp.where(row == cells_y - 1, planes[3, 4, x : x + 1, :], 0.0)
        face[...] = scale * plane
    row = iota((cells_x, depth), 0)
    for q, face, y in ((2, face_y0, 0), (3, face_y1, cells_y - 1)):
        plane = energy[:, y, :] + dep4[:, y, :] + planes[q, 4]
        plane = plane + jnp.where(row == 0, planes[0, 4, y : y + 1, :], 0.0)
        plane = plane + jnp.where(row == cells_x - 1, planes[1, 4, y : y + 1, :], 0.0)
        face[...] = scale * plane


def update_kernel(
    cells_x, cells_y, density, momentum, energy, dep, planes, halo_x0, halo_x1, halo_y0, halo_y1,
    rho_out, impulse, energy_out, fastest, pressure,
):
    depth = energy.shape[2]
    scale = ADIABATIC_INDEX - 1.0
    shape = (cells_y, depth)
    row = iota(shape, 0)
    lane = iota(shape, 1)

    def with_planes(f, x, value):
        if x == 0:
            value = value + planes[0, f]
        if x == cells_x - 1:
            value = value + planes[1, f]
        value = value + jnp.where(row == 0, planes[2, f, x : x + 1, :], 0.0)
        return value + jnp.where(row == cells_y - 1, planes[3, f, x : x + 1, :], 0.0)

    pressure[0] = halo_x0[...]
    pressure[cells_x + 1] = halo_x1[...]
    for x in range(cells_x):
        value = with_planes(4, x, energy[x] + dep[4, x])
        energy_out[x] = value
        pressure[x + 1] = scale * value
    top = jnp.zeros(shape, F32)
    for x in range(cells_x):
        here = pressure[x + 1]
        grad_x = 0.5 * (pressure[x + 2] - pressure[x])
        after = jnp.where(row == cells_y - 1, halo_y1[x : x + 1, :], pltpu.roll(here, cells_y - 1, 0))
        before = jnp.where(row == 0, halo_y0[x : x + 1, :], pltpu.roll(here, 1, 0))
        grad_y = 0.5 * (after - before)
        after = jnp.where(lane == depth - 1, 0.0, pltpu.roll(here, depth - 1, 1))
        before = jnp.where(lane == 0, 0.0, pltpu.roll(here, 1, 1))
        grad_z = 0.5 * (after - before)
        rho = with_planes(0, x, density[x] + dep[0, x])
        rho_out[x] = rho
        largest = jnp.zeros(shape, F32)
        for k, grad in enumerate((grad_x, grad_y, grad_z)):
            value = with_planes(1 + k, x, momentum[k, x] + dep[1 + k, x]) - KICK * grad
            impulse[k, x] = value
            largest = jnp.maximum(largest, jnp.abs(value))
        wave = largest / rho + jnp.sqrt(ADIABATIC_INDEX * here / rho)
        top = jnp.maximum(top, wave)
    fastest[...] = jnp.max(top, axis=(0, 1), keepdims=True)


def call(kernel, outs, scratch=(), out_specs=None, in_specs=None, aliases=None, name=None, **extra):
    if in_specs is not None:
        extra["in_specs"] = in_specs
    if out_specs is not None:
        extra["out_specs"] = out_specs
    return pl.pallas_call(
        kernel,
        out_shape=outs,
        scratch_shapes=list(scratch),
        input_output_aliases=aliases or {},
        compiler_params=pltpu.CompilerParams(vmem_limit_bytes=48 * 1024 * 1024),
        name=name,
        **extra,
    )


def on_device(
    density, momentum, energy, parcel_mass, droplet_velocity, parcel_temp, parcel_cell, parcel_count
):
    cells_x, cells_y, depth = density.shape
    rows = parcel_mass.shape[0]
    capacity = rows // 16
    chunks = rows // LANES
    sds = jax.ShapeDtypeStruct
    whole = pl.BlockSpec(memory_space=VMEM)
    bucket = sds((8, capacity), F32)
    *buckets, stay = call(
        functools.partial(prep_kernel, cells_x, cells_y),
        (bucket, bucket, bucket, bucket, sds((8, rows), F32)),
        scratch=(
            VMEM((8, rows), F32),
            VMEM((chunks, LANES), I32),
            VMEM((chunks, LANES), I32),
            VMEM((chunks, LANES), F32),
            VMEM((chunks, 8, LANES), F32),
            VMEM((chunks, LANES), I32),
            pltpu.SMEM((chunks, LANES), I32),
            VMEM((4, capacity // LANES + 1, 8, LANES), F32),
            pltpu.SemaphoreType.DMA,
        ),
        in_specs=[pl.BlockSpec(memory_space=pltpu.SMEM)] + [whole] * 4,
        name="prep",
    )(
        parcel_count,
        parcel_mass.reshape(chunks, LANES),
        parcel_temp.reshape(chunks, LANES),
        droplet_velocity,
        parcel_cell,
    )

    def exchange(to_low_x, to_high_x, to_low_y, to_high_y):
        got = []
        for axis, down, up in (("gx", to_low_x, to_high_x), ("gy", to_low_y, to_high_y)):
            ends = lax.axis_size(axis) - 1
            got.append(lax.ppermute(up, axis, [(i, i + 1) for i in range(ends)]))
            got.append(lax.ppermute(down, axis, [(i + 1, i) for i in range(ends)]))
        return got

    arrived = exchange(*buckets)
    slots = rows + 4 * capacity
    state, where_to, dep = call(
        functools.partial(deposit_kernel, cells_x, cells_y, min(1024, rows)),
        (sds((5, slots), F32), sds((3, slots), I32), sds((5, cells_x * cells_y, depth), F32)),
        scratch=(VMEM((10 * cells_x * cells_y, depth), F32),),
        name="deposit",
    )(stay)
    dep = dep.reshape(5, cells_x, cells_y, depth)
    face = lambda n: sds((n, depth), F32)
    planes, *faces, state, where_to = call(
        functools.partial(arrive_kernel, cells_x, cells_y),
        (
            sds((4, 5, cells_x, depth), F32),
            face(cells_y), face(cells_y), face(cells_x), face(cells_x),
            sds(state.shape, F32),
            sds(where_to.shape, I32),
        ),
        in_specs=[whole] * 5
        + [pl.BlockSpec((None, cells_x, cells_y, depth), lambda i: (4, 0, 0, 0))]
        + [pl.BlockSpec(memory_space=pl.ANY)] * 2,
        out_specs=(whole,) * 5
        + (
            pl.BlockSpec((5, 4 * capacity), lambda i: (0, rows // (4 * capacity))),
            pl.BlockSpec((3, 4 * capacity), lambda i: (0, rows // (4 * capacity))),
        ),
        aliases={6: 5, 7: 6},
        name="arrive",
        grid=(1,),
    )(*arrived, energy, dep, state, where_to)
    halos = exchange(*faces)
    rho, impulse, energy_out, top = call(
        functools.partial(update_kernel, cells_x, cells_y),
        (
            sds(density.shape, F32),
            sds(momentum.shape, F32),
            sds(energy.shape, F32),
            sds((1, 1), F32),
        ),
        scratch=(VMEM((cells_x + 2, cells_y, depth), F32),),
        name="update",
    )(density, momentum, energy, dep, planes, *halos)
    fastest = lax.pmax(top[0, 0], ("gx", "gy"))
    return rho, impulse, energy_out, state, where_to, COURANT / fastest


def solution(mesh):
    both = ("gx", "gy")
    return jax.shard_map(
        on_device,
        mesh=mesh,
        in_specs=(
            P("gx", "gy", None),
            P(None, "gx", "gy", None),
            P("gx", "gy", None),
            P(both),
            P(None, both),
            P(both),
            P(None, both),
            P(both),
        ),
        out_specs=(
            P("gx", "gy", None),
            P(None, "gx", "gy", None),
            P("gx", "gy", None),
            P(None, both),
            P(None, both),
            P(),
        ),
        check_vma=False,
    )
```

```python
import functools

import jax
import jax.numpy as jnp
from jax import lax
from jax.experimental import pallas as pl
from jax.experimental.pallas import tpu as pltpu
from jax.sharding import PartitionSpec as P

ADIABATIC_INDEX = 1.4
KICK = 0.25
COURANT = 0.4
SHRINK = 0.5

F32 = jnp.float32
BF16 = jnp.bfloat16
I32 = jnp.int32
LANES = 128
VMEM = pltpu.VMEM
TRANSPOSED = (((1,), (1,)), ((), ()))


def iota(shape, dim, dtype=I32):
    return lax.broadcasted_iota(dtype, shape, dim)


def sigmoid_of(temp):
    return 1.0 / (1.0 + jnp.exp(-2.0 * (temp - 2.0)))


def prep_kernel(
    cells_x, cells_y, count, mass, temp, vel, cell,
    out0, out1, out2, out3, stay,
    mass_v, temp_v, vel_v, cell_v, pay, cx, cy, pos, compact, table_v, table_s, tiles, sems,
):
    fetches = [
        pltpu.make_async_copy(there, here, sems.at[i])
        for i, (there, here) in enumerate(
            ((cell, cell_v), (temp, temp_v), (mass, mass_v), (vel, vel_v))
        )
    ]
    for fetch in fetches:
        fetch.start()
    mass, temp, vel, cell = mass_v, temp_v, vel_v, cell_v
    fetches[0].wait()
    chunks = mass.shape[0]
    anchor_x = lax.axis_index("gx") * cells_x
    anchor_y = lax.axis_index("gy") * cells_y
    for b in range(chunks):
        lanes = slice(b * LANES, (b + 1) * LANES)
        cx[b : b + 1, :] = cell[0:1, lanes]
        cy[b : b + 1, :] = cell[1:2, lanes]
    shape = (chunks, LANES)
    live = iota(shape, 0) * LANES + iota(shape, 1) < count[0]
    fetches[1].wait()
    fetches[2].wait()
    kept = mass[...] * (1.0 - SHRINK * jnp.where(live, sigmoid_of(temp[...]), 0.0))
    local_x = cx[...] - anchor_x
    local_y = cy[...] - anchor_y
    heading = jnp.where(
        local_x < 0,
        0,
        jnp.where(
            local_x >= cells_x, 1, jnp.where(local_y < 0, 2, jnp.where(local_y >= cells_y, 3, 4))
        ),
    )
    heading = jnp.where(live, heading, 5)
    masks = [jnp.where(heading == h, 1.0, 0.0) for h in range(4)]
    lane_r = iota((LANES, 2 * LANES), 0)
    lane_c = iota((LANES, 2 * LANES), 1)
    scan = jnp.where((lane_r < lane_c) | (lane_c >= LANES), 1.0, 0.0).astype(BF16)
    both = jnp.dot(
        jnp.concatenate(masks, axis=0).astype(BF16), scan, preferred_element_type=F32
    )
    inner = [both[h * chunks : (h + 1) * chunks, :LANES] for h in range(4)]
    total = [both[h * chunks : (h + 1) * chunks, LANES:] for h in range(4)]
    below = jnp.where(iota((chunks, chunks), 1) < iota((chunks, chunks), 0), 1.0, 0.0).astype(BF16)
    base = jnp.dot(
        below, jnp.concatenate(total, axis=1).astype(BF16), preferred_element_type=F32
    )
    lane = iota(shape, 1)
    offset = jnp.zeros(shape, F32)
    place = jnp.full(shape, -1.0, F32)
    words = jnp.zeros(shape, I32)
    for h in range(4):
        place = jnp.where(heading == h, inner[h] + offset, place)
        base_h = base[:, h * LANES : (h + 1) * LANES]
        word = base_h.astype(I32) + offset.astype(I32) * 1024 + total[h].astype(I32) * (1024 * 256)
        words = jnp.where(lane == h, word, words)
        offset = offset + total[h]
    table_v[...] = words
    load = pltpu.make_async_copy(table_v, table_s, sems.at[4])
    load.start()
    pos[...] = place
    fetches[3].wait()
    pay[1:4, :] = vel[...]
    pay[5:8, :] = cell[...].astype(F32)
    stays = jnp.where(heading == 4, 1.0, 0.0)
    for b in range(chunks):
        lanes = slice(b * LANES, (b + 1) * LANES)
        pay[0:1, lanes] = kept[b : b + 1, :]
        pay[4:5, lanes] = temp[b : b + 1, :]
    for b in range(chunks):
        lanes = slice(b * LANES, (b + 1) * LANES)
        stay[:, lanes] = jnp.where(stays[b : b + 1, :] > 0.0, pay[:, lanes], 0.0)
    group = 16

    def pack(g, carry):
        for u in range(group):
            b = g * group + u
            slots = pos[pl.ds(b, 1), :]
            onehot = jnp.where(slots == iota((LANES, LANES), 0).astype(F32), 1.0, 0.0).astype(BF16)
            rows = pay[:, pl.ds(pl.multiple_of(b * LANES, LANES), LANES)]
            high = rows.astype(BF16).astype(F32)
            rest = rows - high
            middle = rest.astype(BF16).astype(F32)
            low = rest - middle
            parts = jnp.concatenate([high, middle, low, jnp.zeros_like(low)], axis=0).astype(BF16)
            got = lax.dot_general(parts, onehot, TRANSPOSED, preferred_element_type=F32)
            compact[b] = got[0:8] + got[8:16] + got[16:24]
        return carry

    lax.fori_loop(0, chunks // group, pack, 0)
    tiles[...] = jnp.zeros(tiles.shape, F32)
    load.wait()
    lane8 = iota((8, LANES), 1)
    unroll = 8

    def place_all(g, carry):
        carry = list(carry)
        for u in range(unroll):
            b = g * unroll + u
            rows = compact[b]
            for h in range(4):
                word = table_s[b, h]
                start = word & 1023
                first = (word >> 10) & 255
                number = word >> 18
                within = start & (LANES - 1)
                end = within + number
                turned = pltpu.roll(rows, (start - first) & (LANES - 1), 1)
                merged = jnp.where((lane8 >= within) & (lane8 < end), turned, carry[h])
                tiles[h, start >> 7] = merged
                over = jnp.where(lane8 < end - LANES, turned, 0.0)
                carry[h] = jnp.where(end >= LANES, over, merged)
        return tuple(carry)

    carry = lax.fori_loop(
        0, chunks // unroll, place_all, tuple(jnp.zeros((8, LANES), F32) for _ in range(4))
    )
    for h in range(4):
        word = table_s[chunks - 1, h]
        tiles[h, ((word & 1023) + (word >> 18)) >> 7] = carry[h]
    for h, out in enumerate((out0, out1, out2, out3)):
        for t in range(out.shape[1] // LANES):
            out[:, t * LANES : (t + 1) * LANES] = tiles[h, t]


def source_rows(rows):
    kept, temp = rows[0:1], rows[4:5]
    v0, v1, v2 = rows[1:2], rows[2:3], rows[3:4]
    share = sigmoid_of(temp)
    gone = kept * share / (1.0 - SHRINK * share)
    heat = temp + 0.5 * (v0 * v0 + v1 * v1 + v2 * v2)
    fields = [gone, gone * v0, gone * v1, gone * v2, gone * heat]
    high = [f.astype(BF16).astype(F32) for f in fields]
    low = [f - g for f, g in zip(fields, high)]
    return high + low


def spread(columns, sources, number):
    n = columns.shape[1]
    hot = jnp.where(columns == iota((number, n), 0).astype(F32), 1.0, 0.0).astype(BF16)
    hot = hot.reshape(number // 16, 16, n)
    parts = []
    for source in sources:
        value = jnp.broadcast_to(source, (16, n)).astype(BF16)
        parts.append((hot * value[None]).reshape(number, n))
    return jnp.concatenate(parts, axis=0)


def depth_onehot(rows, depth):
    n = rows.shape[1]
    return jnp.where(rows[7:8] == iota((depth, n), 0).astype(F32), 1.0, 0.0).astype(BF16)


def deposit_kernel(cells_x, cells_y, step, stay, state, where_to, dep, acc):
    total = stay.shape[1]
    columns = cells_x * cells_y
    depth = dep.shape[2]
    anchor_x = (lax.axis_index("gx") * cells_x).astype(F32)
    anchor_y = (lax.axis_index("gy") * cells_y).astype(F32)
    acc[...] = jnp.zeros(acc.shape, F32)

    def one(k, carry):
        rows = stay[:, pl.ds(pl.multiple_of(k * step, step), step)]
        column = (rows[5:6] - anchor_x) * cells_y + (rows[6:7] - anchor_y)
        left = spread(column, source_rows(rows), columns)
        acc[...] += lax.dot_general(
            left, depth_onehot(rows, depth), TRANSPOSED, preferred_element_type=F32
        )
        return carry

    lax.fori_loop(0, total // step, one, 0)
    for f in range(5):
        dep[f] = (
            acc[f * columns : (f + 1) * columns, :] + acc[(5 + f) * columns : (6 + f) * columns, :]
        )
    state[:, :total] = stay[0:5, :]
    where_to[:, :total] = stay[5:8, :].astype(I32)


def arrive_kernel(
    cells_x, cells_y, in0, in1, in2, in3, energy, dep4, state_in, where_in,
    planes, face_x0, face_x1, face_y0, face_y1, state, where_to,
):
    depth = planes.shape[3]
    anchor_x = (lax.axis_index("gx") * cells_x).astype(F32)
    anchor_y = (lax.axis_index("gy") * cells_y).astype(F32)
    capacity = in0.shape[1]
    for q, table in enumerate((in0, in1, in2, in3)):
        rows = table[...]
        along = (rows[6:7] - anchor_y) if q < 2 else (rows[5:6] - anchor_x)
        number = cells_y if q < 2 else cells_x
        left = spread(along, source_rows(rows), number)
        got = lax.dot_general(left, depth_onehot(rows, depth), TRANSPOSED, preferred_element_type=F32)
        for f in range(5):
            planes[q, f] = (
                got[f * number : (f + 1) * number] + got[(5 + f) * number : (6 + f) * number]
            )
        lanes = slice(q * capacity, (q + 1) * capacity)
        state[:, lanes] = rows[0:5]
        where_to[:, lanes] = rows[5:8].astype(I32)
    scale = ADIABATIC_INDEX - 1.0
    row = iota((cells_y, depth), 0)
    for q, face, x in ((0, face_x0, 0), (1, face_x1, cells_x - 1)):
        plane = energy[x] + dep4[x] + planes[q, 4]
        plane = plane + jnp.where(row == 0, planes[2, 4, x : x + 1, :], 0.0)
        plane = plane + jnp.where(row == cells_y - 1, planes[3, 4, x : x + 1, :], 0.0)
        face[...] = scale * plane
    row = iota((cells_x, depth), 0)
    for q, face, y in ((2, face_y0, 0), (3, face_y1, cells_y - 1)):
        plane = energy[:, y, :] + dep4[:, y, :] + planes[q, 4]
        plane = plane + jnp.where(row == 0, planes[0, 4, y : y + 1, :], 0.0)
        plane = plane + jnp.where(row == cells_x - 1, planes[1, 4, y : y + 1, :], 0.0)
        face[...] = scale * plane


def update_kernel(
    cells_x, cells_y, density, momentum, energy, dep, planes, halo_x0, halo_x1, halo_y0, halo_y1,
    rho_out, impulse, energy_out, fastest, pressure,
):
    depth = energy.shape[2]
    scale = ADIABATIC_INDEX - 1.0
    shape = (cells_y, depth)
    row = iota(shape, 0)
    lane = iota(shape, 1)

    def with_planes(f, x, value):
        if x == 0:
            value = value + planes[0, f]
        if x == cells_x - 1:
            value = value + planes[1, f]
        value = value + jnp.where(row == 0, planes[2, f, x : x + 1, :], 0.0)
        return value + jnp.where(row == cells_y - 1, planes[3, f, x : x + 1, :], 0.0)

    pressure[0] = halo_x0[...]
    pressure[cells_x + 1] = halo_x1[...]
    for x in range(cells_x):
        value = with_planes(4, x, energy[x] + dep[4, x])
        energy_out[x] = value
        pressure[x + 1] = scale * value
    top = jnp.zeros(shape, F32)
    for x in range(cells_x):
        here = pressure[x + 1]
        grad_x = 0.5 * (pressure[x + 2] - pressure[x])
        after = jnp.where(row == cells_y - 1, halo_y1[x : x + 1, :], pltpu.roll(here, cells_y - 1, 0))
        before = jnp.where(row == 0, halo_y0[x : x + 1, :], pltpu.roll(here, 1, 0))
        grad_y = 0.5 * (after - before)
        after = jnp.where(lane == depth - 1, 0.0, pltpu.roll(here, depth - 1, 1))
        before = jnp.where(lane == 0, 0.0, pltpu.roll(here, 1, 1))
        grad_z = 0.5 * (after - before)
        rho = with_planes(0, x, density[x] + dep[0, x])
        rho_out[x] = rho
        largest = jnp.zeros(shape, F32)
        for k, grad in enumerate((grad_x, grad_y, grad_z)):
            value = with_planes(1 + k, x, momentum[k, x] + dep[1 + k, x]) - KICK * grad
            impulse[k, x] = value
            largest = jnp.maximum(largest, jnp.abs(value))
        wave = largest / rho + jnp.sqrt(ADIABATIC_INDEX * here / rho)
        top = jnp.maximum(top, wave)
    fastest[...] = jnp.broadcast_to(jnp.max(top, axis=(0, 1), keepdims=True), fastest.shape)


def call(kernel, outs, scratch=(), out_specs=None, in_specs=None, aliases=None, name=None, **extra):
    if in_specs is not None:
        extra["in_specs"] = in_specs
    if out_specs is not None:
        extra["out_specs"] = out_specs
    return pl.pallas_call(
        kernel,
        out_shape=outs,
        scratch_shapes=list(scratch),
        input_output_aliases=aliases or {},
        compiler_params=pltpu.CompilerParams(vmem_limit_bytes=48 * 1024 * 1024),
        name=name,
        **extra,
    )


def on_device(
    density, momentum, energy, parcel_mass, droplet_velocity, parcel_temp, parcel_cell, parcel_count
):
    cells_x, cells_y, depth = density.shape
    rows = parcel_mass.shape[0]
    capacity = rows // 16
    chunks = rows // LANES
    sds = jax.ShapeDtypeStruct
    whole = pl.BlockSpec(memory_space=VMEM)
    bucket = sds((8, capacity), F32)
    *buckets, stay = call(
        functools.partial(prep_kernel, cells_x, cells_y),
        (bucket, bucket, bucket, bucket, sds((8, rows), F32)),
        scratch=(
            VMEM((chunks, LANES), F32),
            VMEM((chunks, LANES), F32),
            VMEM((3, rows), F32),
            VMEM((3, rows), I32),
            VMEM((8, rows), F32),
            VMEM((chunks, LANES), I32),
            VMEM((chunks, LANES), I32),
            VMEM((chunks, LANES), F32),
            VMEM((chunks, 8, LANES), F32),
            VMEM((chunks, LANES), I32),
            pltpu.SMEM((chunks, LANES), I32),
            VMEM((4, capacity // LANES + 1, 8, LANES), F32),
            pltpu.SemaphoreType.DMA((5,)),
        ),
        in_specs=[pl.BlockSpec(memory_space=pltpu.SMEM)] + [pl.BlockSpec(memory_space=pltpu.HBM)] * 4,
        name="prep",
    )(
        parcel_count,
        parcel_mass.reshape(chunks, LANES),
        parcel_temp.reshape(chunks, LANES),
        droplet_velocity,
        parcel_cell,
    )

    def exchange(to_low_x, to_high_x, to_low_y, to_high_y):
        got = []
        for axis, down, up in (("gx", to_low_x, to_high_x), ("gy", to_low_y, to_high_y)):
            ends = lax.axis_size(axis) - 1
            got.append(lax.ppermute(up, axis, [(i, i + 1) for i in range(ends)]))
            got.append(lax.ppermute(down, axis, [(i + 1, i) for i in range(ends)]))
        return got

    arrived = exchange(*buckets)
    slots = rows + 4 * capacity
    state, where_to, dep = call(
        functools.partial(deposit_kernel, cells_x, cells_y, min(1024, rows)),
        (sds((5, slots), F32), sds((3, slots), I32), sds((5, cells_x * cells_y, depth), F32)),
        scratch=(VMEM((10 * cells_x * cells_y, depth), F32),),
        name="deposit",
    )(stay)
    dep = dep.reshape(5, cells_x, cells_y, depth)
    face = lambda n: sds((n, depth), F32)
    planes, *faces, state, where_to = call(
        functools.partial(arrive_kernel, cells_x, cells_y),
        (
            sds((4, 5, cells_x, depth), F32),
            face(cells_y), face(cells_y), face(cells_x), face(cells_x),
            sds(state.shape, F32),
            sds(where_to.shape, I32),
        ),
        in_specs=[whole] * 5
        + [pl.BlockSpec((None, cells_x, cells_y, depth), lambda i: (4, 0, 0, 0))]
        + [pl.BlockSpec(memory_space=pl.ANY)] * 2,
        out_specs=(whole,) * 5
        + (
            pl.BlockSpec((5, 4 * capacity), lambda i: (0, rows // (4 * capacity))),
            pl.BlockSpec((3, 4 * capacity), lambda i: (0, rows // (4 * capacity))),
        ),
        aliases={6: 5, 7: 6},
        name="arrive",
        grid=(1,),
    )(*arrived, energy, dep, state, where_to)
    halos = exchange(*faces)
    rho, impulse, energy_out, top = call(
        functools.partial(update_kernel, cells_x, cells_y),
        (
            sds(density.shape, F32),
            sds(momentum.shape, F32),
            sds(energy.shape, F32),
            sds((lax.axis_size(("gx", "gy")), LANES), F32),
        ),
        scratch=(VMEM((cells_x + 2, cells_y, depth), F32),),
        name="update",
    )(density, momentum, energy, dep, planes, *halos)
    fastest = jnp.max(lax.all_to_all(top, ("gx", "gy"), 0, 0, tiled=True))
    return rho, impulse, energy_out, state, where_to, COURANT / fastest


def solution(mesh):
    both = ("gx", "gy")
    return jax.shard_map(
        on_device,
        mesh=mesh,
        in_specs=(
            P("gx", "gy", None),
            P(None, "gx", "gy", None),
            P("gx", "gy", None),
            P(both),
            P(None, both),
            P(both),
            P(None, both),
            P(both),
        ),
        out_specs=(
            P("gx", "gy", None),
            P(None, "gx", "gy", None),
            P("gx", "gy", None),
            P(None, both),
            P(None, both),
            P(),
        ),
        check_vma=False,
    )
```

```python
import functools

import jax
import jax.numpy as jnp
from jax import lax
from jax.experimental import pallas as pl
from jax.experimental.pallas import tpu as pltpu
from jax.sharding import PartitionSpec as P

ADIABATIC_INDEX = 1.4
KICK = 0.25
COURANT = 0.4
SHRINK = 0.5

F32 = jnp.float32
BF16 = jnp.bfloat16
I32 = jnp.int32
LANES = 128
VMEM = pltpu.VMEM
TRANSPOSED = (((1,), (1,)), ((), ()))


def iota(shape, dim, dtype=I32):
    return lax.broadcasted_iota(dtype, shape, dim)


def sigmoid_of(temp):
    return 1.0 / (1.0 + jnp.exp(-2.0 * (temp - 2.0)))


def prep_kernel(
    cells_x, cells_y, step, count, mass, temp, vel, cell, energy,
    even, odd, stay, own, leaving, partial,
    mass_v, temp_v, vel_v, cell_v, pay, cx, cy, pos, compact, table_v, table_s, tiles, acc, sems,
):
    fetches = [
        pltpu.make_async_copy(there, here, sems.at[i])
        for i, (there, here) in enumerate(
            ((cell, cell_v), (temp, temp_v), (mass, mass_v), (vel, vel_v))
        )
    ]
    for fetch in fetches:
        fetch.start()
    mass, temp, vel, cell = mass_v, temp_v, vel_v, cell_v
    fetches[0].wait()
    chunks = mass.shape[0]
    anchor_x = lax.axis_index("gx") * cells_x
    anchor_y = lax.axis_index("gy") * cells_y
    anchor_xf, anchor_yf = anchors(cells_x, cells_y)
    for b in range(chunks):
        lanes = slice(b * LANES, (b + 1) * LANES)
        cx[b : b + 1, :] = cell[0:1, lanes]
        cy[b : b + 1, :] = cell[1:2, lanes]
    shape = (chunks, LANES)
    live = iota(shape, 0) * LANES + iota(shape, 1) < count[0]
    fetches[1].wait()
    fetches[2].wait()
    kept = mass[...] * (1.0 - SHRINK * jnp.where(live, sigmoid_of(temp[...]), 0.0))
    local_x = cx[...] - anchor_x
    local_y = cy[...] - anchor_y
    heading = jnp.where(
        local_x < 0,
        0,
        jnp.where(
            local_x >= cells_x, 1, jnp.where(local_y < 0, 2, jnp.where(local_y >= cells_y, 3, 4))
        ),
    )
    heading = jnp.where(live, heading, 5)
    masks = [jnp.where(heading == h, 1.0, 0.0) for h in range(4)]
    lane_r = iota((LANES, 2 * LANES), 0)
    lane_c = iota((LANES, 2 * LANES), 1)
    scan = jnp.where((lane_r < lane_c) | (lane_c >= LANES), 1.0, 0.0).astype(BF16)
    both = jnp.dot(
        jnp.concatenate(masks, axis=0).astype(BF16), scan, preferred_element_type=F32
    )
    inner = [both[h * chunks : (h + 1) * chunks, :LANES] for h in range(4)]
    total = [both[h * chunks : (h + 1) * chunks, LANES:] for h in range(4)]
    below = jnp.where(iota((chunks, chunks), 1) < iota((chunks, chunks), 0), 1.0, 0.0).astype(BF16)
    base = jnp.dot(
        below, jnp.concatenate(total, axis=1).astype(BF16), preferred_element_type=F32
    )
    lane = iota(shape, 1)
    offset = jnp.zeros(shape, F32)
    place = jnp.full(shape, -1.0, F32)
    words = jnp.zeros(shape, I32)
    for h in range(4):
        place = jnp.where(heading == h, inner[h] + offset, place)
        base_h = base[:, h * LANES : (h + 1) * LANES]
        word = base_h.astype(I32) + offset.astype(I32) * 1024 + total[h].astype(I32) * (1024 * 256)
        words = jnp.where(lane == h, word, words)
        offset = offset + total[h]
    table_v[...] = words
    load = pltpu.make_async_copy(table_v, table_s, sems.at[4])
    load.start()
    pos[...] = place
    fetches[3].wait()
    pay[1:4, :] = vel[...]
    pay[5:8, :] = cell[...].astype(F32)
    stays = jnp.where(heading == 4, 1.0, 0.0)
    for b in range(chunks):
        lanes = slice(b * LANES, (b + 1) * LANES)
        pay[0:1, lanes] = kept[b : b + 1, :]
        pay[4:5, lanes] = temp[b : b + 1, :]
    for b in range(chunks):
        lanes = slice(b * LANES, (b + 1) * LANES)
        stay[:, lanes] = jnp.where(stays[b : b + 1, :] > 0.0, pay[:, lanes], 0.0)
    group = 16

    def pack(g, carry):
        for u in range(group):
            b = g * group + u
            slots = pos[pl.ds(b, 1), :]
            onehot = jnp.where(slots == iota((LANES, LANES), 0).astype(F32), 1.0, 0.0).astype(BF16)
            rows = pay[:, pl.ds(pl.multiple_of(b * LANES, LANES), LANES)]
            high = rows.astype(BF16).astype(F32)
            rest = rows - high
            middle = rest.astype(BF16).astype(F32)
            low = rest - middle
            parts = jnp.concatenate([high, middle, low, jnp.zeros_like(low)], axis=0).astype(BF16)
            got = lax.dot_general(parts, onehot, TRANSPOSED, preferred_element_type=F32)
            compact[b] = got[0:8] + got[8:16] + got[16:24]
        return carry

    lax.fori_loop(0, chunks // group, pack, 0)
    tiles[...] = jnp.zeros(tiles.shape, F32)
    load.wait()
    lane8 = iota((8, LANES), 1)
    unroll = 8

    def place_all(g, carry):
        carry = list(carry)
        for u in range(unroll):
            b = g * unroll + u
            rows = compact[b]
            for h in range(4):
                word = table_s[b, h]
                start = word & 1023
                first = (word >> 10) & 255
                number = word >> 18
                within = start & (LANES - 1)
                end = within + number
                turned = pltpu.roll(rows, (start - first) & (LANES - 1), 1)
                merged = jnp.where((lane8 >= within) & (lane8 < end), turned, carry[h])
                tiles[h, start >> 7] = merged
                over = jnp.where(lane8 < end - LANES, turned, 0.0)
                carry[h] = jnp.where(end >= LANES, over, merged)
        return tuple(carry)

    carry = lax.fori_loop(
        0, chunks // unroll, place_all, tuple(jnp.zeros((8, LANES), F32) for _ in range(4))
    )
    for h in range(4):
        word = table_s[chunks - 1, h]
        tiles[h, ((word & 1023) + (word >> 18)) >> 7] = carry[h]
    width = 4 * LANES
    buckets = [
        jnp.concatenate([tiles[h, t] for t in range(width // LANES)], axis=1) for h in range(4)
    ]
    for h in range(4):
        along = (buckets[h][6:7] - anchor_yf) if h < 2 else (buckets[h][5:6] - anchor_xf)
        number = cells_y if h < 2 else cells_x
        leaving[h] = one_field(buckets[h], along, number, 4)
    for h in range(2):
        own[h] = buckets[h]
    columns = cells_x * cells_y
    deposit_fields((4,), anchor_xf, anchor_yf, cells_y, step, stay, acc)
    for x in range(cells_x):
        rows = slice(x * cells_y, (x + 1) * cells_y)
        partial[x] = energy[x] + (acc[rows] + acc[columns + x * cells_y : columns + (x + 1) * cells_y])
    up = message(buckets[3], partial[:, cells_y - 1, :], leaving[0, -1:, :], leaving[1, -1:, :])
    down = message(buckets[2], partial[:, 0, :], leaving[0, 0:1, :], leaving[1, 0:1, :])
    send_pair("gy", even, odd, up, down)


def message(bucket, plane, first, second):
    half = plane.shape[0] // 2
    rest = jnp.zeros((6, plane.shape[1]), F32)
    return jnp.concatenate(
        [bucket, plane[:half], plane[half:], jnp.concatenate([first, second, rest], axis=0)], axis=1
    )


def unpack(got, depth):
    width = got.shape[1] - 3 * depth
    plane = jnp.concatenate(
        [got[:, width : width + depth], got[:, width + depth : width + 2 * depth]], axis=0
    )
    corner = got[:, width + 2 * depth :]
    return got[:, :width], plane, corner[0:1], corner[1:2]


def send_pair(axis, even, odd, up, down):
    is_even = (lax.axis_index(axis) & 1) == 0
    even[...] = jnp.where(is_even, up, down)
    odd[...] = jnp.where(is_even, down, up)


def receive_pair(axis, even, odd):
    is_even = (lax.axis_index(axis) & 1) == 0
    return jnp.where(is_even, odd[...], even[...]), jnp.where(is_even, even[...], odd[...])


def anchors(cells_x, cells_y):
    return (
        (lax.axis_index("gx") * cells_x).astype(F32),
        (lax.axis_index("gy") * cells_y).astype(F32),
    )


def source_rows(rows):
    kept, temp = rows[0:1], rows[4:5]
    v0, v1, v2 = rows[1:2], rows[2:3], rows[3:4]
    share = sigmoid_of(temp)
    gone = kept * share / (1.0 - SHRINK * share)
    heat = temp + 0.5 * (v0 * v0 + v1 * v1 + v2 * v2)
    fields = [gone, gone * v0, gone * v1, gone * v2, gone * heat]
    high = [f.astype(BF16).astype(F32) for f in fields]
    low = [f - g for f, g in zip(fields, high)]
    return high + low


def spread(columns, sources, number):
    n = columns.shape[1]
    hot = jnp.where(columns == iota((number, n), 0).astype(F32), 1.0, 0.0).astype(BF16)
    hot = hot.reshape(number // 16, 16, n)
    parts = []
    for source in sources:
        value = jnp.broadcast_to(source, (16, n)).astype(BF16)
        parts.append((hot * value[None]).reshape(number, n))
    return jnp.concatenate(parts, axis=0)


def depth_onehot(rows, depth):
    n = rows.shape[1]
    return jnp.where(rows[7:8] == iota((depth, n), 0).astype(F32), 1.0, 0.0).astype(BF16)


def deposit_fields(fields, anchor_x, anchor_y, cells_y, step, stay, acc):
    total = stay.shape[1]
    columns = acc.shape[0] // (2 * len(fields))
    depth = acc.shape[1]
    acc[...] = jnp.zeros(acc.shape, F32)

    def one(k, carry):
        rows = stay[:, pl.ds(pl.multiple_of(k * step, step), step)]
        column = (rows[5:6] - anchor_x) * cells_y + (rows[6:7] - anchor_y)
        sources = source_rows(rows)
        left = spread(
            column, [sources[f] for f in fields] + [sources[5 + f] for f in fields], columns
        )
        acc[...] += lax.dot_general(
            left, depth_onehot(rows, depth), TRANSPOSED, preferred_element_type=F32
        )
        return carry

    lax.fori_loop(0, total // step, one, 0)


def one_field(rows, along, number, f):
    sources = source_rows(rows)
    left = spread(along, [sources[f], sources[5 + f]], number)
    got = lax.dot_general(left, depth_onehot(rows, 256), TRANSPOSED, preferred_element_type=F32)
    return got[:number] + got[number:]


def deposit_kernel(cells_x, cells_y, step, fields, with_tables, *refs):
    columns = cells_x * cells_y
    if with_tables:
        stay, dep, state, where_to, acc = refs
        total = stay.shape[1]
        state[:, :total] = stay[0:5, :]
        where_to[:, :total] = stay[5:8, :].astype(I32)
    else:
        stay, _, dep, acc = refs
    deposit_fields(fields, *anchors(cells_x, cells_y), cells_y, step, stay, acc)
    n = len(fields)
    for f in range(n):
        for x in range(cells_x):
            high = slice((f * cells_x + x) * cells_y, (f * cells_x + x + 1) * cells_y)
            low = slice(n * columns + high.start, n * columns + high.stop)
            dep[f, x] = acc[high, :] + acc[low, :]


def arrivals(rows, along, number, depth):
    left = spread(along, source_rows(rows), number)
    got = lax.dot_general(left, depth_onehot(rows, depth), TRANSPOSED, preferred_element_type=F32)
    return [
        got[f * number : (f + 1) * number] + got[(5 + f) * number : (6 + f) * number]
        for f in range(5)
    ]


def relay_kernel(cells_x, cells_y, in_even, in_odd, partial, own, leaving, even, odd, planes, halo):
    depth = partial.shape[2]
    anchor_x, _ = anchors(cells_x, cells_y)
    got = receive_pair("gy", in_even, in_odd)
    parts = [unpack(g, depth) for g in got]
    for q, (rows, plane, _, _) in enumerate(parts):
        for f, value in enumerate(arrivals(rows, rows[5:6] - anchor_x, cells_x, depth)):
            planes[q, f] = value
        halo[q] = plane + leaving[2 + q]
    row = iota((cells_y, depth), 0)

    def side(x):
        value = partial[x] + jnp.where(row == 0, planes[0, 4, x : x + 1, :], 0.0)
        return value + jnp.where(row == cells_y - 1, planes[1, 4, x : x + 1, :], 0.0)

    up = message(own[1], side(cells_x - 1), parts[0][3], parts[1][3])
    down = message(own[0], side(0), parts[0][2], parts[1][2])
    send_pair("gx", even, odd, up, down)


def update_kernel(
    cells_x, cells_y, y_even, y_odd, x_even, x_odd, density, momentum, partial, dep01, dep23,
    planes_y, halo_y, leaving, state_in, where_in,
    rho_out, impulse, energy_out, fastest, state, where_to, pressure, planes_x,
):
    depth = partial.shape[2]
    _, anchor_y = anchors(cells_x, cells_y)
    scale = ADIABATIC_INDEX - 1.0
    shape = (cells_y, depth)
    row = iota(shape, 0)
    lane = iota(shape, 1)
    parts = [unpack(g, depth) for g in receive_pair("gx", x_even, x_odd)]
    for q, (rows, plane, _, _) in enumerate(parts):
        for f, value in enumerate(arrivals(rows, rows[6:7] - anchor_y, cells_y, depth)):
            planes_x[q, f] = value
        pressure[q * (cells_x + 1)] = scale * (plane + leaving[q])
    row_x = iota((cells_x, depth), 0)
    halos = []
    for q in range(2):
        value = halo_y[q] + jnp.where(row_x == 0, parts[0][2 + q], 0.0)
        halos.append(scale * (value + jnp.where(row_x == cells_x - 1, parts[1][2 + q], 0.0)))
    tables = [parts[0][0], parts[1][0]] + [
        unpack(g, depth)[0] for g in receive_pair("gy", y_even, y_odd)
    ]
    for q, rows in enumerate(tables):
        lanes = slice(q * rows.shape[1], (q + 1) * rows.shape[1])
        state[:, lanes] = rows[0:5]
        where_to[:, lanes] = rows[5:8].astype(I32)

    def with_planes(f, x, value):
        if x == 0:
            value = value + planes_x[0, f]
        if x == cells_x - 1:
            value = value + planes_x[1, f]
        value = value + jnp.where(row == 0, planes_y[0, f, x : x + 1, :], 0.0)
        return value + jnp.where(row == cells_y - 1, planes_y[1, f, x : x + 1, :], 0.0)

    for x in range(cells_x):
        value = with_planes(4, x, partial[x])
        energy_out[x] = value
        pressure[x + 1] = scale * value
    top = jnp.zeros(shape, F32)
    for x in range(cells_x):
        here = pressure[x + 1]
        grad_x = 0.5 * (pressure[x + 2] - pressure[x])
        after = jnp.where(
            row == cells_y - 1, halos[1][x : x + 1, :], pltpu.roll(here, cells_y - 1, 0)
        )
        before = jnp.where(row == 0, halos[0][x : x + 1, :], pltpu.roll(here, 1, 0))
        grad_y = 0.5 * (after - before)
        after = jnp.where(lane == depth - 1, 0.0, pltpu.roll(here, depth - 1, 1))
        before = jnp.where(lane == 0, 0.0, pltpu.roll(here, 1, 1))
        grad_z = 0.5 * (after - before)
        rho = with_planes(0, x, density[x] + dep01[0, x])
        rho_out[x] = rho
        largest = jnp.zeros(shape, F32)
        deposits = (dep01[1, x], dep23[0, x], dep23[1, x])
        for k, grad in enumerate((grad_x, grad_y, grad_z)):
            value = with_planes(1 + k, x, momentum[k, x] + deposits[k]) - KICK * grad
            impulse[k, x] = value
            largest = jnp.maximum(largest, jnp.abs(value))
        wave = largest / rho + jnp.sqrt(ADIABATIC_INDEX * here / rho)
        top = jnp.maximum(top, wave)
    fastest[...] = jnp.broadcast_to(jnp.max(top, axis=(0, 1), keepdims=True), fastest.shape)


def call(kernel, outs, scratch=(), out_specs=None, in_specs=None, aliases=None, name=None, **extra):
    if in_specs is not None:
        extra["in_specs"] = in_specs
    if out_specs is not None:
        extra["out_specs"] = out_specs
    return pl.pallas_call(
        kernel,
        out_shape=outs,
        scratch_shapes=list(scratch),
        input_output_aliases=aliases or {},
        compiler_params=pltpu.CompilerParams(vmem_limit_bytes=48 * 1024 * 1024),
        name=name,
        **extra,
    )


def swap(axis, even, odd):
    size = lax.axis_size(axis)
    pairs = lambda first: [
        p for i in range(first, size - 1, 2) for p in ((i, i + 1), (i + 1, i))
    ]
    return lax.ppermute(even, axis, pairs(0)), lax.ppermute(odd, axis, pairs(1))


def on_device(
    density, momentum, energy, parcel_mass, droplet_velocity, parcel_temp, parcel_cell, parcel_count
):
    cells_x, cells_y, depth = density.shape
    rows = parcel_mass.shape[0]
    capacity = rows // 16
    chunks = rows // LANES
    columns = cells_x * cells_y
    step = min(1024, rows)
    sds = jax.ShapeDtypeStruct
    whole = pl.BlockSpec(memory_space=VMEM)
    parcels = sds((8, capacity + 3 * depth), F32)
    even, odd, stay, own, leaving, partial = call(
        functools.partial(prep_kernel, cells_x, cells_y, step),
        (
            parcels,
            parcels,
            sds((8, rows), F32),
            sds((2, 8, capacity), F32),
            sds((4, cells_x, depth), F32),
            sds(energy.shape, F32),
        ),
        scratch=(
            VMEM((chunks, LANES), F32),
            VMEM((chunks, LANES), F32),
            VMEM((3, rows), F32),
            VMEM((3, rows), I32),
            VMEM((8, rows), F32),
            VMEM((chunks, LANES), I32),
            VMEM((chunks, LANES), I32),
            VMEM((chunks, LANES), F32),
            VMEM((chunks, 8, LANES), F32),
            VMEM((chunks, LANES), I32),
            pltpu.SMEM((chunks, LANES), I32),
            VMEM((4, capacity // LANES + 1, 8, LANES), F32),
            VMEM((2 * columns, depth), F32),
            pltpu.SemaphoreType.DMA((5,)),
        ),
        in_specs=[pl.BlockSpec(memory_space=pltpu.SMEM)]
        + [pl.BlockSpec(memory_space=pltpu.HBM)] * 4
        + [whole],
        name="prep",
    )(
        parcel_count,
        parcel_mass.reshape(chunks, LANES),
        parcel_temp.reshape(chunks, LANES),
        droplet_velocity,
        parcel_cell,
        energy,
    )
    y_even, y_odd = swap("gy", even, odd)
    slots = rows + 4 * capacity
    two = sds((2, cells_x, cells_y, depth), F32)
    sums = (VMEM((4 * columns, depth), F32),)
    dep01, state, where_to = call(
        functools.partial(deposit_kernel, cells_x, cells_y, step, (0, 1), True),
        (two, sds((5, slots), F32), sds((3, slots), I32)),
        scratch=sums,
        name="deposit01",
    )(stay)
    even, odd, planes_y, halo_y = call(
        functools.partial(relay_kernel, cells_x, cells_y),
        (parcels, parcels, sds((2, 5, cells_x, depth), F32), sds((2, cells_x, depth), F32)),
        name="relay",
    )(y_even, y_odd, partial, own, leaving)
    x_even, x_odd = swap("gx", even, odd)
    (dep23,) = call(
        functools.partial(deposit_kernel, cells_x, cells_y, step, (2, 3), False),
        (two,),
        scratch=sums,
        in_specs=[whole, pl.BlockSpec(memory_space=pl.ANY)],
        name="deposit23",
    )(stay, halo_y)
    last = rows // (4 * capacity)
    rho, impulse, energy_out, top, state, where_to = call(
        functools.partial(update_kernel, cells_x, cells_y),
        (
            sds(density.shape, F32),
            sds(momentum.shape, F32),
            sds(energy.shape, F32),
            sds((lax.axis_size(("gx", "gy")), LANES), F32),
            sds(state.shape, F32),
            sds(where_to.shape, I32),
        ),
        scratch=(
            VMEM((cells_x + 2, cells_y, depth), F32),
            VMEM((2, 5, cells_y, depth), F32),
        ),
        in_specs=[whole] * 12 + [pl.BlockSpec(memory_space=pl.ANY)] * 2,
        out_specs=(whole,) * 4
        + (
            pl.BlockSpec((5, 4 * capacity), lambda i: (0, last)),
            pl.BlockSpec((3, 4 * capacity), lambda i: (0, last)),
        ),
        aliases={12: 4, 13: 5},
        grid=(1,),
        name="update",
    )(
        y_even, y_odd, x_even, x_odd, density, momentum, partial, dep01, dep23,
        planes_y, halo_y, leaving, state, where_to,
    )
    fastest = jnp.max(lax.all_to_all(top, ("gx", "gy"), 0, 0, tiled=True))
    return rho, impulse, energy_out, state, where_to, COURANT / fastest


def solution(mesh):
    both = ("gx", "gy")
    return jax.shard_map(
        on_device,
        mesh=mesh,
        in_specs=(
            P("gx", "gy", None),
            P(None, "gx", "gy", None),
            P("gx", "gy", None),
            P(both),
            P(None, both),
            P(both),
            P(None, both),
            P(both),
        ),
        out_specs=(
            P("gx", "gy", None),
            P(None, "gx", "gy", None),
            P("gx", "gy", None),
            P(None, both),
            P(None, both),
            P(),
        ),
        check_vma=False,
    )
```

```python
import functools

import jax
import jax.numpy as jnp
from jax import lax
from jax.experimental import pallas as pl
from jax.experimental.pallas import tpu as pltpu
from jax.sharding import PartitionSpec as P

ADIABATIC_INDEX = 1.4
KICK = 0.25
COURANT = 0.4
SHRINK = 0.5

F32 = jnp.float32
BF16 = jnp.bfloat16
I32 = jnp.int32
LANES = 128
VMEM = pltpu.VMEM
TRANSPOSED = (((1,), (1,)), ((), ()))


def iota(shape, dim, dtype=I32):
    return lax.broadcasted_iota(dtype, shape, dim)


def sigmoid_of(temp):
    return 1.0 / (1.0 + jnp.exp(-2.0 * (temp - 2.0)))


def prep_kernel(
    cells_x, cells_y, step, count, mass, temp, vel, cell, energy,
    even, odd, stay, own, leaving, partial,
    mass_v, temp_v, vel_v, cell_v, pay, cx, cy, pos, compact, table_v, table_s, tiles, acc, sems,
):
    fetches = [
        pltpu.make_async_copy(there, here, sems.at[i])
        for i, (there, here) in enumerate(
            ((cell, cell_v), (temp, temp_v), (mass, mass_v), (vel, vel_v))
        )
    ]
    for fetch in fetches:
        fetch.start()
    mass, temp, vel, cell = mass_v, temp_v, vel_v, cell_v
    fetches[0].wait()
    chunks = mass.shape[0]
    anchor_x = lax.axis_index("gx") * cells_x
    anchor_y = lax.axis_index("gy") * cells_y
    anchor_xf, anchor_yf = anchors(cells_x, cells_y)
    for b in range(chunks):
        lanes = slice(b * LANES, (b + 1) * LANES)
        cx[b : b + 1, :] = cell[0:1, lanes]
        cy[b : b + 1, :] = cell[1:2, lanes]
    shape = (chunks, LANES)
    live = iota(shape, 0) * LANES + iota(shape, 1) < count[0]
    fetches[1].wait()
    fetches[2].wait()
    kept = mass[...] * (1.0 - SHRINK * jnp.where(live, sigmoid_of(temp[...]), 0.0))
    local_x = cx[...] - anchor_x
    local_y = cy[...] - anchor_y
    heading = jnp.where(
        local_x < 0,
        0,
        jnp.where(
            local_x >= cells_x, 1, jnp.where(local_y < 0, 2, jnp.where(local_y >= cells_y, 3, 4))
        ),
    )
    heading = jnp.where(live, heading, 5)
    masks = [jnp.where(heading == h, 1.0, 0.0) for h in range(4)]
    lane_r = iota((LANES, 2 * LANES), 0)
    lane_c = iota((LANES, 2 * LANES), 1)
    scan = jnp.where((lane_r < lane_c) | (lane_c >= LANES), 1.0, 0.0).astype(BF16)
    both = jnp.dot(
        jnp.concatenate(masks, axis=0).astype(BF16), scan, preferred_element_type=F32
    )
    inner = [both[h * chunks : (h + 1) * chunks, :LANES] for h in range(4)]
    total = [both[h * chunks : (h + 1) * chunks, LANES:] for h in range(4)]
    below = jnp.where(iota((chunks, chunks), 1) < iota((chunks, chunks), 0), 1.0, 0.0).astype(BF16)
    base = jnp.dot(
        below, jnp.concatenate(total, axis=1).astype(BF16), preferred_element_type=F32
    )
    lane = iota(shape, 1)
    offset = jnp.zeros(shape, F32)
    place = jnp.full(shape, -1.0, F32)
    words = jnp.zeros(shape, I32)
    for h in range(4):
        place = jnp.where(heading == h, inner[h] + offset, place)
        base_h = base[:, h * LANES : (h + 1) * LANES]
        word = base_h.astype(I32) + offset.astype(I32) * 1024 + total[h].astype(I32) * (1024 * 256)
        words = jnp.where(lane == h, word, words)
        offset = offset + total[h]
    table_v[...] = words
    load = pltpu.make_async_copy(table_v, table_s, sems.at[4])
    load.start()
    pos[...] = place
    fetches[3].wait()
    pay[1:4, :] = vel[...]
    pay[5:8, :] = cell[...].astype(F32)
    stays = jnp.where(heading == 4, 1.0, 0.0)
    for b in range(chunks):
        lanes = slice(b * LANES, (b + 1) * LANES)
        pay[0:1, lanes] = kept[b : b + 1, :]
        pay[4:5, lanes] = temp[b : b + 1, :]
    for b in range(chunks):
        lanes = slice(b * LANES, (b + 1) * LANES)
        stay[:, lanes] = jnp.where(stays[b : b + 1, :] > 0.0, pay[:, lanes], 0.0)
    group = 16

    def pack(g, carry):
        for u in range(group):
            b = g * group + u
            slots = pos[pl.ds(b, 1), :]
            onehot = jnp.where(slots == iota((LANES, LANES), 0).astype(F32), 1.0, 0.0).astype(BF16)
            rows = pay[:, pl.ds(pl.multiple_of(b * LANES, LANES), LANES)]
            high = rows.astype(BF16).astype(F32)
            rest = rows - high
            middle = rest.astype(BF16).astype(F32)
            low = rest - middle
            parts = jnp.concatenate([high, middle, low, jnp.zeros_like(low)], axis=0).astype(BF16)
            got = lax.dot_general(parts, onehot, TRANSPOSED, preferred_element_type=F32)
            compact[b] = got[0:8] + got[8:16] + got[16:24]
        return carry

    lax.fori_loop(0, chunks // group, pack, 0)
    tiles[...] = jnp.zeros(tiles.shape, F32)
    load.wait()
    lane8 = iota((8, LANES), 1)
    unroll = 8

    def place_all(g, carry):
        carry = list(carry)
        for u in range(unroll):
            b = g * unroll + u
            rows = compact[b]
            for h in range(4):
                word = table_s[b, h]
                start = word & 1023
                first = (word >> 10) & 255
                number = word >> 18
                within = start & (LANES - 1)
                end = within + number
                turned = pltpu.roll(rows, (start - first) & (LANES - 1), 1)
                merged = jnp.where((lane8 >= within) & (lane8 < end), turned, carry[h])
                tiles[h, start >> 7] = merged
                over = jnp.where(lane8 < end - LANES, turned, 0.0)
                carry[h] = jnp.where(end >= LANES, over, merged)
        return tuple(carry)

    carry = lax.fori_loop(
        0, chunks // unroll, place_all, tuple(jnp.zeros((8, LANES), F32) for _ in range(4))
    )
    for h in range(4):
        word = table_s[chunks - 1, h]
        tiles[h, ((word & 1023) + (word >> 18)) >> 7] = carry[h]
    width = 4 * LANES
    buckets = [
        jnp.concatenate([tiles[h, t] for t in range(width // LANES)], axis=1) for h in range(4)
    ]
    for h in range(4):
        along = (buckets[h][6:7] - anchor_yf) if h < 2 else (buckets[h][5:6] - anchor_xf)
        number = cells_y if h < 2 else cells_x
        leaving[h] = one_field(buckets[h], along, number, acc.shape[1], 4)
    for h in range(2):
        own[h] = buckets[h]
    columns = cells_x * cells_y
    deposit_fields((4,), anchor_xf, anchor_yf, cells_y, step, stay, acc)
    for x in range(cells_x):
        rows = slice(x * cells_y, (x + 1) * cells_y)
        partial[x] = energy[x] + (acc[rows] + acc[columns + x * cells_y : columns + (x + 1) * cells_y])
    up = message(buckets[3], partial[:, cells_y - 1, :], leaving[0, -1:, :], leaving[1, -1:, :])
    down = message(buckets[2], partial[:, 0, :], leaving[0, 0:1, :], leaving[1, 0:1, :])
    send_pair("gy", even, odd, up, down)


def message(bucket, plane, first, second):
    half = plane.shape[0] // 2
    rest = jnp.zeros((6, plane.shape[1]), F32)
    return jnp.concatenate(
        [bucket, plane[:half], plane[half:], jnp.concatenate([first, second, rest], axis=0)], axis=1
    )


def unpack(got, depth):
    width = got.shape[1] - 3 * depth
    plane = jnp.concatenate(
        [got[:, width : width + depth], got[:, width + depth : width + 2 * depth]], axis=0
    )
    corner = got[:, width + 2 * depth :]
    return got[:, :width], plane, corner[0:1], corner[1:2]


def send_pair(axis, even, odd, up, down):
    is_even = (lax.axis_index(axis) & 1) == 0
    even[...] = jnp.where(is_even, up, down)
    odd[...] = jnp.where(is_even, down, up)


def receive_pair(axis, even, odd):
    is_even = (lax.axis_index(axis) & 1) == 0
    return jnp.where(is_even, odd[...], even[...]), jnp.where(is_even, even[...], odd[...])


def anchors(cells_x, cells_y):
    return (
        (lax.axis_index("gx") * cells_x).astype(F32),
        (lax.axis_index("gy") * cells_y).astype(F32),
    )


def source_rows(rows):
    kept, temp = rows[0:1], rows[4:5]
    v0, v1, v2 = rows[1:2], rows[2:3], rows[3:4]
    share = sigmoid_of(temp)
    gone = kept * share / (1.0 - SHRINK * share)
    heat = temp + 0.5 * (v0 * v0 + v1 * v1 + v2 * v2)
    fields = [gone, gone * v0, gone * v1, gone * v2, gone * heat]
    high = [f.astype(BF16).astype(F32) for f in fields]
    low = [f - g for f, g in zip(fields, high)]
    return high + low


def spread(columns, sources, number):
    n = columns.shape[1]
    hot = jnp.where(columns == iota((number, n), 0).astype(F32), 1.0, 0.0).astype(BF16)
    hot = hot.reshape(number // 16, 16, n)
    parts = []
    for source in sources:
        value = jnp.broadcast_to(source, (16, n)).astype(BF16)
        parts.append((hot * value[None]).reshape(number, n))
    return jnp.concatenate(parts, axis=0)


def depth_onehot(rows, depth):
    n = rows.shape[1]
    return jnp.where(rows[7:8] == iota((depth, n), 0).astype(F32), 1.0, 0.0).astype(BF16)


def deposit_fields(fields, anchor_x, anchor_y, cells_y, step, stay, acc):
    total = stay.shape[1]
    columns = acc.shape[0] // (2 * len(fields))
    depth = acc.shape[1]
    acc[...] = jnp.zeros(acc.shape, F32)

    def one(k, carry):
        rows = stay[:, pl.ds(pl.multiple_of(k * step, step), step)]
        column = (rows[5:6] - anchor_x) * cells_y + (rows[6:7] - anchor_y)
        sources = source_rows(rows)
        left = spread(
            column, [sources[f] for f in fields] + [sources[5 + f] for f in fields], columns
        )
        acc[...] += lax.dot_general(
            left, depth_onehot(rows, depth), TRANSPOSED, preferred_element_type=F32
        )
        return carry

    lax.fori_loop(0, total // step, one, 0)


def one_field(rows, along, number, depth, f):
    sources = source_rows(rows)
    left = spread(along, [sources[f], sources[5 + f]], number)
    got = lax.dot_general(left, depth_onehot(rows, depth), TRANSPOSED, preferred_element_type=F32)
    return got[:number] + got[number:]


def deposit_kernel(cells_x, cells_y, step, fields, with_tables, *refs):
    columns = cells_x * cells_y
    if with_tables:
        stay, dep, state, where_to, acc = refs
        total = stay.shape[1]
        state[:, :total] = stay[0:5, :]
        where_to[:, :total] = stay[5:8, :].astype(I32)
    else:
        stay, _, dep, acc = refs
    deposit_fields(fields, *anchors(cells_x, cells_y), cells_y, step, stay, acc)
    n = len(fields)
    for f in range(n):
        for x in range(cells_x):
            high = slice((f * cells_x + x) * cells_y, (f * cells_x + x + 1) * cells_y)
            low = slice(n * columns + high.start, n * columns + high.stop)
            dep[f, x] = acc[high, :] + acc[low, :]


def arrivals(rows, along, number, depth):
    left = spread(along, source_rows(rows), number)
    got = lax.dot_general(left, depth_onehot(rows, depth), TRANSPOSED, preferred_element_type=F32)
    return [
        got[f * number : (f + 1) * number] + got[(5 + f) * number : (6 + f) * number]
        for f in range(5)
    ]


def relay_kernel(
    cells_x, cells_y, in_even, in_odd, partial, own, leaving, _, even, odd, planes, halo
):
    depth = partial.shape[2]
    anchor_x, _ = anchors(cells_x, cells_y)
    got = receive_pair("gy", in_even, in_odd)
    parts = [unpack(g, depth) for g in got]
    for q, (rows, plane, _, _) in enumerate(parts):
        for f, value in enumerate(arrivals(rows, rows[5:6] - anchor_x, cells_x, depth)):
            planes[q, f] = value
        halo[q] = plane + leaving[2 + q]
    row = iota((cells_y, depth), 0)

    def side(x):
        value = partial[x] + jnp.where(row == 0, planes[0, 4, x : x + 1, :], 0.0)
        return value + jnp.where(row == cells_y - 1, planes[1, 4, x : x + 1, :], 0.0)

    up = message(own[1], side(cells_x - 1), parts[0][3], parts[1][3])
    down = message(own[0], side(0), parts[0][2], parts[1][2])
    send_pair("gx", even, odd, up, down)


def update_kernel(
    cells_x, cells_y, y_even, y_odd, x_even, x_odd, density, momentum, partial, dep01, dep23,
    planes_y, halo_y, leaving, state_in, where_in,
    rho_out, impulse, energy_out, fastest, state, where_to, pressure, planes_x,
):
    depth = partial.shape[2]
    _, anchor_y = anchors(cells_x, cells_y)
    scale = ADIABATIC_INDEX - 1.0
    shape = (cells_y, depth)
    row = iota(shape, 0)
    lane = iota(shape, 1)
    parts = [unpack(g, depth) for g in receive_pair("gx", x_even, x_odd)]
    for q, (rows, plane, _, _) in enumerate(parts):
        for f, value in enumerate(arrivals(rows, rows[6:7] - anchor_y, cells_y, depth)):
            planes_x[q, f] = value
        pressure[q * (cells_x + 1)] = scale * (plane + leaving[q])
    row_x = iota((cells_x, depth), 0)
    halos = []
    for q in range(2):
        value = halo_y[q] + jnp.where(row_x == 0, parts[0][2 + q], 0.0)
        halos.append(scale * (value + jnp.where(row_x == cells_x - 1, parts[1][2 + q], 0.0)))
    tables = [parts[0][0], parts[1][0]] + [
        unpack(g, depth)[0] for g in receive_pair("gy", y_even, y_odd)
    ]
    for q, rows in enumerate(tables):
        lanes = slice(q * rows.shape[1], (q + 1) * rows.shape[1])
        state[:, lanes] = rows[0:5]
        where_to[:, lanes] = rows[5:8].astype(I32)

    def with_planes(f, x, value):
        if x == 0:
            value = value + planes_x[0, f]
        if x == cells_x - 1:
            value = value + planes_x[1, f]
        value = value + jnp.where(row == 0, planes_y[0, f, x : x + 1, :], 0.0)
        return value + jnp.where(row == cells_y - 1, planes_y[1, f, x : x + 1, :], 0.0)

    for x in range(cells_x):
        value = with_planes(4, x, partial[x])
        energy_out[x] = value
        pressure[x + 1] = scale * value
    top = jnp.zeros(shape, F32)
    for x in range(cells_x):
        here = pressure[x + 1]
        grad_x = 0.5 * (pressure[x + 2] - pressure[x])
        after = jnp.where(
            row == cells_y - 1, halos[1][x : x + 1, :], pltpu.roll(here, cells_y - 1, 0)
        )
        before = jnp.where(row == 0, halos[0][x : x + 1, :], pltpu.roll(here, 1, 0))
        grad_y = 0.5 * (after - before)
        after = jnp.where(lane == depth - 1, 0.0, pltpu.roll(here, depth - 1, 1))
        before = jnp.where(lane == 0, 0.0, pltpu.roll(here, 1, 1))
        grad_z = 0.5 * (after - before)
        rho = with_planes(0, x, density[x] + dep01[0, x])
        rho_out[x] = rho
        largest = jnp.zeros(shape, F32)
        deposits = (dep01[1, x], dep23[0, x], dep23[1, x])
        for k, grad in enumerate((grad_x, grad_y, grad_z)):
            value = with_planes(1 + k, x, momentum[k, x] + deposits[k]) - KICK * grad
            impulse[k, x] = value
            largest = jnp.maximum(largest, jnp.abs(value))
        wave = largest / rho + jnp.sqrt(ADIABATIC_INDEX * here / rho)
        top = jnp.maximum(top, wave)
    fastest[...] = jnp.broadcast_to(jnp.max(top, axis=(0, 1), keepdims=True), fastest.shape)


def call(
    kernel, outs, scratch=(), out_specs=None, in_specs=None, aliases=None, name=None, vmem=48, **extra
):
    if in_specs is not None:
        extra["in_specs"] = in_specs
    if out_specs is not None:
        extra["out_specs"] = out_specs
    return pl.pallas_call(
        kernel,
        out_shape=outs,
        scratch_shapes=list(scratch),
        input_output_aliases=aliases or {},
        compiler_params=pltpu.CompilerParams(vmem_limit_bytes=vmem * 1024 * 1024),
        name=name,
        **extra,
    )


def swap(axis, even, odd):
    size = lax.axis_size(axis)
    pairs = lambda first: [
        p for i in range(first, size - 1, 2) for p in ((i, i + 1), (i + 1, i))
    ]
    return lax.ppermute(even, axis, pairs(0)), lax.ppermute(odd, axis, pairs(1))


def on_device(
    density, momentum, energy, parcel_mass, droplet_velocity, parcel_temp, parcel_cell, parcel_count
):
    cells_x, cells_y, depth = density.shape
    rows = parcel_mass.shape[0]
    capacity = rows // 16
    chunks = rows // LANES
    columns = cells_x * cells_y
    step = min(1024, rows)
    sds = jax.ShapeDtypeStruct
    whole = pl.BlockSpec(memory_space=VMEM)
    parcels = sds((8, capacity + 3 * depth), F32)
    even, odd, stay, own, leaving, partial = call(
        functools.partial(prep_kernel, cells_x, cells_y, step),
        (
            parcels,
            parcels,
            sds((8, rows), F32),
            sds((2, 8, capacity), F32),
            sds((4, cells_x, depth), F32),
            sds(energy.shape, F32),
        ),
        scratch=(
            VMEM((chunks, LANES), F32),
            VMEM((chunks, LANES), F32),
            VMEM((3, rows), F32),
            VMEM((3, rows), I32),
            VMEM((8, rows), F32),
            VMEM((chunks, LANES), I32),
            VMEM((chunks, LANES), I32),
            VMEM((chunks, LANES), F32),
            VMEM((chunks, 8, LANES), F32),
            VMEM((chunks, LANES), I32),
            pltpu.SMEM((chunks, LANES), I32),
            VMEM((4, capacity // LANES + 1, 8, LANES), F32),
            VMEM((2 * columns, depth), F32),
            pltpu.SemaphoreType.DMA((5,)),
        ),
        in_specs=[pl.BlockSpec(memory_space=pltpu.SMEM)]
        + [pl.BlockSpec(memory_space=pltpu.HBM)] * 4
        + [whole],
        name="prep",
    )(
        parcel_count,
        parcel_mass.reshape(chunks, LANES),
        parcel_temp.reshape(chunks, LANES),
        droplet_velocity,
        parcel_cell,
        energy,
    )
    y_even, y_odd = swap("gy", even, odd)
    slots = rows + 4 * capacity
    two = sds((2, cells_x, cells_y, depth), F32)
    sums = (VMEM((4 * columns, depth), F32),)
    dep01, state, where_to = call(
        functools.partial(deposit_kernel, cells_x, cells_y, step, (0, 1), True),
        (two, sds((5, slots), F32), sds((3, slots), I32)),
        scratch=sums,
        name="deposit01",
    )(stay)
    even, odd, planes_y, halo_y = call(
        functools.partial(relay_kernel, cells_x, cells_y),
        (parcels, parcels, sds((2, 5, cells_x, depth), F32), sds((2, cells_x, depth), F32)),
        in_specs=[whole] * 5 + [pl.BlockSpec(memory_space=pl.ANY)],
        name="relay",
    )(y_even, y_odd, partial, own, leaving, dep01)
    x_even, x_odd = swap("gx", even, odd)
    (dep23,) = call(
        functools.partial(deposit_kernel, cells_x, cells_y, step, (2, 3), False),
        (two,),
        scratch=sums,
        in_specs=[whole, pl.BlockSpec(memory_space=pl.ANY)],
        name="deposit23",
    )(stay, halo_y)
    last = rows // (4 * capacity)
    rho, impulse, energy_out, top, state, where_to = call(
        functools.partial(update_kernel, cells_x, cells_y),
        (
            sds(density.shape, F32),
            sds(momentum.shape, F32),
            sds(energy.shape, F32),
            sds((lax.axis_size(("gx", "gy")), LANES), F32),
            sds(state.shape, F32),
            sds(where_to.shape, I32),
        ),
        scratch=(
            VMEM((cells_x + 2, cells_y, depth), F32),
            VMEM((2, 5, cells_y, depth), F32),
        ),
        in_specs=[whole] * 12 + [pl.BlockSpec(memory_space=pl.ANY)] * 2,
        out_specs=(whole,) * 4
        + (
            pl.BlockSpec((5, 4 * capacity), lambda i: (0, last)),
            pl.BlockSpec((3, 4 * capacity), lambda i: (0, last)),
        ),
        aliases={12: 4, 13: 5},
        grid=(1,),
        name="update",
    )(
        y_even, y_odd, x_even, x_odd, density, momentum, partial, dep01, dep23,
        planes_y, halo_y, leaving, state, where_to,
    )
    fastest = jnp.max(lax.all_to_all(top, ("gx", "gy"), 0, 0, tiled=True))
    return rho, impulse, energy_out, state, where_to, COURANT / fastest


def solution(mesh):
    both = ("gx", "gy")
    return jax.shard_map(
        on_device,
        mesh=mesh,
        in_specs=(
            P("gx", "gy", None),
            P(None, "gx", "gy", None),
            P("gx", "gy", None),
            P(both),
            P(None, both),
            P(both),
            P(None, both),
            P(both),
        ),
        out_specs=(
            P("gx", "gy", None),
            P(None, "gx", "gy", None),
            P("gx", "gy", None),
            P(None, both),
            P(None, both),
            P(),
        ),
        check_vma=False,
    )
```

```python
import functools

import jax
import jax.numpy as jnp
from jax import lax
from jax.experimental import pallas as pl
from jax.experimental.pallas import tpu as pltpu
from jax.sharding import PartitionSpec as P

ADIABATIC_INDEX = 1.4
KICK = 0.25
COURANT = 0.4
SHRINK = 0.5

F32 = jnp.float32
BF16 = jnp.bfloat16
I32 = jnp.int32
LANES = 128
VMEM = pltpu.VMEM
TRANSPOSED = (((1,), (1,)), ((), ()))


def iota(shape, dim, dtype=I32):
    return lax.broadcasted_iota(dtype, shape, dim)


def sigmoid_of(temp):
    return 1.0 / (1.0 + jnp.exp(-2.0 * (temp - 2.0)))


def rank_kernel(cells_x, cells_y, count, cell, place, stays, words, masks, cx, cy):
    chunks = place.shape[0]
    anchor_x = lax.axis_index("gx") * cells_x
    anchor_y = lax.axis_index("gy") * cells_y
    for b in range(chunks):
        lanes = slice(b * LANES, (b + 1) * LANES)
        cx[b : b + 1, :] = cell[0:1, lanes]
        cy[b : b + 1, :] = cell[1:2, lanes]
    shape = (chunks, LANES)
    lane = iota(shape, 1)
    live = iota(shape, 0) * LANES + lane < count[0]
    local_x = cx[...] - anchor_x
    local_y = cy[...] - anchor_y
    heading = jnp.where(
        local_x < 0,
        0,
        jnp.where(
            local_x >= cells_x, 1, jnp.where(local_y < 0, 2, jnp.where(local_y >= cells_y, 3, 4))
        ),
    )
    heading = jnp.where(live, heading, 5)
    hits = [jnp.where(heading == h, 1.0, 0.0) for h in range(4)]
    lane_r = iota((LANES, 2 * LANES), 0)
    lane_c = iota((LANES, 2 * LANES), 1)
    scan = jnp.where((lane_r < lane_c) | (lane_c >= LANES), 1.0, 0.0).astype(BF16)
    both = jnp.dot(jnp.concatenate(hits, axis=0).astype(BF16), scan, preferred_element_type=F32)
    inner = [both[h * chunks : (h + 1) * chunks, :LANES] for h in range(4)]
    total = [both[h * chunks : (h + 1) * chunks, LANES:] for h in range(4)]
    below = jnp.where(iota((chunks, chunks), 1) < iota((chunks, chunks), 0), 1.0, 0.0).astype(BF16)
    base = jnp.dot(
        below, jnp.concatenate(total, axis=1).astype(BF16), preferred_element_type=F32
    ).astype(I32)
    offset = jnp.zeros(shape, F32)
    spot = jnp.full(shape, -1.0, F32)
    word = jnp.zeros(shape, I32)
    for h in range(4):
        spot = jnp.where(heading == h, inner[h] + offset, spot)
        start = base[:, h * LANES : (h + 1) * LANES]
        within = start & (LANES - 1)
        end = within + total[h].astype(I32)
        turn = (start - offset.astype(I32)) & (LANES - 1)
        word = jnp.where(lane == h, (start >> 7) * LANES + turn, word)
        last = start + total[h].astype(I32)
        word = jnp.where(lane == 4 + h, last >> 7, word)
        masks[h, 0] = jnp.where((lane >= within) & (lane < end), 1.0, 0.0)
        masks[h, 1] = jnp.where(lane < end - LANES, 1.0, 0.0)
        masks[h, 2] = jnp.where(end >= LANES, 1.0, 0.0)
        offset = offset + total[h]
    words[...] = word
    place[...] = spot
    stays[...] = jnp.where(heading == 4, 1.0, 0.0)


def prep_kernel(
    cells_x, cells_y, step, mass, temp, vel, cell, energy, pos, stays, words, masks,
    even, odd, stay, own, leaving, partial,
    pay, compact, table, tiles, acc, sem,
):
    load = pltpu.make_async_copy(words, table, sem)
    load.start()
    chunks = mass.shape[0]
    anchor_xf, anchor_yf = anchors(cells_x, cells_y)
    kept = mass[...] * (1.0 - SHRINK * sigmoid_of(temp[...]))
    pay[1:4, :] = vel[...]
    pay[5:8, :] = cell[...].astype(F32)
    for b in range(chunks):
        lanes = slice(b * LANES, (b + 1) * LANES)
        pay[0:1, lanes] = kept[b : b + 1, :]
        pay[4:5, lanes] = temp[b : b + 1, :]
    for b in range(chunks):
        lanes = slice(b * LANES, (b + 1) * LANES)
        stay[:, lanes] = jnp.where(stays[b : b + 1, :] > 0.0, pay[:, lanes], 0.0)
    group = 16

    def pack(g, carry):
        for u in range(group):
            b = g * group + u
            slots = pos[pl.ds(b, 1), :]
            onehot = jnp.where(slots == iota((LANES, LANES), 0).astype(F32), 1.0, 0.0).astype(BF16)
            rows = pay[:, pl.ds(pl.multiple_of(b * LANES, LANES), LANES)]
            high = rows.astype(BF16).astype(F32)
            rest = rows - high
            middle = rest.astype(BF16).astype(F32)
            low = rest - middle
            parts = jnp.concatenate([high, middle, low, jnp.zeros_like(low)], axis=0).astype(BF16)
            got = lax.dot_general(parts, onehot, TRANSPOSED, preferred_element_type=F32)
            compact[b] = got[0:8] + got[8:16] + got[16:24]
        return carry

    lax.fori_loop(0, chunks // group, pack, 0)
    tiles[...] = jnp.zeros(tiles.shape, F32)
    load.wait()
    unroll = 8

    def place_all(g, carry):
        carry = list(carry)
        for u in range(unroll):
            b = g * unroll + u
            rows = compact[b]
            for h in range(4):
                word = table[b, h]
                turned = pltpu.roll(rows, word & (LANES - 1), 1)
                merged = jnp.where(masks[h, 0, pl.ds(b, 1), :] > 0.0, turned, carry[h])
                tiles[h, word >> 7] = merged
                rest = jnp.where(masks[h, 2, pl.ds(b, 1), :] > 0.0, 0.0, merged)
                carry[h] = jnp.where(masks[h, 1, pl.ds(b, 1), :] > 0.0, turned, rest)
        return tuple(carry)

    carry = lax.fori_loop(
        0, chunks // unroll, place_all, tuple(jnp.zeros((8, LANES), F32) for _ in range(4))
    )
    for h in range(4):
        tiles[h, table[chunks - 1, 4 + h]] = carry[h]
    width = own.shape[2]
    buckets = [
        jnp.concatenate([tiles[h, t] for t in range(width // LANES)], axis=1) for h in range(4)
    ]
    for h in range(4):
        along = (buckets[h][6:7] - anchor_yf) if h < 2 else (buckets[h][5:6] - anchor_xf)
        number = cells_y if h < 2 else cells_x
        leaving[h] = one_field(buckets[h], along, number, acc.shape[1], 4)
    for h in range(2):
        own[h] = buckets[h]
    columns = cells_x * cells_y
    deposit_fields((4,), anchor_xf, anchor_yf, cells_y, step, stay, acc)
    for x in range(cells_x):
        rows = slice(x * cells_y, (x + 1) * cells_y)
        partial[x] = energy[x] + (acc[rows] + acc[columns + x * cells_y : columns + (x + 1) * cells_y])
    up = message(buckets[3], partial[:, cells_y - 1, :], leaving[0, -1:, :], leaving[1, -1:, :])
    down = message(buckets[2], partial[:, 0, :], leaving[0, 0:1, :], leaving[1, 0:1, :])
    send_pair("gy", even, odd, up, down)


def message(bucket, plane, first, second):
    half = plane.shape[0] // 2
    rest = jnp.zeros((6, plane.shape[1]), F32)
    return jnp.concatenate(
        [bucket, plane[:half], plane[half:], jnp.concatenate([first, second, rest], axis=0)], axis=1
    )


def unpack(got, depth):
    width = got.shape[1] - 3 * depth
    plane = jnp.concatenate(
        [got[:, width : width + depth], got[:, width + depth : width + 2 * depth]], axis=0
    )
    corner = got[:, width + 2 * depth :]
    return got[:, :width], plane, corner[0:1], corner[1:2]


def send_pair(axis, even, odd, up, down):
    is_even = (lax.axis_index(axis) & 1) == 0
    even[...] = jnp.where(is_even, up, down)
    odd[...] = jnp.where(is_even, down, up)


def receive_pair(axis, even, odd):
    is_even = (lax.axis_index(axis) & 1) == 0
    return jnp.where(is_even, odd[...], even[...]), jnp.where(is_even, even[...], odd[...])


def anchors(cells_x, cells_y):
    return (
        (lax.axis_index("gx") * cells_x).astype(F32),
        (lax.axis_index("gy") * cells_y).astype(F32),
    )


def source_rows(rows):
    kept, temp = rows[0:1], rows[4:5]
    v0, v1, v2 = rows[1:2], rows[2:3], rows[3:4]
    share = sigmoid_of(temp)
    gone = kept * share / (1.0 - SHRINK * share)
    heat = temp + 0.5 * (v0 * v0 + v1 * v1 + v2 * v2)
    fields = [gone, gone * v0, gone * v1, gone * v2, gone * heat]
    high = [f.astype(BF16).astype(F32) for f in fields]
    low = [f - g for f, g in zip(fields, high)]
    return high + low


def spread(columns, sources, number):
    n = columns.shape[1]
    hot = jnp.where(columns == iota((number, n), 0).astype(F32), 1.0, 0.0).astype(BF16)
    hot = hot.reshape(number // 16, 16, n)
    parts = []
    for source in sources:
        value = jnp.broadcast_to(source, (16, n)).astype(BF16)
        parts.append((hot * value[None]).reshape(number, n))
    return jnp.concatenate(parts, axis=0)


def depth_onehot(rows, depth):
    n = rows.shape[1]
    return jnp.where(rows[7:8] == iota((depth, n), 0).astype(F32), 1.0, 0.0).astype(BF16)


def deposit_fields(fields, anchor_x, anchor_y, cells_y, step, stay, acc):
    total = stay.shape[1]
    columns = acc.shape[0] // (2 * len(fields))
    depth = acc.shape[1]
    acc[...] = jnp.zeros(acc.shape, F32)

    def one(k, carry):
        rows = stay[:, pl.ds(pl.multiple_of(k * step, step), step)]
        column = (rows[5:6] - anchor_x) * cells_y + (rows[6:7] - anchor_y)
        sources = source_rows(rows)
        left = spread(
            column, [sources[f] for f in fields] + [sources[5 + f] for f in fields], columns
        )
        acc[...] += lax.dot_general(
            left, depth_onehot(rows, depth), TRANSPOSED, preferred_element_type=F32
        )
        return carry

    lax.fori_loop(0, total // step, one, 0)


def one_field(rows, along, number, depth, f):
    sources = source_rows(rows)
    left = spread(along, [sources[f], sources[5 + f]], number)
    got = lax.dot_general(left, depth_onehot(rows, depth), TRANSPOSED, preferred_element_type=F32)
    return got[:number] + got[number:]


def deposit_kernel(cells_x, cells_y, step, fields, with_tables, *refs):
    columns = cells_x * cells_y
    if with_tables:
        stay, dep, state, where_to, acc = refs
        total = stay.shape[1]
        state[:, :total] = stay[0:5, :]
        where_to[:, :total] = stay[5:8, :].astype(I32)
    else:
        stay, _, dep, acc = refs
    deposit_fields(fields, *anchors(cells_x, cells_y), cells_y, step, stay, acc)
    n = len(fields)
    for f in range(n):
        for x in range(cells_x):
            high = slice((f * cells_x + x) * cells_y, (f * cells_x + x + 1) * cells_y)
            low = slice(n * columns + high.start, n * columns + high.stop)
            dep[f, x] = acc[high, :] + acc[low, :]


def arrivals(rows, along, number, depth):
    left = spread(along, source_rows(rows), number)
    got = lax.dot_general(left, depth_onehot(rows, depth), TRANSPOSED, preferred_element_type=F32)
    return [
        got[f * number : (f + 1) * number] + got[(5 + f) * number : (6 + f) * number]
        for f in range(5)
    ]


def relay_kernel(
    cells_x, cells_y, in_even, in_odd, partial, own, leaving, _, even, odd, planes, halo
):
    depth = partial.shape[2]
    anchor_x, _ = anchors(cells_x, cells_y)
    got = receive_pair("gy", in_even, in_odd)
    parts = [unpack(g, depth) for g in got]
    for q, (rows, plane, _, _) in enumerate(parts):
        for f, value in enumerate(arrivals(rows, rows[5:6] - anchor_x, cells_x, depth)):
            planes[q, f] = value
        halo[q] = plane + leaving[2 + q]
    row = iota((cells_y, depth), 0)

    def side(x):
        value = partial[x] + jnp.where(row == 0, planes[0, 4, x : x + 1, :], 0.0)
        return value + jnp.where(row == cells_y - 1, planes[1, 4, x : x + 1, :], 0.0)

    up = message(own[1], side(cells_x - 1), parts[0][3], parts[1][3])
    down = message(own[0], side(0), parts[0][2], parts[1][2])
    send_pair("gx", even, odd, up, down)


def update_kernel(
    cells_x, cells_y, y_even, y_odd, x_even, x_odd, density, momentum, partial, dep01, dep23,
    planes_y, halo_y, leaving, state_in, where_in,
    rho_out, impulse, energy_out, fastest, state, where_to, pressure, planes_x,
):
    depth = partial.shape[2]
    _, anchor_y = anchors(cells_x, cells_y)
    scale = ADIABATIC_INDEX - 1.0
    shape = (cells_y, depth)
    row = iota(shape, 0)
    lane = iota(shape, 1)
    parts = [unpack(g, depth) for g in receive_pair("gx", x_even, x_odd)]
    for q, (rows, plane, _, _) in enumerate(parts):
        for f, value in enumerate(arrivals(rows, rows[6:7] - anchor_y, cells_y, depth)):
            planes_x[q, f] = value
        pressure[q * (cells_x + 1)] = scale * (plane + leaving[q])
    row_x = iota((cells_x, depth), 0)
    halos = []
    for q in range(2):
        value = halo_y[q] + jnp.where(row_x == 0, parts[0][2 + q], 0.0)
        halos.append(scale * (value + jnp.where(row_x == cells_x - 1, parts[1][2 + q], 0.0)))
    tables = [parts[0][0], parts[1][0]] + [
        unpack(g, depth)[0] for g in receive_pair("gy", y_even, y_odd)
    ]
    for q, rows in enumerate(tables):
        lanes = slice(q * rows.shape[1], (q + 1) * rows.shape[1])
        state[:, lanes] = rows[0:5]
        where_to[:, lanes] = rows[5:8].astype(I32)

    def with_planes(f, x, value):
        if x == 0:
            value = value + planes_x[0, f]
        if x == cells_x - 1:
            value = value + planes_x[1, f]
        value = value + jnp.where(row == 0, planes_y[0, f, x : x + 1, :], 0.0)
        return value + jnp.where(row == cells_y - 1, planes_y[1, f, x : x + 1, :], 0.0)

    for x in range(cells_x):
        value = with_planes(4, x, partial[x])
        energy_out[x] = value
        pressure[x + 1] = scale * value
    top = jnp.zeros(shape, F32)
    for x in range(cells_x):
        here = pressure[x + 1]
        grad_x = 0.5 * (pressure[x + 2] - pressure[x])
        after = jnp.where(
            row == cells_y - 1, halos[1][x : x + 1, :], pltpu.roll(here, cells_y - 1, 0)
        )
        before = jnp.where(row == 0, halos[0][x : x + 1, :], pltpu.roll(here, 1, 0))
        grad_y = 0.5 * (after - before)
        after = jnp.where(lane == depth - 1, 0.0, pltpu.roll(here, depth - 1, 1))
        before = jnp.where(lane == 0, 0.0, pltpu.roll(here, 1, 1))
        grad_z = 0.5 * (after - before)
        rho = with_planes(0, x, density[x] + dep01[0, x])
        rho_out[x] = rho
        largest = jnp.zeros(shape, F32)
        deposits = (dep01[1, x], dep23[0, x], dep23[1, x])
        for k, grad in enumerate((grad_x, grad_y, grad_z)):
            value = with_planes(1 + k, x, momentum[k, x] + deposits[k]) - KICK * grad
            impulse[k, x] = value
            largest = jnp.maximum(largest, jnp.abs(value))
        wave = largest / rho + jnp.sqrt(ADIABATIC_INDEX * here / rho)
        top = jnp.maximum(top, wave)
    fastest[...] = jnp.broadcast_to(jnp.max(top, axis=(0, 1), keepdims=True), fastest.shape)


def call(
    kernel, outs, scratch=(), out_specs=None, in_specs=None, aliases=None, name=None, vmem=48, **extra
):
    if in_specs is not None:
        extra["in_specs"] = in_specs
    if out_specs is not None:
        extra["out_specs"] = out_specs
    return pl.pallas_call(
        kernel,
        out_shape=outs,
        scratch_shapes=list(scratch),
        input_output_aliases=aliases or {},
        compiler_params=pltpu.CompilerParams(vmem_limit_bytes=vmem * 1024 * 1024),
        name=name,
        **extra,
    )


def swap(axis, even, odd):
    size = lax.axis_size(axis)
    pairs = lambda first: [
        p for i in range(first, size - 1, 2) for p in ((i, i + 1), (i + 1, i))
    ]
    return lax.ppermute(even, axis, pairs(0)), lax.ppermute(odd, axis, pairs(1))


def on_device(
    density, momentum, energy, parcel_mass, droplet_velocity, parcel_temp, parcel_cell, parcel_count
):
    cells_x, cells_y, depth = density.shape
    rows = parcel_mass.shape[0]
    capacity = rows // 16
    chunks = rows // LANES
    columns = cells_x * cells_y
    step = min(1024, rows)
    sds = jax.ShapeDtypeStruct
    whole = pl.BlockSpec(memory_space=VMEM)
    parcels = sds((8, capacity + 3 * depth), F32)
    dense = sds((chunks, LANES), F32)
    place, stays, words, masks = call(
        functools.partial(rank_kernel, cells_x, cells_y),
        (dense, dense, sds((chunks, LANES), I32), sds((4, 3, chunks, LANES), F32)),
        scratch=(VMEM((chunks, LANES), I32), VMEM((chunks, LANES), I32)),
        in_specs=[pl.BlockSpec(memory_space=pltpu.SMEM), whole],
        name="rank",
        cost_estimate=pl.CostEstimate(flops=10**9, bytes_accessed=10**6, transcendentals=0),
    )(parcel_count, parcel_cell)
    even, odd, stay, own, leaving, partial = call(
        functools.partial(prep_kernel, cells_x, cells_y, step),
        (
            parcels,
            parcels,
            sds((8, rows), F32),
            sds((2, 8, capacity), F32),
            sds((4, cells_x, depth), F32),
            sds(energy.shape, F32),
        ),
        scratch=(
            VMEM((8, rows), F32),
            VMEM((chunks, 8, LANES), F32),
            pltpu.SMEM((chunks, LANES), I32),
            VMEM((4, capacity // LANES + 1, 8, LANES), F32),
            VMEM((2 * columns, depth), F32),
            pltpu.SemaphoreType.DMA,
        ),
        name="prep",
    )(
        parcel_mass.reshape(chunks, LANES),
        parcel_temp.reshape(chunks, LANES),
        droplet_velocity,
        parcel_cell,
        energy,
        place,
        stays,
        words,
        masks,
    )
    y_even, y_odd = swap("gy", even, odd)
    slots = rows + 4 * capacity
    two = sds((2, cells_x, cells_y, depth), F32)
    sums = (VMEM((4 * columns, depth), F32),)
    dep01, state, where_to = call(
        functools.partial(deposit_kernel, cells_x, cells_y, step, (0, 1), True),
        (two, sds((5, slots), F32), sds((3, slots), I32)),
        scratch=sums,
        name="deposit01",
    )(stay)
    even, odd, planes_y, halo_y = call(
        functools.partial(relay_kernel, cells_x, cells_y),
        (parcels, parcels, sds((2, 5, cells_x, depth), F32), sds((2, cells_x, depth), F32)),
        in_specs=[whole] * 5 + [pl.BlockSpec(memory_space=pl.ANY)],
        name="relay",
    )(y_even, y_odd, partial, own, leaving, dep01)
    x_even, x_odd = swap("gx", even, odd)
    (dep23,) = call(
        functools.partial(deposit_kernel, cells_x, cells_y, step, (2, 3), False),
        (two,),
        scratch=sums,
        in_specs=[whole, pl.BlockSpec(memory_space=pl.ANY)],
        name="deposit23",
    )(stay, halo_y)
    last = rows // (4 * capacity)
    rho, impulse, energy_out, top, state, where_to = call(
        functools.partial(update_kernel, cells_x, cells_y),
        (
            sds(density.shape, F32),
            sds(momentum.shape, F32),
            sds(energy.shape, F32),
            sds((lax.axis_size(("gx", "gy")), LANES), F32),
            sds(state.shape, F32),
            sds(where_to.shape, I32),
        ),
        scratch=(
            VMEM((cells_x + 2, cells_y, depth), F32),
            VMEM((2, 5, cells_y, depth), F32),
        ),
        in_specs=[whole] * 12 + [pl.BlockSpec(memory_space=pl.ANY)] * 2,
        out_specs=(whole,) * 4
        + (
            pl.BlockSpec((5, 4 * capacity), lambda i: (0, last)),
            pl.BlockSpec((3, 4 * capacity), lambda i: (0, last)),
        ),
        aliases={12: 4, 13: 5},
        grid=(1,),
        name="update",
    )(
        y_even, y_odd, x_even, x_odd, density, momentum, partial, dep01, dep23,
        planes_y, halo_y, leaving, state, where_to,
    )
    fastest = jnp.max(lax.all_to_all(top, ("gx", "gy"), 0, 0, tiled=True))
    return rho, impulse, energy_out, state, where_to, COURANT / fastest


def solution(mesh):
    both = ("gx", "gy")
    return jax.shard_map(
        on_device,
        mesh=mesh,
        in_specs=(
            P("gx", "gy", None),
            P(None, "gx", "gy", None),
            P("gx", "gy", None),
            P(both),
            P(None, both),
            P(both),
            P(None, both),
            P(both),
        ),
        out_specs=(
            P("gx", "gy", None),
            P(None, "gx", "gy", None),
            P("gx", "gy", None),
            P(None, both),
            P(None, both),
            P(),
        ),
        check_vma=False,
    )
```

```python
import functools

import jax
import jax.numpy as jnp
from jax import lax
from jax.experimental import pallas as pl
from jax.experimental.pallas import tpu as pltpu
from jax.sharding import PartitionSpec as P

ADIABATIC_INDEX = 1.4
KICK = 0.25
COURANT = 0.4
SHRINK = 0.5

F32 = jnp.float32
BF16 = jnp.bfloat16
I32 = jnp.int32
LANES = 128
VMEM = pltpu.VMEM
TRANSPOSED = (((1,), (1,)), ((), ()))


def iota(shape, dim, dtype=I32):
    return lax.broadcasted_iota(dtype, shape, dim)


def sigmoid_of(temp):
    return 1.0 / (1.0 + jnp.exp(-2.0 * (temp - 2.0)))


def rank_kernel(cells_x, cells_y, count, cell, place, stays, words, masks, cx, cy):
    chunks = place.shape[0]
    anchor_x = lax.axis_index("gx") * cells_x
    anchor_y = lax.axis_index("gy") * cells_y
    for b in range(chunks):
        lanes = slice(b * LANES, (b + 1) * LANES)
        cx[b : b + 1, :] = cell[0:1, lanes]
        cy[b : b + 1, :] = cell[1:2, lanes]
    shape = (chunks, LANES)
    lane = iota(shape, 1)
    live = iota(shape, 0) * LANES + lane < count[0]
    local_x = cx[...] - anchor_x
    local_y = cy[...] - anchor_y
    heading = jnp.where(
        local_x < 0,
        0,
        jnp.where(
            local_x >= cells_x, 1, jnp.where(local_y < 0, 2, jnp.where(local_y >= cells_y, 3, 4))
        ),
    )
    heading = jnp.where(live, heading, 5)
    hits = [jnp.where(heading == h, 1.0, 0.0) for h in range(4)]
    lane_r = iota((LANES, 2 * LANES), 0)
    lane_c = iota((LANES, 2 * LANES), 1)
    scan = jnp.where((lane_r < lane_c) | (lane_c >= LANES), 1.0, 0.0).astype(BF16)
    both = jnp.dot(jnp.concatenate(hits, axis=0).astype(BF16), scan, preferred_element_type=F32)
    inner = [both[h * chunks : (h + 1) * chunks, :LANES] for h in range(4)]
    total = [both[h * chunks : (h + 1) * chunks, LANES:] for h in range(4)]
    below = jnp.where(iota((chunks, chunks), 1) < iota((chunks, chunks), 0), 1.0, 0.0).astype(BF16)
    base = jnp.dot(
        below, jnp.concatenate(total, axis=1).astype(BF16), preferred_element_type=F32
    ).astype(I32)
    offset = jnp.zeros(shape, F32)
    spot = jnp.full(shape, -1.0, F32)
    word = jnp.zeros(shape, I32)
    for h in range(4):
        spot = jnp.where(heading == h, inner[h] + offset, spot)
        start = base[:, h * LANES : (h + 1) * LANES]
        within = start & (LANES - 1)
        end = within + total[h].astype(I32)
        turn = (start - offset.astype(I32)) & (LANES - 1)
        word = jnp.where(lane == h, (start >> 7) * LANES + turn, word)
        last = start + total[h].astype(I32)
        word = jnp.where(lane == 4 + h, last >> 7, word)
        masks[h, 0] = jnp.where((lane >= within) & (lane < end), 1.0, 0.0)
        masks[h, 1] = jnp.where(lane < end - LANES, 1.0, 0.0)
        masks[h, 2] = jnp.where(end >= LANES, 1.0, 0.0)
        offset = offset + total[h]
    words[...] = word
    place[...] = spot
    stays[...] = jnp.where(heading == 4, 1.0, 0.0)


def prep_kernel(
    cells_x, cells_y, step, mass, temp, vel, cell, energy, pos, stays, words, masks,
    even, odd, stay, own, leaving, partial,
    pay, compact, table, tiles, acc, sem,
):
    load = pltpu.make_async_copy(words, table, sem)
    load.start()
    chunks = mass.shape[0]
    anchor_xf, anchor_yf = anchors(cells_x, cells_y)
    kept = mass[...] * (1.0 - SHRINK * sigmoid_of(temp[...]))
    pay[1:4, :] = vel[...]
    pay[5:8, :] = cell[...].astype(F32)
    for b in range(chunks):
        lanes = slice(b * LANES, (b + 1) * LANES)
        pay[0:1, lanes] = kept[b : b + 1, :]
        pay[4:5, lanes] = temp[b : b + 1, :]
    for b in range(chunks):
        lanes = slice(b * LANES, (b + 1) * LANES)
        stay[:, lanes] = jnp.where(stays[b : b + 1, :] > 0.0, pay[:, lanes], 0.0)
    group = 16

    def pack(g, carry):
        for u in range(group):
            b = g * group + u
            slots = pos[pl.ds(b, 1), :]
            onehot = jnp.where(slots == iota((LANES, LANES), 0).astype(F32), 1.0, 0.0).astype(BF16)
            rows = pay[:, pl.ds(pl.multiple_of(b * LANES, LANES), LANES)]
            high = rows.astype(BF16).astype(F32)
            rest = rows - high
            middle = rest.astype(BF16).astype(F32)
            low = rest - middle
            parts = jnp.concatenate([high, middle, low, jnp.zeros_like(low)], axis=0).astype(BF16)
            got = lax.dot_general(parts, onehot, TRANSPOSED, preferred_element_type=F32)
            compact[b] = got[0:8] + got[8:16] + got[16:24]
        return carry

    lax.fori_loop(0, chunks // group, pack, 0)
    tiles[...] = jnp.zeros(tiles.shape, F32)
    load.wait()
    unroll = 8

    def place_all(g, carry):
        carry = list(carry)
        for u in range(unroll):
            b = g * unroll + u
            rows = compact[b]
            for h in range(4):
                word = table[b, h]
                turned = pltpu.roll(rows, word & (LANES - 1), 1)
                merged = jnp.where(masks[h, 0, pl.ds(b, 1), :] > 0.0, turned, carry[h])
                tiles[h, word >> 7] = merged
                rest = jnp.where(masks[h, 2, pl.ds(b, 1), :] > 0.0, 0.0, merged)
                carry[h] = jnp.where(masks[h, 1, pl.ds(b, 1), :] > 0.0, turned, rest)
        return tuple(carry)

    carry = lax.fori_loop(
        0, chunks // unroll, place_all, tuple(jnp.zeros((8, LANES), F32) for _ in range(4))
    )
    for h in range(4):
        tiles[h, table[chunks - 1, 4 + h]] = carry[h]
    width = own.shape[2]
    buckets = [
        jnp.concatenate([tiles[h, t] for t in range(width // LANES)], axis=1) for h in range(4)
    ]
    for h in range(4):
        along = (buckets[h][6:7] - anchor_yf) if h < 2 else (buckets[h][5:6] - anchor_xf)
        number = cells_y if h < 2 else cells_x
        leaving[h] = one_field(buckets[h], along, number, acc.shape[1], 4)
    for h in range(2):
        own[h] = buckets[h]
    outer_energy(cells_x, cells_y, anchor_xf, anchor_yf, step, stay, acc)
    planes = [acc[q * 2 * cells_y : (q * 2 + 1) * cells_y] + acc[(q * 2 + 1) * cells_y : (q * 2 + 2) * cells_y] for q in range(4)]
    partial[0] = energy[0] + planes[0]
    partial[1] = energy[cells_x - 1] + planes[1]
    up = message(
        buckets[3], energy[:, cells_y - 1, :] + planes[3], leaving[0, -1:, :], leaving[1, -1:, :]
    )
    down = message(buckets[2], energy[:, 0, :] + planes[2], leaving[0, 0:1, :], leaving[1, 0:1, :])
    send_pair("gy", even, odd, up, down)


def message(bucket, plane, first, second):
    half = plane.shape[0] // 2
    rest = jnp.zeros((6, plane.shape[1]), F32)
    return jnp.concatenate(
        [bucket, plane[:half], plane[half:], jnp.concatenate([first, second, rest], axis=0)], axis=1
    )


def unpack(got, depth):
    width = got.shape[1] - 3 * depth
    plane = jnp.concatenate(
        [got[:, width : width + depth], got[:, width + depth : width + 2 * depth]], axis=0
    )
    corner = got[:, width + 2 * depth :]
    return got[:, :width], plane, corner[0:1], corner[1:2]


def send_pair(axis, even, odd, up, down):
    is_even = (lax.axis_index(axis) & 1) == 0
    even[...] = jnp.where(is_even, up, down)
    odd[...] = jnp.where(is_even, down, up)


def receive_pair(axis, even, odd):
    is_even = (lax.axis_index(axis) & 1) == 0
    return jnp.where(is_even, odd[...], even[...]), jnp.where(is_even, even[...], odd[...])


def anchors(cells_x, cells_y):
    return (
        (lax.axis_index("gx") * cells_x).astype(F32),
        (lax.axis_index("gy") * cells_y).astype(F32),
    )


def source_rows(rows):
    kept, temp = rows[0:1], rows[4:5]
    v0, v1, v2 = rows[1:2], rows[2:3], rows[3:4]
    share = sigmoid_of(temp)
    gone = kept * share / (1.0 - SHRINK * share)
    heat = temp + 0.5 * (v0 * v0 + v1 * v1 + v2 * v2)
    fields = [gone, gone * v0, gone * v1, gone * v2, gone * heat]
    high = [f.astype(BF16).astype(F32) for f in fields]
    low = [f - g for f, g in zip(fields, high)]
    return high + low


def spread(columns, sources, number):
    n = columns.shape[1]
    hot = jnp.where(columns == iota((number, n), 0).astype(F32), 1.0, 0.0).astype(BF16)
    hot = hot.reshape(number // 16, 16, n)
    parts = []
    for source in sources:
        value = jnp.broadcast_to(source, (16, n)).astype(BF16)
        parts.append((hot * value[None]).reshape(number, n))
    return jnp.concatenate(parts, axis=0)


def depth_onehot(rows, depth):
    n = rows.shape[1]
    return jnp.where(rows[7:8] == iota((depth, n), 0).astype(F32), 1.0, 0.0).astype(BF16)


def outer_energy(cells_x, cells_y, anchor_x, anchor_y, step, stay, acc):
    total = stay.shape[1]
    depth = acc.shape[1]
    acc[...] = jnp.zeros(acc.shape, F32)

    def one(k, carry):
        rows = stay[:, pl.ds(pl.multiple_of(k * step, step), step)]
        x = rows[5:6] - anchor_x
        y = rows[6:7] - anchor_y
        sources = source_rows(rows)
        pair = (sources[4], sources[9])
        on_x = [jnp.where(x == at, v, 0.0) for at in (0.0, cells_x - 1.0) for v in pair]
        on_y = [jnp.where(y == at, v, 0.0) for at in (0.0, cells_y - 1.0) for v in pair]
        left = jnp.concatenate([spread(y, on_x, cells_y), spread(x, on_y, cells_x)], axis=0)
        acc[...] += lax.dot_general(
            left, depth_onehot(rows, depth), TRANSPOSED, preferred_element_type=F32
        )
        return carry

    lax.fori_loop(0, total // step, one, 0)


def one_field(rows, along, number, depth, f):
    sources = source_rows(rows)
    left = spread(along, [sources[f], sources[5 + f]], number)
    got = lax.dot_general(left, depth_onehot(rows, depth), TRANSPOSED, preferred_element_type=F32)
    return got[:number] + got[number:]


def deposit_kernel(cells_x, cells_y, step, steps, *refs):
    columns = cells_x * cells_y
    if steps[0] == 0:
        stay, dep, state, where_to, acc = refs
        before = None
        total = stay.shape[1]
        state[:, :total] = stay[0:5, :]
        where_to[:, :total] = stay[5:8, :].astype(I32)
    else:
        stay, before, _, dep, acc = refs
    anchor_x, anchor_y = anchors(cells_x, cells_y)
    acc[...] = jnp.zeros(acc.shape, F32)

    def one(k, carry):
        rows = stay[:, pl.ds(pl.multiple_of(k * step, step), step)]
        column = (rows[5:6] - anchor_x) * cells_y + (rows[6:7] - anchor_y)
        acc[...] += lax.dot_general(
            spread(column, source_rows(rows), columns),
            depth_onehot(rows, dep.shape[3]),
            TRANSPOSED,
            preferred_element_type=F32,
        )
        return carry

    lax.fori_loop(*steps, one, 0)
    for f in range(5):
        for x in range(cells_x):
            high = slice((f * cells_x + x) * cells_y, (f * cells_x + x + 1) * cells_y)
            low = slice(5 * columns + high.start, 5 * columns + high.stop)
            value = acc[high, :] + acc[low, :]
            dep[f, x] = value if before is None else before[f, x] + value


def arrivals(rows, along, number, depth):
    left = spread(along, source_rows(rows), number)
    got = lax.dot_general(left, depth_onehot(rows, depth), TRANSPOSED, preferred_element_type=F32)
    return [
        got[f * number : (f + 1) * number] + got[(5 + f) * number : (6 + f) * number]
        for f in range(5)
    ]


def relay_kernel(
    cells_x, cells_y, in_even, in_odd, partial, own, leaving, _, even, odd, planes, halo
):
    depth = partial.shape[2]
    anchor_x, _ = anchors(cells_x, cells_y)
    got = receive_pair("gy", in_even, in_odd)
    parts = [unpack(g, depth) for g in got]
    for q, (rows, plane, _, _) in enumerate(parts):
        for f, value in enumerate(arrivals(rows, rows[5:6] - anchor_x, cells_x, depth)):
            planes[q, f] = value
        halo[q] = plane + leaving[2 + q]
    row = iota((cells_y, depth), 0)

    def side(x):
        value = partial[min(x, 1)] + jnp.where(row == 0, planes[0, 4, x : x + 1, :], 0.0)
        return value + jnp.where(row == cells_y - 1, planes[1, 4, x : x + 1, :], 0.0)

    up = message(own[1], side(cells_x - 1), parts[0][3], parts[1][3])
    down = message(own[0], side(0), parts[0][2], parts[1][2])
    send_pair("gx", even, odd, up, down)


def update_kernel(
    cells_x, cells_y, y_even, y_odd, x_even, x_odd, density, momentum, energy, dep,
    planes_y, halo_y, leaving, state_in, where_in,
    rho_out, impulse, energy_out, fastest, state, where_to, pressure, planes_x,
):
    depth = energy.shape[2]
    _, anchor_y = anchors(cells_x, cells_y)
    scale = ADIABATIC_INDEX - 1.0
    shape = (cells_y, depth)
    row = iota(shape, 0)
    lane = iota(shape, 1)
    parts = [unpack(g, depth) for g in receive_pair("gx", x_even, x_odd)]
    for q, (rows, plane, _, _) in enumerate(parts):
        for f, value in enumerate(arrivals(rows, rows[6:7] - anchor_y, cells_y, depth)):
            planes_x[q, f] = value
        pressure[q * (cells_x + 1)] = scale * (plane + leaving[q])
    row_x = iota((cells_x, depth), 0)
    halos = []
    for q in range(2):
        value = halo_y[q] + jnp.where(row_x == 0, parts[0][2 + q], 0.0)
        halos.append(scale * (value + jnp.where(row_x == cells_x - 1, parts[1][2 + q], 0.0)))
    tables = [parts[0][0], parts[1][0]] + [
        unpack(g, depth)[0] for g in receive_pair("gy", y_even, y_odd)
    ]
    for q, rows in enumerate(tables):
        lanes = slice(q * rows.shape[1], (q + 1) * rows.shape[1])
        state[:, lanes] = rows[0:5]
        where_to[:, lanes] = rows[5:8].astype(I32)

    def with_planes(f, x, value):
        if x == 0:
            value = value + planes_x[0, f]
        if x == cells_x - 1:
            value = value + planes_x[1, f]
        value = value + jnp.where(row == 0, planes_y[0, f, x : x + 1, :], 0.0)
        return value + jnp.where(row == cells_y - 1, planes_y[1, f, x : x + 1, :], 0.0)

    for x in range(cells_x):
        value = with_planes(4, x, energy[x] + dep[4, x])
        energy_out[x] = value
        pressure[x + 1] = scale * value
    top = jnp.zeros(shape, F32)
    for x in range(cells_x):
        here = pressure[x + 1]
        grad_x = 0.5 * (pressure[x + 2] - pressure[x])
        after = jnp.where(
            row == cells_y - 1, halos[1][x : x + 1, :], pltpu.roll(here, cells_y - 1, 0)
        )
        before = jnp.where(row == 0, halos[0][x : x + 1, :], pltpu.roll(here, 1, 0))
        grad_y = 0.5 * (after - before)
        after = jnp.where(lane == depth - 1, 0.0, pltpu.roll(here, depth - 1, 1))
        before = jnp.where(lane == 0, 0.0, pltpu.roll(here, 1, 1))
        grad_z = 0.5 * (after - before)
        rho = with_planes(0, x, density[x] + dep[0, x])
        rho_out[x] = rho
        largest = jnp.zeros(shape, F32)
        for k, grad in enumerate((grad_x, grad_y, grad_z)):
            value = with_planes(1 + k, x, momentum[k, x] + dep[1 + k, x]) - KICK * grad
            impulse[k, x] = value
            largest = jnp.maximum(largest, jnp.abs(value))
        wave = largest / rho + jnp.sqrt(ADIABATIC_INDEX * here / rho)
        top = jnp.maximum(top, wave)
    fastest[...] = jnp.broadcast_to(jnp.max(top, axis=(0, 1), keepdims=True), fastest.shape)


def call(
    kernel, outs, scratch=(), out_specs=None, in_specs=None, aliases=None, name=None, vmem=48, **extra
):
    if in_specs is not None:
        extra["in_specs"] = in_specs
    if out_specs is not None:
        extra["out_specs"] = out_specs
    return pl.pallas_call(
        kernel,
        out_shape=outs,
        scratch_shapes=list(scratch),
        input_output_aliases=aliases or {},
        compiler_params=pltpu.CompilerParams(vmem_limit_bytes=vmem * 1024 * 1024),
        name=name,
        **extra,
    )


def swap(axis, even, odd):
    size = lax.axis_size(axis)
    pairs = lambda first: [
        p for i in range(first, size - 1, 2) for p in ((i, i + 1), (i + 1, i))
    ]
    return lax.ppermute(even, axis, pairs(0)), lax.ppermute(odd, axis, pairs(1))


def on_device(
    density, momentum, energy, parcel_mass, droplet_velocity, parcel_temp, parcel_cell, parcel_count
):
    cells_x, cells_y, depth = density.shape
    rows = parcel_mass.shape[0]
    capacity = rows // 16
    chunks = rows // LANES
    columns = cells_x * cells_y
    step = min(1024, rows)
    sds = jax.ShapeDtypeStruct
    whole = pl.BlockSpec(memory_space=VMEM)
    parcels = sds((8, capacity + 3 * depth), F32)
    dense = sds((chunks, LANES), F32)
    place, stays, words, masks = call(
        functools.partial(rank_kernel, cells_x, cells_y),
        (dense, dense, sds((chunks, LANES), I32), sds((4, 3, chunks, LANES), F32)),
        scratch=(VMEM((chunks, LANES), I32), VMEM((chunks, LANES), I32)),
        in_specs=[pl.BlockSpec(memory_space=pltpu.SMEM), whole],
        name="rank",
        cost_estimate=pl.CostEstimate(flops=10**9, bytes_accessed=10**6, transcendentals=0),
    )(parcel_count, parcel_cell)
    even, odd, stay, own, leaving, partial = call(
        functools.partial(prep_kernel, cells_x, cells_y, step),
        (
            parcels,
            parcels,
            sds((8, rows), F32),
            sds((2, 8, capacity), F32),
            sds((4, cells_x, depth), F32),
            sds((2, cells_y, depth), F32),
        ),
        scratch=(
            VMEM((8, rows), F32),
            VMEM((chunks, 8, LANES), F32),
            pltpu.SMEM((chunks, LANES), I32),
            VMEM((4, capacity // LANES + 1, 8, LANES), F32),
            VMEM((4 * (cells_x + cells_y), depth), F32),
            pltpu.SemaphoreType.DMA,
        ),
        name="prep",
    )(
        parcel_mass.reshape(chunks, LANES),
        parcel_temp.reshape(chunks, LANES),
        droplet_velocity,
        parcel_cell,
        energy,
        place,
        stays,
        words,
        masks,
    )
    y_even, y_odd = swap("gy", even, odd)
    slots = rows + 4 * capacity
    five = sds((5, cells_x, cells_y, depth), F32)
    sums = (VMEM((10 * columns, depth), F32),)
    steps = rows // step
    middle = steps * 5 // 8
    dep, state, where_to = call(
        functools.partial(deposit_kernel, cells_x, cells_y, step, (0, middle)),
        (five, sds((5, slots), F32), sds((3, slots), I32)),
        scratch=sums,
        name="deposit1",
    )(stay)
    even, odd, planes_y, halo_y = call(
        functools.partial(relay_kernel, cells_x, cells_y),
        (parcels, parcels, sds((2, 5, cells_x, depth), F32), sds((2, cells_x, depth), F32)),
        in_specs=[whole] * 5 + [pl.BlockSpec(memory_space=pl.ANY)],
        name="relay",
    )(y_even, y_odd, partial, own, leaving, dep)
    x_even, x_odd = swap("gx", even, odd)
    (dep,) = call(
        functools.partial(deposit_kernel, cells_x, cells_y, step, (middle, steps)),
        (five,),
        scratch=sums,
        in_specs=[whole, whole, pl.BlockSpec(memory_space=pl.ANY)],
        name="deposit2",
    )(stay, dep, halo_y)
    last = rows // (4 * capacity)
    rho, impulse, energy_out, top, state, where_to = call(
        functools.partial(update_kernel, cells_x, cells_y),
        (
            sds(density.shape, F32),
            sds(momentum.shape, F32),
            sds(energy.shape, F32),
            sds((lax.axis_size(("gx", "gy")), LANES), F32),
            sds(state.shape, F32),
            sds(where_to.shape, I32),
        ),
        scratch=(
            VMEM((cells_x + 2, cells_y, depth), F32),
            VMEM((2, 5, cells_y, depth), F32),
        ),
        in_specs=[whole] * 11 + [pl.BlockSpec(memory_space=pl.ANY)] * 2,
        out_specs=(whole,) * 4
        + (
            pl.BlockSpec((5, 4 * capacity), lambda i: (0, last)),
            pl.BlockSpec((3, 4 * capacity), lambda i: (0, last)),
        ),
        aliases={11: 4, 12: 5},
        grid=(1,),
        name="update",
    )(
        y_even, y_odd, x_even, x_odd, density, momentum, energy, dep,
        planes_y, halo_y, leaving, state, where_to,
    )
    fastest = jnp.max(lax.all_to_all(top, ("gx", "gy"), 0, 0, tiled=True), axis=0)[0]
    return rho, impulse, energy_out, state, where_to, COURANT / fastest


def solution(mesh):
    both = ("gx", "gy")
    return jax.shard_map(
        on_device,
        mesh=mesh,
        in_specs=(
            P("gx", "gy", None),
            P(None, "gx", "gy", None),
            P("gx", "gy", None),
            P(both),
            P(None, both),
            P(both),
            P(None, both),
            P(both),
        ),
        out_specs=(
            P("gx", "gy", None),
            P(None, "gx", "gy", None),
            P("gx", "gy", None),
            P(None, both),
            P(None, both),
            P(),
        ),
        check_vma=False,
    )
```

```python
import functools

import jax
import jax.numpy as jnp
from jax import lax
from jax.experimental import pallas as pl
from jax.experimental.pallas import tpu as pltpu
from jax.sharding import PartitionSpec as P


ADIABATIC_INDEX = 1.4
KICK = 0.25
COURANT = 0.4
SHRINK = 0.5

F32 = jnp.float32
BF16 = jnp.bfloat16
I32 = jnp.int32
LANES = 128
VMEM = pltpu.VMEM
TRANSPOSED = (((1,), (1,)), ((), ()))


def iota(shape, dim, dtype=I32):
    return lax.broadcasted_iota(dtype, shape, dim)


def sigmoid_of(temp):
    return 1.0 / (1.0 + jnp.exp(-2.0 * (temp - 2.0)))


def rank_kernel(cells_x, cells_y, count, cell, place, stays, words, masks, cx, cy):
    chunks = place.shape[0]
    anchor_x = lax.axis_index("gx") * cells_x
    anchor_y = lax.axis_index("gy") * cells_y
    for b in range(chunks):
        lanes = slice(b * LANES, (b + 1) * LANES)
        cx[b : b + 1, :] = cell[0:1, lanes]
        cy[b : b + 1, :] = cell[1:2, lanes]
    shape = (chunks, LANES)
    lane = iota(shape, 1)
    live = iota(shape, 0) * LANES + lane < count[0]
    local_x = cx[...] - anchor_x
    local_y = cy[...] - anchor_y
    heading = jnp.where(
        local_x < 0,
        0,
        jnp.where(
            local_x >= cells_x, 1, jnp.where(local_y < 0, 2, jnp.where(local_y >= cells_y, 3, 4))
        ),
    )
    heading = jnp.where(live, heading, 5)
    hits = [jnp.where(heading == h, 1.0, 0.0) for h in range(4)]
    lane_r = iota((LANES, 2 * LANES), 0)
    lane_c = iota((LANES, 2 * LANES), 1)
    scan = jnp.where((lane_r < lane_c) | (lane_c >= LANES), 1.0, 0.0).astype(BF16)
    both = jnp.dot(jnp.concatenate(hits, axis=0).astype(BF16), scan, preferred_element_type=F32)
    inner = [both[h * chunks : (h + 1) * chunks, :LANES] for h in range(4)]
    total = [both[h * chunks : (h + 1) * chunks, LANES:] for h in range(4)]
    below = jnp.where(iota((chunks, chunks), 1) < iota((chunks, chunks), 0), 1.0, 0.0).astype(BF16)
    base = jnp.dot(
        below, jnp.concatenate(total, axis=1).astype(BF16), preferred_element_type=F32
    ).astype(I32)
    offset = jnp.zeros(shape, F32)
    spot = jnp.full(shape, -1.0, F32)
    word = jnp.zeros(shape, I32)
    for h in range(4):
        spot = jnp.where(heading == h, inner[h] + offset, spot)
        start = base[:, h * LANES : (h + 1) * LANES]
        within = start & (LANES - 1)
        end = within + total[h].astype(I32)
        turn = (start - offset.astype(I32)) & (LANES - 1)
        word = jnp.where(lane == h, (start >> 7) * LANES + turn, word)
        last = start + total[h].astype(I32)
        word = jnp.where(lane == 4 + h, last >> 7, word)
        masks[h, 0] = jnp.where((lane >= within) & (lane < end), 1.0, 0.0)
        masks[h, 1] = jnp.where(lane < end - LANES, 1.0, 0.0)
        masks[h, 2] = jnp.where(end >= LANES, 1.0, 0.0)
        offset = offset + total[h]
    words[...] = word
    place[...] = spot
    stays[...] = jnp.where(heading == 4, 1.0, 0.0)


def prep_kernel(
    cells_x, cells_y, step, mass, temp, vel, cell, energy, pos, stays, words, masks,
    even, odd, stay, own, leaving, partial,
    pay, compact, table, tiles, acc, sem,
):
    load = pltpu.make_async_copy(words, table, sem)
    load.start()
    chunks = mass.shape[0]
    anchor_xf, anchor_yf = anchors(cells_x, cells_y)
    kept = mass[...] * (1.0 - SHRINK * sigmoid_of(temp[...]))
    pay[1:4, :] = vel[...]
    pay[5:8, :] = cell[...].astype(F32)
    for b in range(chunks):
        lanes = slice(b * LANES, (b + 1) * LANES)
        pay[0:1, lanes] = kept[b : b + 1, :]
        pay[4:5, lanes] = temp[b : b + 1, :]
    for b in range(chunks):
        lanes = slice(b * LANES, (b + 1) * LANES)
        stay[:, lanes] = jnp.where(stays[b : b + 1, :] > 0.0, pay[:, lanes], 0.0)
    group = 16

    def pack(g, carry):
        for u in range(group):
            b = g * group + u
            slots = pos[pl.ds(b, 1), :]
            onehot = jnp.where(slots == iota((LANES, LANES), 0).astype(F32), 1.0, 0.0).astype(BF16)
            rows = pay[:, pl.ds(pl.multiple_of(b * LANES, LANES), LANES)]
            high = rows.astype(BF16).astype(F32)
            rest = rows - high
            middle = rest.astype(BF16).astype(F32)
            low = rest - middle
            parts = jnp.concatenate([high, middle, low, jnp.zeros_like(low)], axis=0).astype(BF16)
            got = lax.dot_general(parts, onehot, TRANSPOSED, preferred_element_type=F32)
            compact[b] = got[0:8] + got[8:16] + got[16:24]
        return carry

    lax.fori_loop(0, chunks // group, pack, 0)
    tiles[...] = jnp.zeros(tiles.shape, F32)
    load.wait()
    unroll = 8

    def place_all(g, carry):
        carry = list(carry)
        for u in range(unroll):
            b = g * unroll + u
            rows = compact[b]
            for h in range(4):
                word = table[b, h]
                turned = pltpu.roll(rows, word & (LANES - 1), 1)
                merged = jnp.where(masks[h, 0, pl.ds(b, 1), :] > 0.0, turned, carry[h])
                tiles[h, word >> 7] = merged
                rest = jnp.where(masks[h, 2, pl.ds(b, 1), :] > 0.0, 0.0, merged)
                carry[h] = jnp.where(masks[h, 1, pl.ds(b, 1), :] > 0.0, turned, rest)
        return tuple(carry)

    carry = lax.fori_loop(
        0, chunks // unroll, place_all, tuple(jnp.zeros((8, LANES), F32) for _ in range(4))
    )
    for h in range(4):
        tiles[h, table[chunks - 1, 4 + h]] = carry[h]
    width = own.shape[2]
    buckets = [
        jnp.concatenate([tiles[h, t] for t in range(width // LANES)], axis=1) for h in range(4)
    ]
    for h in range(4):
        along = (buckets[h][6:7] - anchor_yf) if h < 2 else (buckets[h][5:6] - anchor_xf)
        number = cells_y if h < 2 else cells_x
        leaving[h] = one_field(buckets[h], along, number, acc.shape[1], 4)
    for h in range(2):
        own[h] = buckets[h]
    outer_energy(cells_x, cells_y, anchor_xf, anchor_yf, step, stay, acc)
    planes = [acc[q * 2 * cells_y : (q * 2 + 1) * cells_y] + acc[(q * 2 + 1) * cells_y : (q * 2 + 2) * cells_y] for q in range(4)]
    partial[0] = energy[0] + planes[0]
    partial[1] = energy[cells_x - 1] + planes[1]
    up = message(
        buckets[3], energy[:, cells_y - 1, :] + planes[3], leaving[0, -1:, :], leaving[1, -1:, :]
    )
    down = message(buckets[2], energy[:, 0, :] + planes[2], leaving[0, 0:1, :], leaving[1, 0:1, :])
    send_pair("gy", even, odd, up, down)


def message(bucket, plane, first, second):
    half = plane.shape[0] // 2
    rest = jnp.zeros((6, plane.shape[1]), F32)
    return jnp.concatenate(
        [bucket, plane[:half], plane[half:], jnp.concatenate([first, second, rest], axis=0)], axis=1
    )


def unpack(got, depth):
    width = got.shape[1] - 3 * depth
    plane = jnp.concatenate(
        [got[:, width : width + depth], got[:, width + depth : width + 2 * depth]], axis=0
    )
    corner = got[:, width + 2 * depth :]
    return got[:, :width], plane, corner[0:1], corner[1:2]


def send_pair(axis, even, odd, up, down):
    is_even = (lax.axis_index(axis) & 1) == 0
    even[...] = jnp.where(is_even, up, down)
    odd[...] = jnp.where(is_even, down, up)


def receive_pair(axis, even, odd):
    is_even = (lax.axis_index(axis) & 1) == 0
    return jnp.where(is_even, odd[...], even[...]), jnp.where(is_even, even[...], odd[...])


def anchors(cells_x, cells_y):
    return (
        (lax.axis_index("gx") * cells_x).astype(F32),
        (lax.axis_index("gy") * cells_y).astype(F32),
    )


def source_rows(rows):
    kept, temp = rows[0:1], rows[4:5]
    v0, v1, v2 = rows[1:2], rows[2:3], rows[3:4]
    share = sigmoid_of(temp)
    gone = kept * share / (1.0 - SHRINK * share)
    heat = temp + 0.5 * (v0 * v0 + v1 * v1 + v2 * v2)
    fields = [gone, gone * v0, gone * v1, gone * v2, gone * heat]
    high = [f.astype(BF16).astype(F32) for f in fields]
    low = [f - g for f, g in zip(fields, high)]
    return high + low


def spread(columns, sources, number):
    n = columns.shape[1]
    hot = jnp.where(columns == iota((number, n), 0).astype(F32), 1.0, 0.0).astype(BF16)
    hot = hot.reshape(number // 16, 16, n)
    parts = []
    for source in sources:
        value = jnp.broadcast_to(source, (16, n)).astype(BF16)
        parts.append((hot * value[None]).reshape(number, n))
    return jnp.concatenate(parts, axis=0)


def depth_onehot(rows, depth):
    n = rows.shape[1]
    return jnp.where(rows[7:8] == iota((depth, n), 0).astype(F32), 1.0, 0.0).astype(BF16)


def outer_energy(cells_x, cells_y, anchor_x, anchor_y, step, stay, acc):
    total = stay.shape[1]
    depth = acc.shape[1]
    acc[...] = jnp.zeros(acc.shape, F32)

    def one(k, carry):
        rows = stay[:, pl.ds(pl.multiple_of(k * step, step), step)]
        x = rows[5:6] - anchor_x
        y = rows[6:7] - anchor_y
        sources = source_rows(rows)
        pair = (sources[4], sources[9])
        on_x = [jnp.where(x == at, v, 0.0) for at in (0.0, cells_x - 1.0) for v in pair]
        on_y = [jnp.where(y == at, v, 0.0) for at in (0.0, cells_y - 1.0) for v in pair]
        left = jnp.concatenate([spread(y, on_x, cells_y), spread(x, on_y, cells_x)], axis=0)
        acc[...] += lax.dot_general(
            left, depth_onehot(rows, depth), TRANSPOSED, preferred_element_type=F32
        )
        return carry

    lax.fori_loop(0, total // step, one, 0)


def one_field(rows, along, number, depth, f):
    sources = source_rows(rows)
    left = spread(along, [sources[f], sources[5 + f]], number)
    got = lax.dot_general(left, depth_onehot(rows, depth), TRANSPOSED, preferred_element_type=F32)
    return got[:number] + got[number:]


def deposit_kernel(cells_x, cells_y, step, steps, *refs):
    columns = cells_x * cells_y
    if steps[0] == 0:
        stay, dep, state, where_to = refs
        total = stay.shape[1]
        state[:, :total] = stay[0:5, :]
        where_to[:, :total] = stay[5:8, :].astype(I32)
        dep[...] = jnp.zeros(dep.shape, F32)
    else:
        stay, before, _, dep = refs
        dep[...] = before[...]
    anchor_x, anchor_y = anchors(cells_x, cells_y)

    def one(k, carry):
        rows = stay[:, pl.ds(pl.multiple_of(k * step, step), step)]
        column = (rows[5:6] - anchor_x) * cells_y + (rows[6:7] - anchor_y)
        sources = source_rows(rows)
        onehot = depth_onehot(rows, dep.shape[1])
        left = [spread(column, half, columns) for half in (sources[:5], sources[5:])]
        dep[...] += lax.dot_general(
            jnp.concatenate(left, axis=1),
            jnp.concatenate([onehot, onehot], axis=1),
            TRANSPOSED,
            preferred_element_type=F32,
        )
        return carry

    lax.fori_loop(*steps, one, 0)


def arrivals(rows, along, number, depth):
    left = spread(along, source_rows(rows), number)
    got = lax.dot_general(left, depth_onehot(rows, depth), TRANSPOSED, preferred_element_type=F32)
    return [
        got[f * number : (f + 1) * number] + got[(5 + f) * number : (6 + f) * number]
        for f in range(5)
    ]


def relay_kernel(
    cells_x, cells_y, in_even, in_odd, partial, own, leaving, _, even, odd, planes, halo
):
    depth = partial.shape[2]
    anchor_x, _ = anchors(cells_x, cells_y)
    got = receive_pair("gy", in_even, in_odd)
    parts = [unpack(g, depth) for g in got]
    for q, (rows, plane, _, _) in enumerate(parts):
        for f, value in enumerate(arrivals(rows, rows[5:6] - anchor_x, cells_x, depth)):
            planes[q, f] = value
        halo[q] = plane + leaving[2 + q]
    row = iota((cells_y, depth), 0)

    def side(x):
        value = partial[min(x, 1)] + jnp.where(row == 0, planes[0, 4, x : x + 1, :], 0.0)
        return value + jnp.where(row == cells_y - 1, planes[1, 4, x : x + 1, :], 0.0)

    up = message(own[1], side(cells_x - 1), parts[0][3], parts[1][3])
    down = message(own[0], side(0), parts[0][2], parts[1][2])
    send_pair("gx", even, odd, up, down)


def update_kernel(
    cells_x, cells_y, y_even, y_odd, x_even, x_odd, density, momentum, energy, dep,
    planes_y, halo_y, leaving, state_in, where_in,
    rho_there, impulse_there, energy_there, fastest, state, where_to,
    pressure, planes_x, rho_out, impulse, energy_out, sems,
):
    depth = energy.shape[2]
    _, anchor_y = anchors(cells_x, cells_y)
    scale = ADIABATIC_INDEX - 1.0
    shape = (cells_y, depth)
    row = iota(shape, 0)
    lane = iota(shape, 1)
    parts = [unpack(g, depth) for g in receive_pair("gx", x_even, x_odd)]
    for q, (rows, plane, _, _) in enumerate(parts):
        for f, value in enumerate(arrivals(rows, rows[6:7] - anchor_y, cells_y, depth)):
            planes_x[q, f] = value
        pressure[q * (cells_x + 1)] = scale * (plane + leaving[q])
    row_x = iota((cells_x, depth), 0)
    halos = []
    for q in range(2):
        value = halo_y[q] + jnp.where(row_x == 0, parts[0][2 + q], 0.0)
        halos.append(scale * (value + jnp.where(row_x == cells_x - 1, parts[1][2 + q], 0.0)))
    tables = [parts[0][0], parts[1][0]] + [
        unpack(g, depth)[0] for g in receive_pair("gy", y_even, y_odd)
    ]
    for q, rows in enumerate(tables):
        lanes = slice(q * rows.shape[1], (q + 1) * rows.shape[1])
        state[:, lanes] = rows[0:5]
        where_to[:, lanes] = rows[5:8].astype(I32)

    def with_planes(f, x, value):
        if x == 0:
            value = value + planes_x[0, f]
        if x == cells_x - 1:
            value = value + planes_x[1, f]
        value = value + jnp.where(row == 0, planes_y[0, f, x : x + 1, :], 0.0)
        return value + jnp.where(row == cells_y - 1, planes_y[1, f, x : x + 1, :], 0.0)

    for x in range(cells_x):
        value = with_planes(4, x, energy[x] + dep[4, x])
        energy_out[x] = value
        pressure[x + 1] = scale * value
    leaves = [pltpu.make_async_copy(energy_out, energy_there, sems.at[0])]
    leaves[0].start()
    group = 4
    top = jnp.zeros(shape, F32)
    for x in range(cells_x):
        here = pressure[x + 1]
        grad_x = 0.5 * (pressure[x + 2] - pressure[x])
        after = jnp.where(
            row == cells_y - 1, halos[1][x : x + 1, :], pltpu.roll(here, cells_y - 1, 0)
        )
        before = jnp.where(row == 0, halos[0][x : x + 1, :], pltpu.roll(here, 1, 0))
        grad_y = 0.5 * (after - before)
        after = jnp.where(lane == depth - 1, 0.0, pltpu.roll(here, depth - 1, 1))
        before = jnp.where(lane == 0, 0.0, pltpu.roll(here, 1, 1))
        grad_z = 0.5 * (after - before)
        rho = with_planes(0, x, density[x] + dep[0, x])
        rho_out[x] = rho
        largest = jnp.zeros(shape, F32)
        for k, grad in enumerate((grad_x, grad_y, grad_z)):
            value = with_planes(1 + k, x, momentum[k, x] + dep[1 + k, x]) - KICK * grad
            impulse[k, x] = value
            largest = jnp.maximum(largest, jnp.abs(value))
        wave = largest / rho + jnp.sqrt(ADIABATIC_INDEX * here / rho)
        top = jnp.maximum(top, wave)
        if (x + 1) % group == 0:
            some = pl.ds(x + 1 - group, group)
            for here, there in (
                (rho_out.at[some], rho_there.at[some]),
                (impulse.at[:, some], impulse_there.at[:, some]),
            ):
                leaves.append(pltpu.make_async_copy(here, there, sems.at[len(leaves)]))
                leaves[-1].start()
    fastest[...] = jnp.broadcast_to(jnp.max(top, axis=(0, 1), keepdims=True), fastest.shape)
    for leave in leaves:
        leave.wait()


def call(kernel, outs, scratch=(), out_specs=None, in_specs=None, aliases=None, vmem=48, **extra):
    if in_specs is not None:
        extra["in_specs"] = in_specs
    if out_specs is not None:
        extra["out_specs"] = out_specs
    return pl.pallas_call(
        kernel,
        out_shape=outs,
        scratch_shapes=list(scratch),
        input_output_aliases=aliases or {},
        compiler_params=pltpu.CompilerParams(vmem_limit_bytes=vmem * 1024 * 1024),
        **extra,
    )


def swap(axis, even, odd):
    size = lax.axis_size(axis)
    pairs = lambda first: [
        p for i in range(first, size - 1, 2) for p in ((i, i + 1), (i + 1, i))
    ]
    odd = lax.ppermute(odd, axis, pairs(1))
    even = lax.ppermute(even, axis, pairs(0))
    return even, odd


def on_device(
    density, momentum, energy, parcel_mass, droplet_velocity, parcel_temp, parcel_cell, parcel_count
):
    cells_x, cells_y, depth = density.shape
    rows = parcel_mass.shape[0]
    capacity = rows // 16
    chunks = rows // LANES
    columns = cells_x * cells_y
    step = min(1024, rows)
    sds = jax.ShapeDtypeStruct
    whole = pl.BlockSpec(memory_space=VMEM)
    parcels = sds((8, capacity + 3 * depth), F32)
    dense = sds((chunks, LANES), F32)
    place, stays, words, masks = call(
        functools.partial(rank_kernel, cells_x, cells_y),
        (dense, dense, sds((chunks, LANES), I32), sds((4, 3, chunks, LANES), F32)),
        scratch=(VMEM((chunks, LANES), I32), VMEM((chunks, LANES), I32)),
        in_specs=[pl.BlockSpec(memory_space=pltpu.SMEM), whole],
        cost_estimate=pl.CostEstimate(flops=10**9, bytes_accessed=10**6, transcendentals=0),
    )(parcel_count, parcel_cell)
    even, odd, stay, own, leaving, partial = call(
        functools.partial(prep_kernel, cells_x, cells_y, step),
        (
            parcels,
            parcels,
            sds((8, rows), F32),
            sds((2, 8, capacity), F32),
            sds((4, cells_x, depth), F32),
            sds((2, cells_y, depth), F32),
        ),
        scratch=(
            VMEM((8, rows), F32),
            VMEM((chunks, 8, LANES), F32),
            pltpu.SMEM((chunks, LANES), I32),
            VMEM((4, capacity // LANES + 1, 8, LANES), F32),
            VMEM((4 * (cells_x + cells_y), depth), F32),
            pltpu.SemaphoreType.DMA,
        ),
    )(
        parcel_mass.reshape(chunks, LANES),
        parcel_temp.reshape(chunks, LANES),
        droplet_velocity,
        parcel_cell,
        energy,
        place,
        stays,
        words,
        masks,
    )
    y_even, y_odd = swap("gy", even, odd)
    slots = rows + 4 * capacity
    five = sds((5 * columns, depth), F32)
    steps = rows // step
    middle = steps * 5 // 8
    dep, state, where_to = call(
        functools.partial(deposit_kernel, cells_x, cells_y, step, (0, middle)),
        (five, sds((5, slots), F32), sds((3, slots), I32)),
    )(stay)
    even, odd, planes_y, halo_y = call(
        functools.partial(relay_kernel, cells_x, cells_y),
        (parcels, parcels, sds((2, 5, cells_x, depth), F32), sds((2, cells_x, depth), F32)),
        in_specs=[whole] * 5 + [pl.BlockSpec(memory_space=pl.ANY)],
    )(y_even, y_odd, partial, own, leaving, dep)
    x_even, x_odd = swap("gx", even, odd)
    (dep,) = call(
        functools.partial(deposit_kernel, cells_x, cells_y, step, (middle, steps)),
        (five,),
        in_specs=[whole, whole, pl.BlockSpec(memory_space=pl.ANY)],
        aliases={1: 0},
    )(stay, dep, halo_y)
    dep = dep.reshape(5, cells_x, cells_y, depth)
    last = rows // (4 * capacity)
    rho, impulse, energy_out, top, state, where_to = call(
        functools.partial(update_kernel, cells_x, cells_y),
        (
            sds(density.shape, F32),
            sds(momentum.shape, F32),
            sds(energy.shape, F32),
            sds((lax.axis_size(("gx", "gy")), LANES), F32),
            sds(state.shape, F32),
            sds(where_to.shape, I32),
        ),
        scratch=(
            VMEM((cells_x + 2, cells_y, depth), F32),
            VMEM((2, 5, cells_y, depth), F32),
            VMEM(density.shape, F32),
            VMEM(momentum.shape, F32),
            VMEM(energy.shape, F32),
            pltpu.SemaphoreType.DMA((1 + 2 * (cells_x // 4),)),
        ),
        in_specs=[whole] * 11 + [pl.BlockSpec(memory_space=pl.ANY)] * 2,
        out_specs=(pl.BlockSpec(memory_space=pl.ANY),) * 3
        + (whole,)
        + (
            pl.BlockSpec((5, 4 * capacity), lambda i: (0, last)),
            pl.BlockSpec((3, 4 * capacity), lambda i: (0, last)),
        ),
        aliases={11: 4, 12: 5},
        grid=(1,),
    )(
        y_even, y_odd, x_even, x_odd, density, momentum, energy, dep,
        planes_y, halo_y, leaving, state, where_to,
    )
    fastest = jnp.max(lax.all_to_all(top, ("gx", "gy"), 0, 0, tiled=True), axis=0)[0]
    return rho, impulse, energy_out, state, where_to, COURANT / fastest


def solution(mesh):
    both = ("gx", "gy")
    return jax.shard_map(
        on_device,
        mesh=mesh,
        in_specs=(
            P("gx", "gy", None),
            P(None, "gx", "gy", None),
            P("gx", "gy", None),
            P(both),
            P(None, both),
            P(both),
            P(None, both),
            P(both),
        ),
        out_specs=(
            P("gx", "gy", None),
            P(None, "gx", "gy", None),
            P("gx", "gy", None),
            P(None, both),
            P(None, both),
            P(),
        ),
        check_vma=False,
    )
```

```python
import functools

import jax
import jax.numpy as jnp
from jax import lax
from jax.experimental import pallas as pl
from jax.experimental.pallas import tpu as pltpu
from jax.sharding import PartitionSpec as P


ADIABATIC_INDEX = 1.4
KICK = 0.25
COURANT = 0.4
SHRINK = 0.5

F32 = jnp.float32
BF16 = jnp.bfloat16
I32 = jnp.int32
LANES = 128
KINDS = 6
VMEM = pltpu.VMEM
TRANSPOSED = (((1,), (1,)), ((), ()))


def iota(shape, dim, dtype=I32):
    return lax.broadcasted_iota(dtype, shape, dim)


def sigmoid_of(temp):
    return 1.0 / (1.0 + jnp.exp(-2.0 * (temp - 2.0)))


def rank_kernel(cells_x, cells_y, count, cell, place, stays, words, masks, numbers, cx, cy):
    chunks = place.shape[0]
    anchor_x = lax.axis_index("gx") * cells_x
    anchor_y = lax.axis_index("gy") * cells_y
    for b in range(chunks):
        lanes = slice(b * LANES, (b + 1) * LANES)
        cx[b : b + 1, :] = cell[0:1, lanes]
        cy[b : b + 1, :] = cell[1:2, lanes]
    shape = (chunks, LANES)
    lane = iota(shape, 1)
    live = iota(shape, 0) * LANES + lane < count[0]
    local_x = cx[...] - anchor_x
    local_y = cy[...] - anchor_y
    heading = jnp.where(
        local_x < 0,
        0,
        jnp.where(
            local_x >= cells_x, 1, jnp.where(local_y < 0, 2, jnp.where(local_y >= cells_y, 3, 4))
        ),
    )
    heading = jnp.where((heading == 4) & (local_x >= cells_x // 2), 5, heading)
    heading = jnp.where(live, heading, KINDS)
    hits = [jnp.where(heading == h, 1.0, 0.0) for h in range(KINDS)]
    lane_r = iota((LANES, 2 * LANES), 0)
    lane_c = iota((LANES, 2 * LANES), 1)
    scan = jnp.where((lane_r < lane_c) | (lane_c >= LANES), 1.0, 0.0).astype(BF16)
    both = jnp.dot(jnp.concatenate(hits, axis=0).astype(BF16), scan, preferred_element_type=F32)
    inner = [both[h * chunks : (h + 1) * chunks, :LANES] for h in range(KINDS)]
    total = [both[h * chunks : (h + 1) * chunks, LANES:] for h in range(KINDS)]
    below = jnp.where(iota((chunks, chunks), 1) < iota((chunks, chunks), 0), 1.0, 0.0).astype(BF16)
    base = jnp.dot(
        below, jnp.concatenate(total, axis=1).astype(BF16), preferred_element_type=F32
    ).astype(I32)
    offset = jnp.zeros(shape, F32)
    spot = jnp.full(shape, -1.0, F32)
    word = jnp.zeros(shape, I32)
    number = jnp.zeros((1, LANES), I32)
    for h in range(KINDS):
        spot = jnp.where(heading == h, inner[h] + offset, spot)
        start = base[:, h * LANES : (h + 1) * LANES]
        within = start & (LANES - 1)
        end = within + total[h].astype(I32)
        turn = (start - offset.astype(I32)) & (LANES - 1)
        word = jnp.where(lane == h, (start >> 7) * LANES + turn, word)
        last = start + total[h].astype(I32)
        word = jnp.where(lane == KINDS + h, last >> 7, word)
        number = jnp.where(lane[0:1] == h, last[chunks - 1 :], number)
        masks[h, 0] = jnp.where((lane >= within) & (lane < end), 1.0, 0.0)
        masks[h, 1] = jnp.where(lane < end - LANES, 1.0, 0.0)
        masks[h, 2] = jnp.where(end >= LANES, 1.0, 0.0)
        offset = offset + total[h]
    words[...] = word
    numbers[...] = number
    place[...] = spot
    stays[...] = jnp.where((heading == 4) | (heading == 5), 1.0, 0.0)


def prep_kernel(
    cells_x, cells_y, step, mass, temp, vel, cell, energy, pos, stays, words, masks,
    even, odd, stay, own, leaving, partial, low, high,
    pay, compact, table, tiles, acc, sem,
):
    load = pltpu.make_async_copy(words, table, sem)
    load.start()
    chunks = mass.shape[0]
    anchor_xf, anchor_yf = anchors(cells_x, cells_y)
    kept = mass[...] * (1.0 - SHRINK * sigmoid_of(temp[...]))
    pay[1:4, :] = vel[...]
    pay[5:8, :] = cell[...].astype(F32)
    for b in range(chunks):
        lanes = slice(b * LANES, (b + 1) * LANES)
        pay[0:1, lanes] = kept[b : b + 1, :]
        pay[4:5, lanes] = temp[b : b + 1, :]
    for b in range(chunks):
        lanes = slice(b * LANES, (b + 1) * LANES)
        stay[:, lanes] = jnp.where(stays[b : b + 1, :] > 0.0, pay[:, lanes], 0.0)
    group = 16

    def pack(g, carry):
        for u in range(group):
            b = g * group + u
            slots = pos[pl.ds(b, 1), :]
            onehot = jnp.where(slots == iota((LANES, LANES), 0).astype(F32), 1.0, 0.0).astype(BF16)
            rows = pay[:, pl.ds(pl.multiple_of(b * LANES, LANES), LANES)]
            first = rows.astype(BF16).astype(F32)
            rest = rows - first
            middle = rest.astype(BF16).astype(F32)
            last = rest - middle
            parts = jnp.concatenate([first, middle, last, jnp.zeros_like(last)], axis=0).astype(BF16)
            got = lax.dot_general(parts, onehot, TRANSPOSED, preferred_element_type=F32)
            compact[b] = got[0:8] + got[8:16] + got[16:24]
        return carry

    lax.fori_loop(0, chunks // group, pack, 0)
    for ref in (tiles, low, high):
        ref[...] = jnp.zeros(ref.shape, F32)
    lists = [tiles.at[h] for h in range(4)] + [low, high]
    load.wait()
    unroll = 8

    def place_all(g, carry):
        carry = list(carry)
        for u in range(unroll):
            b = g * unroll + u
            rows = compact[b]
            for h in range(KINDS):
                word = table[b, h]
                turned = pltpu.roll(rows, word & (LANES - 1), 1)
                merged = jnp.where(masks[h, 0, pl.ds(b, 1), :] > 0.0, turned, carry[h])
                lists[h][word >> 7] = merged
                rest = jnp.where(masks[h, 2, pl.ds(b, 1), :] > 0.0, 0.0, merged)
                carry[h] = jnp.where(masks[h, 1, pl.ds(b, 1), :] > 0.0, turned, rest)
        return tuple(carry)

    carry = lax.fori_loop(
        0, chunks // unroll, place_all, tuple(jnp.zeros((8, LANES), F32) for _ in range(KINDS))
    )
    for h in range(KINDS):
        lists[h][table[chunks - 1, KINDS + h]] = carry[h]
    width = own.shape[2]
    buckets = [
        jnp.concatenate([tiles[h, t] for t in range(width // LANES)], axis=1) for h in range(4)
    ]
    for h in range(4):
        along = (buckets[h][6:7] - anchor_yf) if h < 2 else (buckets[h][5:6] - anchor_xf)
        number = cells_y if h < 2 else cells_x
        leaving[h] = one_field(buckets[h], along, number, acc.shape[1], 4)
    for h in range(2):
        own[h] = buckets[h]
    outer_energy(cells_x, cells_y, anchor_xf, anchor_yf, step, stay, acc)
    planes = [acc[q * 2 * cells_y : (q * 2 + 1) * cells_y] + acc[(q * 2 + 1) * cells_y : (q * 2 + 2) * cells_y] for q in range(4)]
    partial[0] = energy[0] + planes[0]
    partial[1] = energy[cells_x - 1] + planes[1]
    up = message(
        buckets[3], energy[:, cells_y - 1, :] + planes[3], leaving[0, -1:, :], leaving[1, -1:, :]
    )
    down = message(buckets[2], energy[:, 0, :] + planes[2], leaving[0, 0:1, :], leaving[1, 0:1, :])
    send_pair("gy", even, odd, up, down)


def message(bucket, plane, first, second):
    half = plane.shape[0] // 2
    rest = jnp.zeros((6, plane.shape[1]), F32)
    return jnp.concatenate(
        [bucket, plane[:half], plane[half:], jnp.concatenate([first, second, rest], axis=0)], axis=1
    )


def unpack(got, depth):
    width = got.shape[1] - 3 * depth
    plane = jnp.concatenate(
        [got[:, width : width + depth], got[:, width + depth : width + 2 * depth]], axis=0
    )
    corner = got[:, width + 2 * depth :]
    return got[:, :width], plane, corner[0:1], corner[1:2]


def send_pair(axis, even, odd, up, down):
    is_even = (lax.axis_index(axis) & 1) == 0
    even[...] = jnp.where(is_even, up, down)
    odd[...] = jnp.where(is_even, down, up)


def receive_pair(axis, even, odd):
    is_even = (lax.axis_index(axis) & 1) == 0
    return jnp.where(is_even, odd[...], even[...]), jnp.where(is_even, even[...], odd[...])


def anchors(cells_x, cells_y):
    return (
        (lax.axis_index("gx") * cells_x).astype(F32),
        (lax.axis_index("gy") * cells_y).astype(F32),
    )


def source_rows(rows):
    kept, temp = rows[0:1], rows[4:5]
    v0, v1, v2 = rows[1:2], rows[2:3], rows[3:4]
    share = sigmoid_of(temp)
    gone = kept * share / (1.0 - SHRINK * share)
    heat = temp + 0.5 * (v0 * v0 + v1 * v1 + v2 * v2)
    fields = [gone, gone * v0, gone * v1, gone * v2, gone * heat]
    high = [f.astype(BF16).astype(F32) for f in fields]
    low = [f - g for f, g in zip(fields, high)]
    return high + low


def spread(columns, sources, number):
    n = columns.shape[1]
    hot = jnp.where(columns == iota((number, n), 0).astype(F32), 1.0, 0.0).astype(BF16)
    hot = hot.reshape(number // 16, 16, n)
    parts = []
    for source in sources:
        value = jnp.broadcast_to(source, (16, n)).astype(BF16)
        parts.append((hot * value[None]).reshape(number, n))
    return jnp.concatenate(parts, axis=0)


def depth_onehot(rows, depth):
    n = rows.shape[1]
    return jnp.where(rows[7:8] == iota((depth, n), 0).astype(F32), 1.0, 0.0).astype(BF16)


def outer_energy(cells_x, cells_y, anchor_x, anchor_y, step, stay, acc):
    total = stay.shape[1]
    depth = acc.shape[1]
    acc[...] = jnp.zeros(acc.shape, F32)

    def one(k, carry):
        rows = stay[:, pl.ds(pl.multiple_of(k * step, step), step)]
        x = rows[5:6] - anchor_x
        y = rows[6:7] - anchor_y
        sources = source_rows(rows)
        pair = (sources[4], sources[9])
        on_x = [jnp.where(x == at, v, 0.0) for at in (0.0, cells_x - 1.0) for v in pair]
        on_y = [jnp.where(y == at, v, 0.0) for at in (0.0, cells_y - 1.0) for v in pair]
        left = jnp.concatenate([spread(y, on_x, cells_y), spread(x, on_y, cells_x)], axis=0)
        acc[...] += lax.dot_general(
            left, depth_onehot(rows, depth), TRANSPOSED, preferred_element_type=F32
        )
        return carry

    lax.fori_loop(0, total // step, one, 0)


def one_field(rows, along, number, depth, f):
    sources = source_rows(rows)
    left = spread(along, [sources[f], sources[5 + f]], number)
    got = lax.dot_general(left, depth_onehot(rows, depth), TRANSPOSED, preferred_element_type=F32)
    return got[:number] + got[number:]


def deposit_kernel(cells_x, cells_y, half, numbers, table, *refs):
    step = 4 * LANES
    if half == 0:
        stay, dep, state, where_to = refs
        total = stay.shape[1]
        state[:, :total] = stay[0:5, :]
        where_to[:, :total] = stay[5:8, :].astype(I32)
    else:
        _, dep = refs
    dep[...] = jnp.zeros(dep.shape, F32)
    columns = cells_x // 2 * cells_y
    anchor_x, anchor_y = anchors(cells_x, cells_y)
    anchor_x = anchor_x + half * (cells_x // 2)

    def one(k, carry):
        rows = jnp.concatenate([table[4 * k + t] for t in range(4)], axis=1)
        column = (rows[5:6] - anchor_x) * cells_y + (rows[6:7] - anchor_y)
        sources = source_rows(rows)
        onehot = depth_onehot(rows, dep.shape[1])
        left = [spread(column, part, columns) for part in (sources[:5], sources[5:])]
        dep[...] += lax.dot_general(
            jnp.concatenate(left, axis=1),
            jnp.concatenate([onehot, onehot], axis=1),
            TRANSPOSED,
            preferred_element_type=F32,
        )
        return carry

    lax.fori_loop(0, (numbers[0, 4 + half] + step - 1) // step, one, 0)


def arrivals(rows, along, number, depth):
    left = spread(along, source_rows(rows), number)
    got = lax.dot_general(left, depth_onehot(rows, depth), TRANSPOSED, preferred_element_type=F32)
    return [
        got[f * number : (f + 1) * number] + got[(5 + f) * number : (6 + f) * number]
        for f in range(5)
    ]


def relay_kernel(
    cells_x, cells_y, in_even, in_odd, partial, own, leaving, _, even, odd, planes, halo
):
    depth = partial.shape[2]
    anchor_x, _ = anchors(cells_x, cells_y)
    got = receive_pair("gy", in_even, in_odd)
    parts = [unpack(g, depth) for g in got]
    for q, (rows, plane, _, _) in enumerate(parts):
        for f, value in enumerate(arrivals(rows, rows[5:6] - anchor_x, cells_x, depth)):
            planes[q, f] = value
        halo[q] = plane + leaving[2 + q]
    row = iota((cells_y, depth), 0)

    def side(x):
        value = partial[min(x, 1)] + jnp.where(row == 0, planes[0, 4, x : x + 1, :], 0.0)
        return value + jnp.where(row == cells_y - 1, planes[1, 4, x : x + 1, :], 0.0)

    up = message(own[1], side(cells_x - 1), parts[0][3], parts[1][3])
    down = message(own[0], side(0), parts[0][2], parts[1][2])
    send_pair("gx", even, odd, up, down)


def update_kernel(
    cells_x, cells_y, y_even, y_odd, x_even, x_odd, density, momentum, energy, dep_low, dep_high,
    planes_y, halo_y, leaving, state_in, where_in,
    rho_out, impulse, energy_out, fastest, state, where_to, pressure, planes_x,
):
    depth = energy.shape[2]
    _, anchor_y = anchors(cells_x, cells_y)
    scale = ADIABATIC_INDEX - 1.0
    shape = (cells_y, depth)
    row = iota(shape, 0)
    lane = iota(shape, 1)
    parts = [unpack(g, depth) for g in receive_pair("gx", x_even, x_odd)]
    for q, (rows, plane, _, _) in enumerate(parts):
        for f, value in enumerate(arrivals(rows, rows[6:7] - anchor_y, cells_y, depth)):
            planes_x[q, f] = value
        pressure[q * (cells_x + 1)] = scale * (plane + leaving[q])
    row_x = iota((cells_x, depth), 0)
    halos = []
    for q in range(2):
        value = halo_y[q] + jnp.where(row_x == 0, parts[0][2 + q], 0.0)
        halos.append(scale * (value + jnp.where(row_x == cells_x - 1, parts[1][2 + q], 0.0)))
    tables = [parts[0][0], parts[1][0]] + [
        unpack(g, depth)[0] for g in receive_pair("gy", y_even, y_odd)
    ]
    for q, rows in enumerate(tables):
        lanes = slice(q * rows.shape[1], (q + 1) * rows.shape[1])
        state[:, lanes] = rows[0:5]
        where_to[:, lanes] = rows[5:8].astype(I32)

    def with_planes(f, x, value):
        half = cells_x // 2
        value = value + (dep_low if x < half else dep_high)[f, x % half]
        if x == 0:
            value = value + planes_x[0, f]
        if x == cells_x - 1:
            value = value + planes_x[1, f]
        value = value + jnp.where(row == 0, planes_y[0, f, x : x + 1, :], 0.0)
        return value + jnp.where(row == cells_y - 1, planes_y[1, f, x : x + 1, :], 0.0)

    for x in range(cells_x):
        value = with_planes(4, x, energy[x])
        energy_out[x] = value
        pressure[x + 1] = scale * value
    top = jnp.zeros(shape, F32)
    for x in range(cells_x):
        here = pressure[x + 1]
        grad_x = 0.5 * (pressure[x + 2] - pressure[x])
        after = jnp.where(
            row == cells_y - 1, halos[1][x : x + 1, :], pltpu.roll(here, cells_y - 1, 0)
        )
        before = jnp.where(row == 0, halos[0][x : x + 1, :], pltpu.roll(here, 1, 0))
        grad_y = 0.5 * (after - before)
        after = jnp.where(lane == depth - 1, 0.0, pltpu.roll(here, depth - 1, 1))
        before = jnp.where(lane == 0, 0.0, pltpu.roll(here, 1, 1))
        grad_z = 0.5 * (after - before)
        rho = with_planes(0, x, density[x])
        rho_out[x] = rho
        largest = jnp.zeros(shape, F32)
        for k, grad in enumerate((grad_x, grad_y, grad_z)):
            value = with_planes(1 + k, x, momentum[k, x]) - KICK * grad
            impulse[k, x] = value
            largest = jnp.maximum(largest, jnp.abs(value))
        wave = largest / rho + jnp.sqrt(ADIABATIC_INDEX * here / rho)
        top = jnp.maximum(top, wave)
    fastest[...] = jnp.broadcast_to(jnp.max(top, axis=(0, 1), keepdims=True), fastest.shape)


def call(kernel, outs, scratch=(), out_specs=None, in_specs=None, aliases=None, vmem=48, **extra):
    if in_specs is not None:
        extra["in_specs"] = in_specs
    if out_specs is not None:
        extra["out_specs"] = out_specs
    return pl.pallas_call(
        kernel,
        out_shape=outs,
        scratch_shapes=list(scratch),
        input_output_aliases=aliases or {},
        compiler_params=pltpu.CompilerParams(vmem_limit_bytes=vmem * 1024 * 1024),
        **extra,
    )


def swap(axis, even, odd):
    size = lax.axis_size(axis)
    pairs = lambda first: [
        p for i in range(first, size - 1, 2) for p in ((i, i + 1), (i + 1, i))
    ]
    odd = lax.ppermute(odd, axis, pairs(1))
    even = lax.ppermute(even, axis, pairs(0))
    return even, odd


def on_device(
    density, momentum, energy, parcel_mass, droplet_velocity, parcel_temp, parcel_cell, parcel_count
):
    cells_x, cells_y, depth = density.shape
    rows = parcel_mass.shape[0]
    capacity = rows // 16
    chunks = rows // LANES
    columns = cells_x * cells_y
    step = min(1024, rows)
    sds = jax.ShapeDtypeStruct
    whole = pl.BlockSpec(memory_space=VMEM)
    parcels = sds((8, capacity + 3 * depth), F32)
    dense = sds((chunks, LANES), F32)
    place, stays, words, masks, numbers = call(
        functools.partial(rank_kernel, cells_x, cells_y),
        (
            dense,
            dense,
            sds((chunks, LANES), I32),
            sds((KINDS, 3, chunks, LANES), F32),
            sds((1, LANES), I32),
        ),
        scratch=(VMEM((chunks, LANES), I32), VMEM((chunks, LANES), I32)),
        in_specs=[pl.BlockSpec(memory_space=pltpu.SMEM), whole],
        cost_estimate=pl.CostEstimate(flops=10**9, bytes_accessed=10**6, transcendentals=0),
    )(parcel_count, parcel_cell)
    even, odd, stay, own, leaving, partial, low, high = call(
        functools.partial(prep_kernel, cells_x, cells_y, step),
        (
            parcels,
            parcels,
            sds((8, rows), F32),
            sds((2, 8, capacity), F32),
            sds((4, cells_x, depth), F32),
            sds((2, cells_y, depth), F32),
            sds((chunks + 1, 8, LANES), F32),
            sds((chunks + 1, 8, LANES), F32),
        ),
        scratch=(
            VMEM((8, rows), F32),
            VMEM((chunks, 8, LANES), F32),
            pltpu.SMEM((chunks, LANES), I32),
            VMEM((4, capacity // LANES + 1, 8, LANES), F32),
            VMEM((4 * (cells_x + cells_y), depth), F32),
            pltpu.SemaphoreType.DMA,
        ),
    )(
        parcel_mass.reshape(chunks, LANES),
        parcel_temp.reshape(chunks, LANES),
        droplet_velocity,
        parcel_cell,
        energy,
        place,
        stays,
        words,
        masks,
    )
    y_even, y_odd = swap("gy", even, odd)
    slots = rows + 4 * capacity
    half = sds((5 * columns // 2, depth), F32)
    smem = pl.BlockSpec(memory_space=pltpu.SMEM)
    dep_low, state, where_to = call(
        functools.partial(deposit_kernel, cells_x, cells_y, 0),
        (half, sds((5, slots), F32), sds((3, slots), I32)),
        in_specs=[smem, whole, whole],
    )(numbers, low, stay)
    even, odd, planes_y, halo_y = call(
        functools.partial(relay_kernel, cells_x, cells_y),
        (parcels, parcels, sds((2, 5, cells_x, depth), F32), sds((2, cells_x, depth), F32)),
        in_specs=[whole] * 5 + [pl.BlockSpec(memory_space=pl.ANY)],
    )(y_even, y_odd, partial, own, leaving, dep_low)
    x_even, x_odd = swap("gx", even, odd)
    (dep_high,) = call(
        functools.partial(deposit_kernel, cells_x, cells_y, 1),
        (half,),
        in_specs=[smem, whole, pl.BlockSpec(memory_space=pl.ANY)],
    )(numbers, high, halo_y)
    dep_low, dep_high = (d.reshape(5, cells_x // 2, cells_y, depth) for d in (dep_low, dep_high))
    last = rows // (4 * capacity)
    rho, impulse, energy_out, top, state, where_to = call(
        functools.partial(update_kernel, cells_x, cells_y),
        (
            sds(density.shape, F32),
            sds(momentum.shape, F32),
            sds(energy.shape, F32),
            sds((lax.axis_size(("gx", "gy")), LANES), F32),
            sds(state.shape, F32),
            sds(where_to.shape, I32),
        ),
        scratch=(
            VMEM((cells_x + 2, cells_y, depth), F32),
            VMEM((2, 5, cells_y, depth), F32),
        ),
        in_specs=[whole] * 12 + [pl.BlockSpec(memory_space=pl.ANY)] * 2,
        out_specs=(whole,) * 4
        + (
            pl.BlockSpec((5, 4 * capacity), lambda i: (0, last)),
            pl.BlockSpec((3, 4 * capacity), lambda i: (0, last)),
        ),
        aliases={12: 4, 13: 5},
        grid=(1,),
    )(
        y_even, y_odd, x_even, x_odd, density, momentum, energy, dep_low, dep_high,
        planes_y, halo_y, leaving, state, where_to,
    )
    fastest = jnp.max(lax.all_to_all(top, ("gx", "gy"), 0, 0, tiled=True), axis=0)[0]
    return rho, impulse, energy_out, state, where_to, COURANT / fastest


def solution(mesh):
    both = ("gx", "gy")
    return jax.shard_map(
        on_device,
        mesh=mesh,
        in_specs=(
            P("gx", "gy", None),
            P(None, "gx", "gy", None),
            P("gx", "gy", None),
            P(both),
            P(None, both),
            P(both),
            P(None, both),
            P(both),
        ),
        out_specs=(
            P("gx", "gy", None),
            P(None, "gx", "gy", None),
            P("gx", "gy", None),
            P(None, both),
            P(None, both),
            P(),
        ),
        check_vma=False,
    )
```

```python
import functools

import jax
import jax.numpy as jnp
from jax import lax
from jax.experimental import pallas as pl
from jax.experimental.pallas import tpu as pltpu
from jax.sharding import PartitionSpec as P


ADIABATIC_INDEX = 1.4
KICK = 0.25
COURANT = 0.4
SHRINK = 0.5

F32 = jnp.float32
BF16 = jnp.bfloat16
I32 = jnp.int32
LANES = 128
KINDS = 6
VMEM = pltpu.VMEM
TRANSPOSED = (((1,), (1,)), ((), ()))


def iota(shape, dim, dtype=I32):
    return lax.broadcasted_iota(dtype, shape, dim)


def sigmoid_of(temp):
    return 1.0 / (1.0 + jnp.exp(-2.0 * (temp - 2.0)))


def rank_kernel(cells_x, cells_y, count, cell, place, stays, words, masks, numbers, cx, cy):
    chunks = place.shape[0]
    anchor_x = lax.axis_index("gx") * cells_x
    anchor_y = lax.axis_index("gy") * cells_y
    for b in range(chunks):
        lanes = slice(b * LANES, (b + 1) * LANES)
        cx[b : b + 1, :] = cell[0:1, lanes]
        cy[b : b + 1, :] = cell[1:2, lanes]
    shape = (chunks, LANES)
    lane = iota(shape, 1)
    live = iota(shape, 0) * LANES + lane < count[0]
    local_x = cx[...] - anchor_x
    local_y = cy[...] - anchor_y
    heading = jnp.where(
        local_x < 0,
        0,
        jnp.where(
            local_x >= cells_x, 1, jnp.where(local_y < 0, 2, jnp.where(local_y >= cells_y, 3, 4))
        ),
    )
    heading = jnp.where((heading == 4) & (local_x >= cells_x // 2), 5, heading)
    heading = jnp.where(live, heading, KINDS)
    hits = [jnp.where(heading == h, 1.0, 0.0) for h in range(KINDS)]
    lane_r = iota((LANES, 2 * LANES), 0)
    lane_c = iota((LANES, 2 * LANES), 1)
    scan = jnp.where((lane_r < lane_c) | (lane_c >= LANES), 1.0, 0.0).astype(BF16)
    both = jnp.dot(jnp.concatenate(hits, axis=0).astype(BF16), scan, preferred_element_type=F32)
    inner = [both[h * chunks : (h + 1) * chunks, :LANES] for h in range(KINDS)]
    total = [both[h * chunks : (h + 1) * chunks, LANES:] for h in range(KINDS)]
    below = jnp.where(iota((chunks, chunks), 1) < iota((chunks, chunks), 0), 1.0, 0.0).astype(BF16)
    base = jnp.dot(
        below, jnp.concatenate(total, axis=1).astype(BF16), preferred_element_type=F32
    ).astype(I32)
    offset = jnp.zeros(shape, F32)
    spot = jnp.full(shape, -1.0, F32)
    word = jnp.zeros(shape, I32)
    number = jnp.zeros((1, LANES), I32)
    for h in range(KINDS):
        spot = jnp.where(heading == h, inner[h] + offset, spot)
        start = base[:, h * LANES : (h + 1) * LANES]
        within = start & (LANES - 1)
        end = within + total[h].astype(I32)
        turn = (start - offset.astype(I32)) & (LANES - 1)
        word = jnp.where(lane == h, (start >> 7) * LANES + turn, word)
        last = start + total[h].astype(I32)
        word = jnp.where(lane == KINDS + h, last >> 7, word)
        number = jnp.where(lane[0:1] == h, last[chunks - 1 :], number)
        masks[h, 0] = jnp.where((lane >= within) & (lane < end), 1.0, 0.0)
        masks[h, 1] = jnp.where(lane < end - LANES, 1.0, 0.0)
        masks[h, 2] = jnp.where(end >= LANES, 1.0, 0.0)
        offset = offset + total[h]
    words[...] = word
    numbers[...] = number
    place[...] = spot
    stays[...] = jnp.where((heading == 4) | (heading == 5), 1.0, 0.0)


def prep_kernel(
    cells_x, cells_y, step, mass, temp, vel, cell, energy, pos, stays, words, masks,
    even, odd, stay, own, leaving, partial, low, high,
    pay, compact, table, tiles, acc, sem,
):
    load = pltpu.make_async_copy(words, table, sem)
    load.start()
    chunks = mass.shape[0]
    anchor_xf, anchor_yf = anchors(cells_x, cells_y)
    kept = mass[...] * (1.0 - SHRINK * sigmoid_of(temp[...]))
    pay[1:4, :] = vel[...]
    pay[5:8, :] = cell[...].astype(F32)
    for b in range(chunks):
        lanes = slice(b * LANES, (b + 1) * LANES)
        pay[0:1, lanes] = kept[b : b + 1, :]
        pay[4:5, lanes] = temp[b : b + 1, :]
    for b in range(chunks):
        lanes = slice(b * LANES, (b + 1) * LANES)
        stay[:, lanes] = jnp.where(stays[b : b + 1, :] > 0.0, pay[:, lanes], 0.0)
    group = min(32, chunks)

    def pack(g, carry):
        for u in range(group):
            b = g * group + u
            slots = pos[pl.ds(b, 1), :]
            onehot = jnp.where(slots == iota((LANES, LANES), 0).astype(F32), 1.0, 0.0).astype(BF16)
            rows = pay[:, pl.ds(pl.multiple_of(b * LANES, LANES), LANES)]
            first = rows.astype(BF16).astype(F32)
            rest = rows - first
            middle = rest.astype(BF16).astype(F32)
            last = rest - middle
            parts = jnp.concatenate([first, middle, last, jnp.zeros_like(last)], axis=0).astype(BF16)
            got = lax.dot_general(parts, onehot, TRANSPOSED, preferred_element_type=F32)
            compact[b] = got[0:8] + got[8:16] + got[16:24]
        return carry

    lax.fori_loop(0, chunks // group, pack, 0)
    for ref in (tiles, low, high):
        ref[...] = jnp.zeros(ref.shape, F32)
    lists = [tiles.at[h] for h in range(4)] + [low, high]
    load.wait()
    unroll = 8

    def place_all(g, carry):
        carry = list(carry)
        for u in range(unroll):
            b = g * unroll + u
            rows = compact[b]
            for h in range(KINDS):
                word = table[b, h]
                turned = pltpu.roll(rows, word & (LANES - 1), 1)
                merged = jnp.where(masks[h, 0, pl.ds(b, 1), :] > 0.0, turned, carry[h])
                lists[h][word >> 7] = merged
                rest = jnp.where(masks[h, 2, pl.ds(b, 1), :] > 0.0, 0.0, merged)
                carry[h] = jnp.where(masks[h, 1, pl.ds(b, 1), :] > 0.0, turned, rest)
        return tuple(carry)

    carry = lax.fori_loop(
        0, chunks // unroll, place_all, tuple(jnp.zeros((8, LANES), F32) for _ in range(KINDS))
    )
    for h in range(KINDS):
        lists[h][table[chunks - 1, KINDS + h]] = carry[h]
    width = own.shape[2]
    buckets = [
        jnp.concatenate([tiles[h, t] for t in range(width // LANES)], axis=1) for h in range(4)
    ]
    for h in range(4):
        along = (buckets[h][6:7] - anchor_yf) if h < 2 else (buckets[h][5:6] - anchor_xf)
        number = cells_y if h < 2 else cells_x
        leaving[h] = one_field(buckets[h], along, number, acc.shape[1], 4)
    for h in range(2):
        own[h] = buckets[h]
    outer_energy(cells_x, cells_y, anchor_xf, anchor_yf, 2 * step, stay, acc)
    planes = [acc[q * 2 * cells_y : (q * 2 + 1) * cells_y] + acc[(q * 2 + 1) * cells_y : (q * 2 + 2) * cells_y] for q in range(4)]
    partial[0] = energy[0] + planes[0]
    partial[1] = energy[cells_x - 1] + planes[1]
    up = message(
        buckets[3], energy[:, cells_y - 1, :] + planes[3], leaving[0, -1:, :], leaving[1, -1:, :]
    )
    down = message(buckets[2], energy[:, 0, :] + planes[2], leaving[0, 0:1, :], leaving[1, 0:1, :])
    send_pair("gy", even, odd, up, down)


def message(bucket, plane, first, second):
    half = plane.shape[0] // 2
    rest = jnp.zeros((6, plane.shape[1]), F32)
    return jnp.concatenate(
        [bucket, plane[:half], plane[half:], jnp.concatenate([first, second, rest], axis=0)], axis=1
    )


def unpack(got, depth):
    width = got.shape[1] - 3 * depth
    plane = jnp.concatenate(
        [got[:, width : width + depth], got[:, width + depth : width + 2 * depth]], axis=0
    )
    corner = got[:, width + 2 * depth :]
    return got[:, :width], plane, corner[0:1], corner[1:2]


def send_pair(axis, even, odd, up, down):
    is_even = (lax.axis_index(axis) & 1) == 0
    even[...] = jnp.where(is_even, up, down)
    odd[...] = jnp.where(is_even, down, up)


def receive_pair(axis, even, odd):
    is_even = (lax.axis_index(axis) & 1) == 0
    return jnp.where(is_even, odd[...], even[...]), jnp.where(is_even, even[...], odd[...])


def anchors(cells_x, cells_y):
    return (
        (lax.axis_index("gx") * cells_x).astype(F32),
        (lax.axis_index("gy") * cells_y).astype(F32),
    )


def source_rows(rows):
    kept, temp = rows[0:1], rows[4:5]
    v0, v1, v2 = rows[1:2], rows[2:3], rows[3:4]
    share = sigmoid_of(temp)
    gone = kept * share / (1.0 - SHRINK * share)
    heat = temp + 0.5 * (v0 * v0 + v1 * v1 + v2 * v2)
    fields = [gone, gone * v0, gone * v1, gone * v2, gone * heat]
    high = [f.astype(BF16).astype(F32) for f in fields]
    low = [f - g for f, g in zip(fields, high)]
    return high + low


def spread(columns, sources, number):
    n = columns.shape[1]
    hot = jnp.where(columns == iota((number, n), 0).astype(F32), 1.0, 0.0).astype(BF16)
    hot = hot.reshape(number // 16, 16, n)
    parts = []
    for source in sources:
        value = jnp.broadcast_to(source, (16, n)).astype(BF16)
        parts.append((hot * value[None]).reshape(number, n))
    return jnp.concatenate(parts, axis=0)


def depth_onehot(rows, depth):
    n = rows.shape[1]
    return jnp.where(rows[7:8] == iota((depth, n), 0).astype(F32), 1.0, 0.0).astype(BF16)


def outer_energy(cells_x, cells_y, anchor_x, anchor_y, step, stay, acc):
    total = stay.shape[1]
    depth = acc.shape[1]
    acc[...] = jnp.zeros(acc.shape, F32)

    def one(k, carry):
        rows = stay[:, pl.ds(pl.multiple_of(k * step, step), step)]
        x = rows[5:6] - anchor_x
        y = rows[6:7] - anchor_y
        sources = source_rows(rows)
        pair = (sources[4], sources[9])
        on_x = [jnp.where(x == at, v, 0.0) for at in (0.0, cells_x - 1.0) for v in pair]
        on_y = [jnp.where(y == at, v, 0.0) for at in (0.0, cells_y - 1.0) for v in pair]
        left = jnp.concatenate([spread(y, on_x, cells_y), spread(x, on_y, cells_x)], axis=0)
        acc[...] += lax.dot_general(
            left, depth_onehot(rows, depth), TRANSPOSED, preferred_element_type=F32
        )
        return carry

    lax.fori_loop(0, total // step, one, 0)


def one_field(rows, along, number, depth, f):
    sources = source_rows(rows)
    left = spread(along, [sources[f], sources[5 + f]], number)
    got = lax.dot_general(left, depth_onehot(rows, depth), TRANSPOSED, preferred_element_type=F32)
    return got[:number] + got[number:]


def deposit_kernel(cells_x, cells_y, half, numbers, table, *refs):
    step = 8 * LANES
    if half == 0:
        stay, dep, state, where_to = refs
        total = stay.shape[1]
        state[:, :total] = stay[0:5, :]
        where_to[:, :total] = stay[5:8, :].astype(I32)
    else:
        _, dep = refs
    dep[...] = jnp.zeros(dep.shape, F32)
    columns = cells_x // 2 * cells_y
    anchor_x, anchor_y = anchors(cells_x, cells_y)
    anchor_x = anchor_x + half * (cells_x // 2)

    def one(k, carry):
        rows = jnp.concatenate([table[8 * k + t] for t in range(8)], axis=1)
        column = (rows[5:6] - anchor_x) * cells_y + (rows[6:7] - anchor_y)
        got = lax.dot_general(
            spread(column, source_rows(rows), columns),
            depth_onehot(rows, dep.shape[1]),
            TRANSPOSED,
            preferred_element_type=F32,
        )
        dep[...] += got[: 5 * columns] + got[5 * columns :]
        return carry

    lax.fori_loop(0, (numbers[0, 4 + half] + step - 1) // step, one, 0)


def arrivals(rows, along, number, depth):
    left = spread(along, source_rows(rows), number)
    got = lax.dot_general(left, depth_onehot(rows, depth), TRANSPOSED, preferred_element_type=F32)
    return [
        got[f * number : (f + 1) * number] + got[(5 + f) * number : (6 + f) * number]
        for f in range(5)
    ]


def relay_kernel(
    cells_x, cells_y, in_even, in_odd, partial, own, leaving, _, even, odd, planes, halo
):
    depth = partial.shape[2]
    anchor_x, _ = anchors(cells_x, cells_y)
    got = receive_pair("gy", in_even, in_odd)
    parts = [unpack(g, depth) for g in got]
    for q, (rows, plane, _, _) in enumerate(parts):
        for f, value in enumerate(arrivals(rows, rows[5:6] - anchor_x, cells_x, depth)):
            planes[q, f] = value
        halo[q] = plane + leaving[2 + q]
    row = iota((cells_y, depth), 0)

    def side(x):
        value = partial[min(x, 1)] + jnp.where(row == 0, planes[0, 4, x : x + 1, :], 0.0)
        return value + jnp.where(row == cells_y - 1, planes[1, 4, x : x + 1, :], 0.0)

    up = message(own[1], side(cells_x - 1), parts[0][3], parts[1][3])
    down = message(own[0], side(0), parts[0][2], parts[1][2])
    send_pair("gx", even, odd, up, down)


def update_kernel(
    cells_x, cells_y, y_even, y_odd, x_even, x_odd, density, momentum, energy, dep_low, dep_high,
    planes_y, halo_y, leaving, state_in, where_in,
    rho_out, impulse, energy_out, fastest, state, where_to, pressure, planes_x,
):
    depth = energy.shape[2]
    _, anchor_y = anchors(cells_x, cells_y)
    scale = ADIABATIC_INDEX - 1.0
    shape = (cells_y, depth)
    row = iota(shape, 0)
    lane = iota(shape, 1)
    parts = [unpack(g, depth) for g in receive_pair("gx", x_even, x_odd)]
    for q, (rows, plane, _, _) in enumerate(parts):
        for f, value in enumerate(arrivals(rows, rows[6:7] - anchor_y, cells_y, depth)):
            planes_x[q, f] = value
        pressure[q * (cells_x + 1)] = scale * (plane + leaving[q])
    row_x = iota((cells_x, depth), 0)
    halos = []
    for q in range(2):
        value = halo_y[q] + jnp.where(row_x == 0, parts[0][2 + q], 0.0)
        halos.append(scale * (value + jnp.where(row_x == cells_x - 1, parts[1][2 + q], 0.0)))
    tables = [parts[0][0], parts[1][0]] + [
        unpack(g, depth)[0] for g in receive_pair("gy", y_even, y_odd)
    ]
    for q, rows in enumerate(tables):
        lanes = slice(q * rows.shape[1], (q + 1) * rows.shape[1])
        state[:, lanes] = rows[0:5]
        where_to[:, lanes] = rows[5:8].astype(I32)

    def with_planes(f, x, value):
        half = cells_x // 2
        value = value + (dep_low if x < half else dep_high)[f, x % half]
        if x == 0:
            value = value + planes_x[0, f]
        if x == cells_x - 1:
            value = value + planes_x[1, f]
        value = value + jnp.where(row == 0, planes_y[0, f, x : x + 1, :], 0.0)
        return value + jnp.where(row == cells_y - 1, planes_y[1, f, x : x + 1, :], 0.0)

    for x in range(cells_x):
        value = with_planes(4, x, energy[x])
        energy_out[x] = value
        pressure[x + 1] = scale * value
    top = jnp.zeros(shape, F32)
    for x in range(cells_x):
        here = pressure[x + 1]
        grad_x = 0.5 * (pressure[x + 2] - pressure[x])
        after = jnp.where(
            row == cells_y - 1, halos[1][x : x + 1, :], pltpu.roll(here, cells_y - 1, 0)
        )
        before = jnp.where(row == 0, halos[0][x : x + 1, :], pltpu.roll(here, 1, 0))
        grad_y = 0.5 * (after - before)
        after = jnp.where(lane == depth - 1, 0.0, pltpu.roll(here, depth - 1, 1))
        before = jnp.where(lane == 0, 0.0, pltpu.roll(here, 1, 1))
        grad_z = 0.5 * (after - before)
        rho = with_planes(0, x, density[x])
        rho_out[x] = rho
        largest = jnp.zeros(shape, F32)
        for k, grad in enumerate((grad_x, grad_y, grad_z)):
            value = with_planes(1 + k, x, momentum[k, x]) - KICK * grad
            impulse[k, x] = value
            largest = jnp.maximum(largest, jnp.abs(value))
        wave = largest / rho + jnp.sqrt(ADIABATIC_INDEX * here / rho)
        top = jnp.maximum(top, wave)
    fastest[...] = jnp.broadcast_to(jnp.max(top, axis=(0, 1), keepdims=True), fastest.shape)


def call(kernel, outs, scratch=(), out_specs=None, in_specs=None, aliases=None, vmem=48, **extra):
    if in_specs is not None:
        extra["in_specs"] = in_specs
    if out_specs is not None:
        extra["out_specs"] = out_specs
    return pl.pallas_call(
        kernel,
        out_shape=outs,
        scratch_shapes=list(scratch),
        input_output_aliases=aliases or {},
        compiler_params=pltpu.CompilerParams(vmem_limit_bytes=vmem * 1024 * 1024),
        **extra,
    )


def swap(axis, even, odd):
    size = lax.axis_size(axis)
    pairs = lambda first: [
        p for i in range(first, size - 1, 2) for p in ((i, i + 1), (i + 1, i))
    ]
    odd = lax.ppermute(odd, axis, pairs(1))
    even = lax.ppermute(even, axis, pairs(0))
    return even, odd


def on_device(
    density, momentum, energy, parcel_mass, droplet_velocity, parcel_temp, parcel_cell, parcel_count
):
    cells_x, cells_y, depth = density.shape
    rows = parcel_mass.shape[0]
    capacity = rows // 16
    chunks = rows // LANES
    columns = cells_x * cells_y
    step = min(1024, rows)
    sds = jax.ShapeDtypeStruct
    whole = pl.BlockSpec(memory_space=VMEM)
    parcels = sds((8, capacity + 3 * depth), F32)
    dense = sds((chunks, LANES), F32)
    place, stays, words, masks, numbers = call(
        functools.partial(rank_kernel, cells_x, cells_y),
        (
            dense,
            dense,
            sds((chunks, LANES), I32),
            sds((KINDS, 3, chunks, LANES), F32),
            sds((1, LANES), I32),
        ),
        scratch=(VMEM((chunks, LANES), I32), VMEM((chunks, LANES), I32)),
        in_specs=[pl.BlockSpec(memory_space=pltpu.SMEM), whole],
        cost_estimate=pl.CostEstimate(flops=10**9, bytes_accessed=10**6, transcendentals=0),
    )(parcel_count, parcel_cell)
    even, odd, stay, own, leaving, partial, low, high = call(
        functools.partial(prep_kernel, cells_x, cells_y, step),
        (
            parcels,
            parcels,
            sds((8, rows), F32),
            sds((2, 8, capacity), F32),
            sds((4, cells_x, depth), F32),
            sds((2, cells_y, depth), F32),
            sds((chunks + 1, 8, LANES), F32),
            sds((chunks + 1, 8, LANES), F32),
        ),
        scratch=(
            VMEM((8, rows), F32),
            VMEM((chunks, 8, LANES), F32),
            pltpu.SMEM((chunks, LANES), I32),
            VMEM((4, capacity // LANES + 1, 8, LANES), F32),
            VMEM((4 * (cells_x + cells_y), depth), F32),
            pltpu.SemaphoreType.DMA,
        ),
    )(
        parcel_mass.reshape(chunks, LANES),
        parcel_temp.reshape(chunks, LANES),
        droplet_velocity,
        parcel_cell,
        energy,
        place,
        stays,
        words,
        masks,
    )
    y_even, y_odd = swap("gy", even, odd)
    slots = rows + 4 * capacity
    half = sds((5 * columns // 2, depth), F32)
    smem = pl.BlockSpec(memory_space=pltpu.SMEM)
    dep_low, state, where_to = call(
        functools.partial(deposit_kernel, cells_x, cells_y, 0),
        (half, sds((5, slots), F32), sds((3, slots), I32)),
        in_specs=[smem, whole, whole],
    )(numbers, low, stay)
    even, odd, planes_y, halo_y = call(
        functools.partial(relay_kernel, cells_x, cells_y),
        (parcels, parcels, sds((2, 5, cells_x, depth), F32), sds((2, cells_x, depth), F32)),
        in_specs=[whole] * 5 + [pl.BlockSpec(memory_space=pl.ANY)],
    )(y_even, y_odd, partial, own, leaving, dep_low)
    x_even, x_odd = swap("gx", even, odd)
    (dep_high,) = call(
        functools.partial(deposit_kernel, cells_x, cells_y, 1),
        (half,),
        in_specs=[smem, whole, pl.BlockSpec(memory_space=pl.ANY)],
    )(numbers, high, halo_y)
    dep_low, dep_high = (d.reshape(5, cells_x // 2, cells_y, depth) for d in (dep_low, dep_high))
    last = rows // (4 * capacity)
    rho, impulse, energy_out, top, state, where_to = call(
        functools.partial(update_kernel, cells_x, cells_y),
        (
            sds(density.shape, F32),
            sds(momentum.shape, F32),
            sds(energy.shape, F32),
            sds((lax.axis_size(("gx", "gy")), LANES), F32),
            sds(state.shape, F32),
            sds(where_to.shape, I32),
        ),
        scratch=(
            VMEM((cells_x + 2, cells_y, depth), F32),
            VMEM((2, 5, cells_y, depth), F32),
        ),
        in_specs=[whole] * 12 + [pl.BlockSpec(memory_space=pl.ANY)] * 2,
        out_specs=(whole,) * 4
        + (
            pl.BlockSpec((5, 4 * capacity), lambda i: (0, last)),
            pl.BlockSpec((3, 4 * capacity), lambda i: (0, last)),
        ),
        aliases={12: 4, 13: 5},
        grid=(1,),
    )(
        y_even, y_odd, x_even, x_odd, density, momentum, energy, dep_low, dep_high,
        planes_y, halo_y, leaving, state, where_to,
    )
    fastest = jnp.max(lax.all_to_all(top, ("gx", "gy"), 0, 0, tiled=True), axis=0)[0]
    return rho, impulse, energy_out, state, where_to, COURANT / fastest


def solution(mesh):
    both = ("gx", "gy")
    return jax.shard_map(
        on_device,
        mesh=mesh,
        in_specs=(
            P("gx", "gy", None),
            P(None, "gx", "gy", None),
            P("gx", "gy", None),
            P(both),
            P(None, both),
            P(both),
            P(None, both),
            P(both),
        ),
        out_specs=(
            P("gx", "gy", None),
            P(None, "gx", "gy", None),
            P("gx", "gy", None),
            P(None, both),
            P(None, both),
            P(),
        ),
        check_vma=False,
    )
```

```python
import functools

import jax
import jax.numpy as jnp
from jax import lax
from jax.experimental import pallas as pl
from jax.experimental.pallas import tpu as pltpu
from jax.sharding import PartitionSpec as P


ADIABATIC_INDEX = 1.4
KICK = 0.25
COURANT = 0.4
SHRINK = 0.5

F32 = jnp.float32
BF16 = jnp.bfloat16
I32 = jnp.int32
LANES = 128
KINDS = 6
CUT = 9
VMEM = pltpu.VMEM
TRANSPOSED = (((1,), (1,)), ((), ()))


def iota(shape, dim, dtype=I32):
    return lax.broadcasted_iota(dtype, shape, dim)


def sigmoid_of(temp):
    return 1.0 / (1.0 + jnp.exp(-2.0 * (temp - 2.0)))


def rank_kernel(cells_x, cells_y, count, cell, place, stays, words, masks, numbers, cx, cy):
    chunks = place.shape[0]
    anchor_x = lax.axis_index("gx") * cells_x
    anchor_y = lax.axis_index("gy") * cells_y
    for b in range(chunks):
        lanes = slice(b * LANES, (b + 1) * LANES)
        cx[b : b + 1, :] = cell[0:1, lanes]
        cy[b : b + 1, :] = cell[1:2, lanes]
    shape = (chunks, LANES)
    lane = iota(shape, 1)
    live = iota(shape, 0) * LANES + lane < count[0]
    local_x = cx[...] - anchor_x
    local_y = cy[...] - anchor_y
    heading = jnp.where(
        local_x < 0,
        0,
        jnp.where(
            local_x >= cells_x, 1, jnp.where(local_y < 0, 2, jnp.where(local_y >= cells_y, 3, 4))
        ),
    )
    heading = jnp.where((heading == 4) & (local_x >= CUT), 5, heading)
    heading = jnp.where(live, heading, KINDS)
    hits = [jnp.where(heading == h, 1.0, 0.0) for h in range(KINDS)]
    lane_r = iota((LANES, 2 * LANES), 0)
    lane_c = iota((LANES, 2 * LANES), 1)
    scan = jnp.where((lane_r < lane_c) | (lane_c >= LANES), 1.0, 0.0).astype(BF16)
    both = jnp.dot(jnp.concatenate(hits, axis=0).astype(BF16), scan, preferred_element_type=F32)
    inner = [both[h * chunks : (h + 1) * chunks, :LANES] for h in range(KINDS)]
    total = [both[h * chunks : (h + 1) * chunks, LANES:] for h in range(KINDS)]
    below = jnp.where(iota((chunks, chunks), 1) < iota((chunks, chunks), 0), 1.0, 0.0).astype(BF16)
    base = jnp.dot(
        below, jnp.concatenate(total, axis=1).astype(BF16), preferred_element_type=F32
    ).astype(I32)
    offset = jnp.zeros(shape, F32)
    spot = jnp.full(shape, -1.0, F32)
    word = jnp.zeros(shape, I32)
    number = jnp.zeros((1, LANES), I32)
    for h in range(KINDS):
        spot = jnp.where(heading == h, inner[h] + offset, spot)
        start = base[:, h * LANES : (h + 1) * LANES]
        within = start & (LANES - 1)
        end = within + total[h].astype(I32)
        turn = (start - offset.astype(I32)) & (LANES - 1)
        word = jnp.where(lane == h, (start >> 7) * LANES + turn, word)
        last = start + total[h].astype(I32)
        word = jnp.where(lane == KINDS + h, last >> 7, word)
        number = jnp.where(lane[0:1] == h, last[chunks - 1 :], number)
        masks[h, 0] = jnp.where((lane >= within) & (lane < end), 1.0, 0.0)
        masks[h, 1] = jnp.where(lane < end - LANES, 1.0, 0.0)
        masks[h, 2] = jnp.where(end >= LANES, 1.0, 0.0)
        offset = offset + total[h]
    words[...] = word
    numbers[...] = number
    place[...] = spot
    stays[...] = jnp.where((heading == 4) | (heading == 5), 1.0, 0.0)


def prep_kernel(
    cells_x, cells_y, step, mass, temp, vel, cell, energy, pos, stays, words, masks,
    even, odd, stay, own, leaving, partial, compact,
    pay, table, tiles, acc, sem,
):
    load = pltpu.make_async_copy(words, table, sem)
    load.start()
    chunks = mass.shape[0]
    anchor_xf, anchor_yf = anchors(cells_x, cells_y)
    kept = mass[...] * (1.0 - SHRINK * sigmoid_of(temp[...]))
    pay[1:4, :] = vel[...]
    pay[5:8, :] = cell[...].astype(F32)
    for b in range(chunks):
        lanes = slice(b * LANES, (b + 1) * LANES)
        pay[0:1, lanes] = kept[b : b + 1, :]
        pay[4:5, lanes] = temp[b : b + 1, :]
    for b in range(chunks):
        lanes = slice(b * LANES, (b + 1) * LANES)
        stay[:, lanes] = jnp.where(stays[b : b + 1, :] > 0.0, pay[:, lanes], 0.0)
    group = min(32, chunks)

    def pack(g, carry):
        for u in range(group):
            b = g * group + u
            slots = pos[pl.ds(b, 1), :]
            onehot = jnp.where(slots == iota((LANES, LANES), 0).astype(F32), 1.0, 0.0).astype(BF16)
            rows = pay[:, pl.ds(pl.multiple_of(b * LANES, LANES), LANES)]
            first = rows.astype(BF16).astype(F32)
            rest = rows - first
            middle = rest.astype(BF16).astype(F32)
            last = rest - middle
            parts = jnp.concatenate([first, middle, last, jnp.zeros_like(last)], axis=0).astype(BF16)
            got = lax.dot_general(parts, onehot, TRANSPOSED, preferred_element_type=F32)
            compact[b] = got[0:8] + got[8:16] + got[16:24]
        return carry

    lax.fori_loop(0, chunks // group, pack, 0)
    tiles[...] = jnp.zeros(tiles.shape, F32)
    load.wait()
    place_runs(range(4), compact, masks, table, [tiles.at[h] for h in range(4)])
    width = own.shape[2]
    buckets = [
        jnp.concatenate([tiles[h, t] for t in range(width // LANES)], axis=1) for h in range(4)
    ]
    for h in range(4):
        along = (buckets[h][6:7] - anchor_yf) if h < 2 else (buckets[h][5:6] - anchor_xf)
        number = cells_y if h < 2 else cells_x
        leaving[h] = one_field(buckets[h], along, number, acc.shape[1], 4)
    for h in range(2):
        own[h] = buckets[h]
    outer_energy(cells_x, cells_y, anchor_xf, anchor_yf, 4 * step, stay, acc)
    planes = [acc[q * 2 * cells_y : (q * 2 + 1) * cells_y] + acc[(q * 2 + 1) * cells_y : (q * 2 + 2) * cells_y] for q in range(4)]
    partial[0] = energy[0] + planes[0]
    partial[1] = energy[cells_x - 1] + planes[1]
    up = message(
        buckets[3], energy[:, cells_y - 1, :] + planes[3], leaving[0, -1:, :], leaving[1, -1:, :]
    )
    down = message(buckets[2], energy[:, 0, :] + planes[2], leaving[0, 0:1, :], leaving[1, 0:1, :])
    send_pair("gy", even, odd, up, down)


def place_runs(kinds, compact, masks, table, lists):
    chunks = compact.shape[0]
    unroll = 8

    def some(g, carry):
        carry = list(carry)
        for u in range(unroll):
            b = g * unroll + u
            rows = compact[b]
            for n, h in enumerate(kinds):
                word = table[b, h]
                turned = pltpu.roll(rows, word & (LANES - 1), 1)
                merged = jnp.where(masks[h, 0, pl.ds(b, 1), :] > 0.0, turned, carry[n])
                lists[n][word >> 7] = merged
                rest = jnp.where(masks[h, 2, pl.ds(b, 1), :] > 0.0, 0.0, merged)
                carry[n] = jnp.where(masks[h, 1, pl.ds(b, 1), :] > 0.0, turned, rest)
        return tuple(carry)

    empty = tuple(jnp.zeros((8, LANES), F32) for _ in kinds)
    carry = lax.fori_loop(0, chunks // unroll, some, empty)
    for n, h in enumerate(kinds):
        lists[n][table[chunks - 1, KINDS + h]] = carry[n]


def message(bucket, plane, first, second):
    half = plane.shape[0] // 2
    rest = jnp.zeros((6, plane.shape[1]), F32)
    return jnp.concatenate(
        [bucket, plane[:half], plane[half:], jnp.concatenate([first, second, rest], axis=0)], axis=1
    )


def unpack(got, depth):
    width = got.shape[1] - 3 * depth
    plane = jnp.concatenate(
        [got[:, width : width + depth], got[:, width + depth : width + 2 * depth]], axis=0
    )
    corner = got[:, width + 2 * depth :]
    return got[:, :width], plane, corner[0:1], corner[1:2]


def send_pair(axis, even, odd, up, down):
    is_even = (lax.axis_index(axis) & 1) == 0
    even[...] = jnp.where(is_even, up, down)
    odd[...] = jnp.where(is_even, down, up)


def receive_pair(axis, even, odd):
    is_even = (lax.axis_index(axis) & 1) == 0
    return jnp.where(is_even, odd[...], even[...]), jnp.where(is_even, even[...], odd[...])


def anchors(cells_x, cells_y):
    return (
        (lax.axis_index("gx") * cells_x).astype(F32),
        (lax.axis_index("gy") * cells_y).astype(F32),
    )


def source_rows(rows):
    kept, temp = rows[0:1], rows[4:5]
    v0, v1, v2 = rows[1:2], rows[2:3], rows[3:4]
    share = sigmoid_of(temp)
    gone = kept * share / (1.0 - SHRINK * share)
    heat = temp + 0.5 * (v0 * v0 + v1 * v1 + v2 * v2)
    fields = [gone, gone * v0, gone * v1, gone * v2, gone * heat]
    high = [f.astype(BF16).astype(F32) for f in fields]
    low = [f - g for f, g in zip(fields, high)]
    return high + low


def spread(columns, sources, number):
    n = columns.shape[1]
    hot = jnp.where(columns == iota((number, n), 0).astype(F32), 1.0, 0.0).astype(BF16)
    hot = hot.reshape(number // 16, 16, n)
    parts = []
    for source in sources:
        value = jnp.broadcast_to(source, (16, n)).astype(BF16)
        parts.append((hot * value[None]).reshape(number, n))
    return jnp.concatenate(parts, axis=0)


def depth_onehot(rows, depth):
    n = rows.shape[1]
    return jnp.where(rows[7:8] == iota((depth, n), 0).astype(F32), 1.0, 0.0).astype(BF16)


def outer_energy(cells_x, cells_y, anchor_x, anchor_y, step, stay, acc):
    total = stay.shape[1]
    depth = acc.shape[1]
    acc[...] = jnp.zeros(acc.shape, F32)

    def one(k, carry):
        rows = stay[:, pl.ds(pl.multiple_of(k * step, step), step)]
        x = rows[5:6] - anchor_x
        y = rows[6:7] - anchor_y
        sources = source_rows(rows)
        pair = (sources[4], sources[9])
        on_x = [jnp.where(x == at, v, 0.0) for at in (0.0, cells_x - 1.0) for v in pair]
        on_y = [jnp.where(y == at, v, 0.0) for at in (0.0, cells_y - 1.0) for v in pair]
        left = jnp.concatenate([spread(y, on_x, cells_y), spread(x, on_y, cells_x)], axis=0)
        acc[...] += lax.dot_general(
            left, depth_onehot(rows, depth), TRANSPOSED, preferred_element_type=F32
        )
        return carry

    lax.fori_loop(0, total // step, one, 0)


def one_field(rows, along, number, depth, f):
    sources = source_rows(rows)
    left = spread(along, [sources[f], sources[5 + f]], number)
    got = lax.dot_general(left, depth_onehot(rows, depth), TRANSPOSED, preferred_element_type=F32)
    return got[:number] + got[number:]


def deposit_kernel(cells_x, cells_y, part, numbers, *refs):
    step = 8 * LANES
    first, last = (0, CUT) if part == 0 else (CUT, cells_x)
    if part == 0:
        compact, words, masks, stay, dep, state, where_to, above, rows_of, table, sem = refs
        load = pltpu.make_async_copy(words, table, sem)
        load.start()
        for ref in (rows_of, above):
            ref[...] = jnp.zeros(ref.shape, F32)
        total = stay.shape[1]
        state[:, :total] = stay[0:5, :]
        where_to[:, :total] = stay[5:8, :].astype(I32)
        load.wait()
        place_runs((4, 5), compact, masks, table, [rows_of, above])
    else:
        rows_of, _, dep = refs
    dep[...] = jnp.zeros(dep.shape, F32)
    columns = (last - first) * cells_y
    anchor_x, anchor_y = anchors(cells_x, cells_y)
    anchor_x = anchor_x + first

    def one(k, carry):
        rows = jnp.concatenate([rows_of[8 * k + t] for t in range(8)], axis=1)
        column = (rows[5:6] - anchor_x) * cells_y + (rows[6:7] - anchor_y)
        got = lax.dot_general(
            spread(column, source_rows(rows), columns),
            depth_onehot(rows, dep.shape[1]),
            TRANSPOSED,
            preferred_element_type=F32,
        )
        dep[...] += got[: 5 * columns] + got[5 * columns :]
        return carry

    lax.fori_loop(0, (numbers[0, 4 + part] + step - 1) // step, one, 0)


def arrivals(rows, along, number, depth):
    left = spread(along, source_rows(rows), number)
    got = lax.dot_general(left, depth_onehot(rows, depth), TRANSPOSED, preferred_element_type=F32)
    return [
        got[f * number : (f + 1) * number] + got[(5 + f) * number : (6 + f) * number]
        for f in range(5)
    ]


def relay_kernel(
    cells_x, cells_y, in_even, in_odd, partial, own, leaving, _, even, odd, planes, halo
):
    depth = partial.shape[2]
    anchor_x, _ = anchors(cells_x, cells_y)
    got = receive_pair("gy", in_even, in_odd)
    parts = [unpack(g, depth) for g in got]
    for q, (rows, plane, _, _) in enumerate(parts):
        for f, value in enumerate(arrivals(rows, rows[5:6] - anchor_x, cells_x, depth)):
            planes[q, f] = value
        halo[q] = plane + leaving[2 + q]
    row = iota((cells_y, depth), 0)

    def side(x):
        value = partial[min(x, 1)] + jnp.where(row == 0, planes[0, 4, x : x + 1, :], 0.0)
        return value + jnp.where(row == cells_y - 1, planes[1, 4, x : x + 1, :], 0.0)

    up = message(own[1], side(cells_x - 1), parts[0][3], parts[1][3])
    down = message(own[0], side(0), parts[0][2], parts[1][2])
    send_pair("gx", even, odd, up, down)


def update_kernel(
    cells_x, cells_y, y_even, y_odd, x_even, x_odd, density, momentum, energy, dep_low, dep_high,
    planes_y, halo_y, leaving, state_in, where_in,
    rho_out, impulse, energy_out, fastest, state, where_to, pressure, planes_x,
):
    depth = energy.shape[2]
    _, anchor_y = anchors(cells_x, cells_y)
    scale = ADIABATIC_INDEX - 1.0
    shape = (cells_y, depth)
    row = iota(shape, 0)
    lane = iota(shape, 1)
    parts = [unpack(g, depth) for g in receive_pair("gx", x_even, x_odd)]
    for q, (rows, plane, _, _) in enumerate(parts):
        for f, value in enumerate(arrivals(rows, rows[6:7] - anchor_y, cells_y, depth)):
            planes_x[q, f] = value
        pressure[q * (cells_x + 1)] = scale * (plane + leaving[q])
    row_x = iota((cells_x, depth), 0)
    halos = []
    for q in range(2):
        value = halo_y[q] + jnp.where(row_x == 0, parts[0][2 + q], 0.0)
        halos.append(scale * (value + jnp.where(row_x == cells_x - 1, parts[1][2 + q], 0.0)))
    tables = [parts[0][0], parts[1][0]] + [
        unpack(g, depth)[0] for g in receive_pair("gy", y_even, y_odd)
    ]
    for q, rows in enumerate(tables):
        lanes = slice(q * rows.shape[1], (q + 1) * rows.shape[1])
        state[:, lanes] = rows[0:5]
        where_to[:, lanes] = rows[5:8].astype(I32)

    def with_planes(f, x, value):
        value = value + (dep_low[f, x] if x < CUT else dep_high[f, x - CUT])
        if x == 0:
            value = value + planes_x[0, f]
        if x == cells_x - 1:
            value = value + planes_x[1, f]
        value = value + jnp.where(row == 0, planes_y[0, f, x : x + 1, :], 0.0)
        return value + jnp.where(row == cells_y - 1, planes_y[1, f, x : x + 1, :], 0.0)

    for x in range(cells_x):
        value = with_planes(4, x, energy[x])
        energy_out[x] = value
        pressure[x + 1] = scale * value
    top = jnp.zeros(shape, F32)
    for x in range(cells_x):
        here = pressure[x + 1]
        grad_x = 0.5 * (pressure[x + 2] - pressure[x])
        after = jnp.where(
            row == cells_y - 1, halos[1][x : x + 1, :], pltpu.roll(here, cells_y - 1, 0)
        )
        before = jnp.where(row == 0, halos[0][x : x + 1, :], pltpu.roll(here, 1, 0))
        grad_y = 0.5 * (after - before)
        after = jnp.where(lane == depth - 1, 0.0, pltpu.roll(here, depth - 1, 1))
        before = jnp.where(lane == 0, 0.0, pltpu.roll(here, 1, 1))
        grad_z = 0.5 * (after - before)
        rho = with_planes(0, x, density[x])
        rho_out[x] = rho
        largest = jnp.zeros(shape, F32)
        for k, grad in enumerate((grad_x, grad_y, grad_z)):
            value = with_planes(1 + k, x, momentum[k, x]) - KICK * grad
            impulse[k, x] = value
            largest = jnp.maximum(largest, jnp.abs(value))
        wave = largest / rho + jnp.sqrt(ADIABATIC_INDEX * here / rho)
        top = jnp.maximum(top, wave)
    fastest[...] = jnp.broadcast_to(jnp.max(top, axis=(0, 1), keepdims=True), fastest.shape)


def call(kernel, outs, scratch=(), out_specs=None, in_specs=None, aliases=None, vmem=48, **extra):
    if in_specs is not None:
        extra["in_specs"] = in_specs
    if out_specs is not None:
        extra["out_specs"] = out_specs
    return pl.pallas_call(
        kernel,
        out_shape=outs,
        scratch_shapes=list(scratch),
        input_output_aliases=aliases or {},
        compiler_params=pltpu.CompilerParams(vmem_limit_bytes=vmem * 1024 * 1024),
        **extra,
    )


def swap(axis, even, odd):
    size = lax.axis_size(axis)
    pairs = lambda first: [
        p for i in range(first, size - 1, 2) for p in ((i, i + 1), (i + 1, i))
    ]
    odd = lax.ppermute(odd, axis, pairs(1))
    even = lax.ppermute(even, axis, pairs(0))
    return even, odd


def on_device(
    density, momentum, energy, parcel_mass, droplet_velocity, parcel_temp, parcel_cell, parcel_count
):
    cells_x, cells_y, depth = density.shape
    rows = parcel_mass.shape[0]
    capacity = rows // 16
    chunks = rows // LANES
    step = min(1024, rows)
    sds = jax.ShapeDtypeStruct
    whole = pl.BlockSpec(memory_space=VMEM)
    parcels = sds((8, capacity + 3 * depth), F32)
    dense = sds((chunks, LANES), F32)
    place, stays, words, masks, numbers = call(
        functools.partial(rank_kernel, cells_x, cells_y),
        (
            dense,
            dense,
            sds((chunks, LANES), I32),
            sds((KINDS, 3, chunks, LANES), F32),
            sds((1, LANES), I32),
        ),
        scratch=(VMEM((chunks, LANES), I32), VMEM((chunks, LANES), I32)),
        in_specs=[pl.BlockSpec(memory_space=pltpu.SMEM), whole],
        cost_estimate=pl.CostEstimate(flops=10**9, bytes_accessed=10**6, transcendentals=0),
    )(parcel_count, parcel_cell)
    even, odd, stay, own, leaving, partial, compact = call(
        functools.partial(prep_kernel, cells_x, cells_y, step),
        (
            parcels,
            parcels,
            sds((8, rows), F32),
            sds((2, 8, capacity), F32),
            sds((4, cells_x, depth), F32),
            sds((2, cells_y, depth), F32),
            sds((chunks, 8, LANES), F32),
        ),
        scratch=(
            VMEM((8, rows), F32),
            pltpu.SMEM((chunks, LANES), I32),
            VMEM((4, capacity // LANES + 1, 8, LANES), F32),
            VMEM((4 * (cells_x + cells_y), depth), F32),
            pltpu.SemaphoreType.DMA,
        ),
    )(
        parcel_mass.reshape(chunks, LANES),
        parcel_temp.reshape(chunks, LANES),
        droplet_velocity,
        parcel_cell,
        energy,
        place,
        stays,
        words,
        masks,
    )
    y_even, y_odd = swap("gy", even, odd)
    slots = rows + 4 * capacity
    side = lambda n: sds((5 * n * cells_y, depth), F32)
    smem = pl.BlockSpec(memory_space=pltpu.SMEM)
    above = sds((chunks + 1, 8, LANES), F32)
    dep_low, state, where_to, high = call(
        functools.partial(deposit_kernel, cells_x, cells_y, 0),
        (side(CUT), sds((5, slots), F32), sds((3, slots), I32), above),
        scratch=(
            VMEM(above.shape, F32),
            pltpu.SMEM((chunks, LANES), I32),
            pltpu.SemaphoreType.DMA,
        ),
        in_specs=[smem] + [whole] * 4,
    )(numbers, compact, words, masks, stay)
    even, odd, planes_y, halo_y = call(
        functools.partial(relay_kernel, cells_x, cells_y),
        (parcels, parcels, sds((2, 5, cells_x, depth), F32), sds((2, cells_x, depth), F32)),
        in_specs=[whole] * 5 + [pl.BlockSpec(memory_space=pl.ANY)],
    )(y_even, y_odd, partial, own, leaving, dep_low)
    x_even, x_odd = swap("gx", even, odd)
    (dep_high,) = call(
        functools.partial(deposit_kernel, cells_x, cells_y, 1),
        (side(cells_x - CUT),),
        in_specs=[smem, whole, pl.BlockSpec(memory_space=pl.ANY)],
    )(numbers, high, halo_y)
    dep_low, dep_high = (d.reshape(5, -1, cells_y, depth) for d in (dep_low, dep_high))
    last = rows // (4 * capacity)
    rho, impulse, energy_out, top, state, where_to = call(
        functools.partial(update_kernel, cells_x, cells_y),
        (
            sds(density.shape, F32),
            sds(momentum.shape, F32),
            sds(energy.shape, F32),
            sds((lax.axis_size(("gx", "gy")), LANES), F32),
            sds(state.shape, F32),
            sds(where_to.shape, I32),
        ),
        scratch=(
            VMEM((cells_x + 2, cells_y, depth), F32),
            VMEM((2, 5, cells_y, depth), F32),
        ),
        in_specs=[whole] * 12 + [pl.BlockSpec(memory_space=pl.ANY)] * 2,
        out_specs=(whole,) * 4
        + (
            pl.BlockSpec((5, 4 * capacity), lambda i: (0, last)),
            pl.BlockSpec((3, 4 * capacity), lambda i: (0, last)),
        ),
        aliases={12: 4, 13: 5},
        grid=(1,),
    )(
        y_even, y_odd, x_even, x_odd, density, momentum, energy, dep_low, dep_high,
        planes_y, halo_y, leaving, state, where_to,
    )
    fastest = jnp.max(lax.all_to_all(top, ("gx", "gy"), 0, 0, tiled=True), axis=0)[0]
    return rho, impulse, energy_out, state, where_to, COURANT / fastest


def solution(mesh):
    both = ("gx", "gy")
    return jax.shard_map(
        on_device,
        mesh=mesh,
        in_specs=(
            P("gx", "gy", None),
            P(None, "gx", "gy", None),
            P("gx", "gy", None),
            P(both),
            P(None, both),
            P(both),
            P(None, both),
            P(both),
        ),
        out_specs=(
            P("gx", "gy", None),
            P(None, "gx", "gy", None),
            P("gx", "gy", None),
            P(None, both),
            P(None, both),
            P(),
        ),
        check_vma=False,
    )
```
